256 devices in a mesh: lon: 16 (over x, y), lat: 16 (over z, core).
Axes of the slice: x: 4, y: 4, z: 8, core: 2. Of those that a mesh axis runs over, the one named last changes fastest.
Arguments:
- meridional_speed: float32 [16, 1024, 4096], P(None, 'lat', 'lon'), may hold values from -6 to 6
- theta_field: float32 [16, 1024, 4096], P(None, 'lat', 'lon'), may hold values from -2 to 30
- tier_vertical_span: float32 [16], replicated, may hold values from 0.5 to 4
- grid_zonal_span: float32 [1024, 4096], P('lat', 'lon'), may hold values from 0.05 to 40
- grid_plan_extent: float32 [1024, 4096], P('lat', 'lon'), may hold values from 0.2 to 5
- ocean_energy_input: float32 [1024, 4096], P('lat', 'lon'), may hold values from -6 to 6
- ocean_tier_tally: int32 [1024, 4096], P('lat', 'lon'), may hold values from 0 to 16, as said below
- grid_region_label: int32 [1024, 4096], P('lat', 'lon'), may hold values from 0 to 3
- seam_matching_meridian: int32 [4096], P('lon'), may hold values from 0 to 4095, as said below
Outputs:
- class_transport: float32 [4, 1024, 128], P(None, 'lat')
- overturning: float32 [4, 1024, 16], P(None, 'lat')
- heat_transport: float32 [4, 1024], P(None, 'lat')
- implied_transport: float32 [4, 1024], P(None, 'lat')
The draws below stay inside these ranges and needn't reach their ends.
Inputs may be any that keep to these rules, and one draw needn't show every extreme that they name: `ocean_tier_tally`: one column, the same at every latitude, has at least one wet level, and every column of the northernmost row has at least one. seam_matching_meridian[i] = (c - i) mod 4096 for a c that each draw picks.
All inputs are finite; a program needn't handle non-finite values.
Results may differ from the reference program's by a relative error of at most 0.0003.
Values sent between devices are 32-bit elements; how exact they have to be, the bound alone decides.
A program may use at most 64 MiB of HBM per device.

```python
import math
import jax
import jax.numpy as jnp
from jax import lax

LOCAL_PARALLELS = 64
VERTICAL_TIERS = 16
THERMAL_BINS = 128
OCEAN_REGIONS = 4
GRID_MERIDIANS = 4096
GRID_PARALLELS = 1024


def draw_grid_zonal_span(key, part):
    column = jnp.arange(GRID_MERIDIANS, dtype=jnp.float32)[None, :] / (GRID_MERIDIANS - 1.0)
    base_width = jnp.exp(jax.random.uniform(key, (GRID_PARALLELS, GRID_MERIDIANS), jnp.float32, jnp.log(0.3), jnp.log(3.0)))
    return (base_width * jnp.exp(jnp.log(3.0) * column)).astype(jnp.float32)


def draw_ocean_tier_tally(key, part):
    raw_depth = jax.random.randint(key, (GRID_PARALLELS, GRID_MERIDIANS), -(VERTICAL_TIERS // 3), VERTICAL_TIERS + 1, dtype=jnp.int32)
    col_depth = jnp.maximum(raw_depth, 0)
    wet_column = jax.random.randint(jax.random.fold_in(key, 11), (), 0, GRID_MERIDIANS, dtype=jnp.int32)
    column_ids = jnp.arange(GRID_MERIDIANS, dtype=jnp.int32)[None, :]
    row_ids = jnp.arange(GRID_PARALLELS, dtype=jnp.int32)[:, None]
    forced = (column_ids == wet_column) | (row_ids == GRID_PARALLELS - 1)
    return jnp.where(forced, jnp.maximum(col_depth, 1), col_depth).astype(jnp.int32)


def draw_seam_matching_meridian(key, part):
    centre = jax.random.randint(key, (), 0, GRID_MERIDIANS, dtype=jnp.int32)
    column_ids = jnp.arange(GRID_MERIDIANS, dtype=jnp.int32)
    return jnp.mod(centre - column_ids + GRID_MERIDIANS, GRID_MERIDIANS).astype(jnp.int32)


def place_ends(array, rng, least, largest):
    shape = array.shape
    spot = [jax.random.randint(jax.random.fold_in(rng, axis), (), 0, shape[axis]) for axis in range(len(shape))]
    array = array.at[tuple(spot)].set(least)
    longest = shape.index(max(shape))
    spot[longest] = (spot[longest] + 1) % shape[longest]
    return array.at[tuple(spot)].set(largest)


def level_of(own_key, dims, shards, low, largest):
    factor_of, own = 1.0, jax.random.fold_in(own_key, 6)
    for position, blocks in shards:
        draws = jnp.exp(jax.random.uniform(jax.random.fold_in(own, position), (blocks,), jnp.float32, low / len(shards), largest / len(shards)))
        factor_of = factor_of * jnp.repeat(draws, dims[position] // blocks).reshape([-1 if axis == position else 1 for axis in range(len(dims))])
    return factor_of


def gaussian(rng, shape, scale, bound, split=(), held_as=jnp.bfloat16):
    array = jax.random.normal(rng, shape, jnp.float32) * scale
    if len(split) > 0:
        array = level_of(rng, shape, split, -0.22, 0.18) * array
    return jnp.clip(array, min=-bound, max=bound).astype(held_as)


def setup_inputs(seed: int = 0) -> dict:
    splits = jax.random.split(jax.random.key(seed), 10)
    meridional_speed = gaussian(splits[0], (VERTICAL_TIERS, GRID_PARALLELS, GRID_MERIDIANS), 1.0, 6.0, ((1, 16), (2, 16)), jnp.float32)
    theta_field = jnp.clip(-2.0 + 32.0 * jax.random.uniform(splits[1], (VERTICAL_TIERS, GRID_PARALLELS, GRID_MERIDIANS), jnp.float32) ** level_of(splits[1], (VERTICAL_TIERS, GRID_PARALLELS, GRID_MERIDIANS), ((1, 16), (2, 16)), -0.2, 0.2), -2.0, 30.0)
    tier_vertical_span = jnp.clip(jnp.exp(jax.random.uniform(splits[2], (VERTICAL_TIERS,), jnp.float32, math.log(0.5), math.log(4.0))), 0.5, 4.0)
    grid_zonal_span = draw_grid_zonal_span(jax.random.fold_in(splits[9], 71), 0)
    grid_plan_extent = jnp.clip(jnp.exp(math.log(5.0) - 3.218876 * jax.random.uniform(splits[4], (GRID_PARALLELS, GRID_MERIDIANS), jnp.float32) ** level_of(splits[4], (GRID_PARALLELS, GRID_MERIDIANS), ((0, 16), (1, 16)), -0.2, 0.2)), 0.2, 5.0)
    ocean_energy_input = gaussian(splits[5], (GRID_PARALLELS, GRID_MERIDIANS), 1.0, 6.0, ((0, 16), (1, 16)), jnp.float32)
    ocean_tier_tally = draw_ocean_tier_tally(jax.random.fold_in(splits[9], 71), 0)
    grid_region_label = place_ends(jax.random.randint(splits[7], (GRID_PARALLELS, GRID_MERIDIANS), 0, OCEAN_REGIONS), jax.random.fold_in(splits[7], 1), 0, OCEAN_REGIONS - 1).astype(jnp.int32)
    seam_matching_meridian = draw_seam_matching_meridian(jax.random.fold_in(splits[9], 71), 0)
    return {"meridional_speed": meridional_speed, "theta_field": theta_field, "tier_vertical_span": tier_vertical_span, "grid_zonal_span": grid_zonal_span, "grid_plan_extent": grid_plan_extent, "ocean_energy_input": ocean_energy_input, "ocean_tier_tally": ocean_tier_tally, "grid_region_label": grid_region_label, "seam_matching_meridian": seam_matching_meridian}


THERMAL_FLOOR = -2.0
THERMAL_RANGE = 32.0

def vertical_aggregate_field(meridional_speed, theta_field, tier_vertical_span, grid_zonal_span, grid_plan_extent, ocean_energy_input, ocean_tier_tally, grid_region_label, subsequent_theta, subsequent_vertical_extent, theta_bucket_tally, region_tally):
    tier_ordinal, parallel_tally, meridian_tally = theta_field.shape
    poleward_theta = jnp.concatenate([theta_field[:, 1:, :], subsequent_theta[:, None, :]], axis=1)
    interface_theta = 0.5 * (theta_field + poleward_theta)
    north_depth = jnp.concatenate([ocean_tier_tally[1:, :], subsequent_vertical_extent[None, :]], axis=0)
    face_depth = jnp.minimum(ocean_tier_tally, north_depth)
    level_iota = lax.broadcasted_iota(jnp.int32, (tier_ordinal, 1, 1), 0)
    wet_mask = (level_iota < face_depth[None, :, :]).astype(jnp.float32)
    water_capacity = wet_mask * tier_vertical_span[:, None, None] * grid_zonal_span[None, :, :]
    mass_conveyance = water_capacity * meridional_speed
    bucket_spacing = THERMAL_RANGE / theta_bucket_tally
    placement_offset = jnp.clip((interface_theta - THERMAL_FLOOR) / bucket_spacing, 0.0, theta_bucket_tally - 1.0)
    lower_real_value = jnp.minimum(jnp.floor(placement_offset), theta_bucket_tally - 2.0)
    upper_interp_factor = placement_offset - lower_real_value
    parallel_ramp = lax.broadcasted_iota(jnp.int32, (1, parallel_tally, 1), 1)
    group_labels = (grid_region_label[None, :, :] * parallel_tally + parallel_ramp) * theta_bucket_tally + lower_real_value.astype(jnp.int32)
    group_labels = group_labels.reshape(-1)
    bucket_aggregate = jax.ops.segment_sum(jnp.concatenate([(mass_conveyance * (1.0 - upper_interp_factor)).reshape(-1), (mass_conveyance * upper_interp_factor).reshape(-1)]), jnp.concatenate([group_labels, group_labels + 1]), num_segments=region_tally * parallel_tally * theta_bucket_tally)
    bucket_aggregate = bucket_aggregate.reshape(region_tally, parallel_tally, theta_bucket_tally)
    basin_iota = lax.broadcasted_iota(jnp.int32, (region_tally, 1, 1), 0)
    bucket_membership = (grid_region_label[None, :, :] == basin_iota).astype(jnp.float32)
    level_sum = jnp.einsum('bji,kji->bjk', bucket_membership, mass_conveyance, precision=lax.Precision.HIGHEST)
    energy_aggregate = jnp.einsum('dwk,wk->dw', bucket_membership, lax.optimization_barrier(jnp.sum(mass_conveyance * interface_theta, axis=0)), precision=lax.Precision.HIGHEST)
    parallel_theta_field = lax.optimization_barrier(jnp.sum(water_capacity * interface_theta, axis=(0, 2)))
    row_wet = lax.optimization_barrier(jnp.sum(water_capacity, axis=(0, 2)))
    flux_rows = jnp.einsum('dwk,wk->dw', bucket_membership, ocean_energy_input * grid_plan_extent, precision=lax.Precision.HIGHEST)
    return (bucket_aggregate, level_sum, energy_aggregate, parallel_theta_field, row_wet, flux_rows)

def finish_rows(bucket_aggregate, level_sum, energy_aggregate, parallel_theta_field, row_wet, unit_scale):
    row_mean = parallel_theta_field / row_wet
    volume_total = lax.optimization_barrier(jnp.sum(level_sum, axis=2))
    heat_out = unit_scale / 16.0 * (energy_aggregate - volume_total * row_mean[None, :])
    stream = unit_scale * jnp.cumsum(level_sum, axis=2)
    return (unit_scale * bucket_aggregate, stream, heat_out)

def reference(meridional_speed, theta_field, tier_vertical_span, grid_zonal_span, grid_plan_extent, ocean_energy_input, ocean_tier_tally, grid_region_label, seam_matching_meridian):
    reflected_theta = jnp.take(theta_field[:, GRID_PARALLELS - 1, :], seam_matching_meridian, axis=1)
    mirror_depth = jnp.take(ocean_tier_tally[GRID_PARALLELS - 1, :], seam_matching_meridian, axis=0)
    unit_scale = math.sqrt(THERMAL_BINS / (GRID_MERIDIANS * VERTICAL_TIERS))

    def row_block(parallel_initial_offset):
        tile_theta_field = lax.dynamic_slice_in_dim(theta_field, parallel_initial_offset, LOCAL_PARALLELS, 1)
        tile_speed_field = lax.dynamic_slice_in_dim(meridional_speed, parallel_initial_offset, LOCAL_PARALLELS, 1)
        tile_vertical_extent = lax.dynamic_slice_in_dim(ocean_tier_tally, parallel_initial_offset, LOCAL_PARALLELS, 0)
        tile_zonal_span = lax.dynamic_slice_in_dim(grid_zonal_span, parallel_initial_offset, LOCAL_PARALLELS, 0)
        tile_plan_extent = lax.dynamic_slice_in_dim(grid_plan_extent, parallel_initial_offset, LOCAL_PARALLELS, 0)
        tile_energy_input = lax.dynamic_slice_in_dim(ocean_energy_input, parallel_initial_offset, LOCAL_PARALLELS, 0)
        tile_region_label = lax.dynamic_slice_in_dim(grid_region_label, parallel_initial_offset, LOCAL_PARALLELS, 0)
        subsequent_offset = jnp.minimum(parallel_initial_offset + LOCAL_PARALLELS, GRID_PARALLELS - 1).astype(jnp.int32)
        final_flag = parallel_initial_offset + LOCAL_PARALLELS >= GRID_PARALLELS
        next_theta_value = lax.dynamic_slice_in_dim(theta_field, subsequent_offset, 1, 1)[:, 0, :]
        later_vertical_extent = lax.dynamic_slice_in_dim(ocean_tier_tally, subsequent_offset, 1, 0)[0]
        next_theta_value = jnp.where(final_flag, reflected_theta, next_theta_value)
        later_vertical_extent = jnp.where(final_flag, mirror_depth, later_vertical_extent)
        return vertical_aggregate_field(tile_speed_field, tile_theta_field, tier_vertical_span, tile_zonal_span, tile_plan_extent, tile_energy_input, tile_vertical_extent, tile_region_label, next_theta_value, later_vertical_extent, THERMAL_BINS, OCEAN_REGIONS)
    starts = jnp.arange(GRID_PARALLELS // LOCAL_PARALLELS, dtype=jnp.int32) * LOCAL_PARALLELS
    bucket_aggregate, level_sum, energy_aggregate, parallel_theta_field, row_wet, flux_rows = lax.map(row_block, starts)
    bucket_aggregate = jnp.transpose(bucket_aggregate, (1, 0, 2, 3)).reshape(OCEAN_REGIONS, GRID_PARALLELS, THERMAL_BINS)
    level_sum = jnp.transpose(level_sum, (1, 0, 2, 3)).reshape(OCEAN_REGIONS, GRID_PARALLELS, VERTICAL_TIERS)
    energy_aggregate = jnp.transpose(energy_aggregate, (1, 0, 2)).reshape(OCEAN_REGIONS, GRID_PARALLELS)
    flux_rows = jnp.transpose(flux_rows, (1, 0, 2)).reshape(OCEAN_REGIONS, GRID_PARALLELS)
    parallel_theta_field = parallel_theta_field.reshape(GRID_PARALLELS)
    row_wet = row_wet.reshape(GRID_PARALLELS)
    class_out, stream, heat_out = finish_rows(bucket_aggregate, level_sum, energy_aggregate, parallel_theta_field, row_wet, unit_scale)
    implied = 2.0 / math.sqrt(GRID_MERIDIANS * GRID_PARALLELS) * jnp.cumsum(flux_rows, axis=1)
    return (class_out, stream, heat_out, implied)
```

```python
import math

import jax
import jax.numpy as jnp
from jax import lax
from jax.experimental import pallas as pl
from jax.experimental.pallas import tpu as pltpu
from jax.sharding import PartitionSpec as P

BINS = 128
REGIONS = 4
TIERS = 16
ROWS = 64
COLS = 256
NLON = 16
NLAT = 16
GROUP = 8
OWNED = ROWS // NLON
HI = 16
LO = BINS // HI
PAY = 24

HEAT, THETA, WET, FLUX, SOUTH = 64, 68, 69, 72, 76

UNIT = math.sqrt(BINS / (COLS * NLON * TIERS))
IMPLIED = 2.0 / math.sqrt(COLS * NLON * ROWS * NLAT)
F32, BF16 = jnp.float32, jnp.bfloat16


def iota(shape, dim):
    return lax.broadcasted_iota(jnp.int32, shape, dim)


def two_terms(x):
    high = x.astype(BF16).astype(F32)
    return high, x - high


def kernel(
    speed_h, theta_h, dz_s, dx_h, area_h, flux_h, tally_h, region_h, seam_s,
    out_class, out_over, out_heat, out_impl,
    th, sp, dx, area, flux, tally, region, bc, part, crow, sfin,
    rs_send, rs_recv, ag_send, ag_recv,
    halo_send, halo_recv, fold_send, fold_recv, pfx_send, pfx_recv,
    in_sem, rs_ssem, rs_rsem, ag_ssem, ag_rsem, fold_ssem, fold_rsem,
    halo_ssem, halo_rsem, pfx_ssem, pfx_rsem,
):
    o = lax.axis_index("lon")
    l = lax.axis_index("lat")
    lane8 = iota((8, 128), 1)

    loads = [
        pltpu.make_async_copy(flux_h, flux, in_sem.at[0]),
        pltpu.make_async_copy(area_h, area, in_sem.at[1]),
        pltpu.make_async_copy(region_h, region, in_sem.at[2]),
        pltpu.make_async_copy(tally_h, tally.at[pl.ds(0, ROWS)], in_sem.at[3]),
        pltpu.make_async_copy(dx_h, dx, in_sem.at[4]),
        pltpu.make_async_copy(theta_h, th.at[:, pl.ds(0, ROWS)], in_sem.at[5]),
        pltpu.make_async_copy(speed_h, sp, in_sem.at[6]),
    ]
    for load in loads:
        load.start()

    barrier = pltpu.get_barrier_semaphore()
    for d in range(1, NLON):
        pl.semaphore_signal(barrier, inc=1, device_id={"lon": lax.rem(o + d, NLON)}, device_id_type=pl.DeviceIdType.MESH)
    for d in range(1, NLAT):
        pl.semaphore_signal(barrier, inc=1, device_id={"lat": lax.rem(l + d, NLAT)}, device_id_type=pl.DeviceIdType.MESH)
    for load in loads:
        load.wait()

    acc = [jnp.zeros((8, COLS), F32) for _ in range(REGIONS)]
    for g in range(ROWS // 8):
        rows = slice(8 * g, 8 * g + 8)
        f = flux[rows, :] * area[rows, :]
        reg = region[rows, :]
        for b in range(REGIONS):
            acc[b] = acc[b] + jnp.where(reg == b, f, 0.0)
    totals = jnp.zeros((8, 128), F32)
    for b in range(REGIONS):
        t = jnp.sum(jnp.sum(acc[b], axis=0, keepdims=True), axis=1, keepdims=True)
        totals = jnp.where(lane8 == SOUTH + b, t, totals)
    pfx_send[...] = totals

    for k in range(TIERS):
        halo_send[k : k + 1, :] = th[k, 0:1, :]
        fold_send[k : k + 1, :] = th[k, ROWS - 1 : ROWS, :]
    halo_send[TIERS:24, :] = jnp.broadcast_to(tally[0:1, :].astype(F32), (8, COLS))
    fold_send[TIERS:24, :] = jnp.broadcast_to(tally[ROWS - 1 : ROWS, :].astype(F32), (8, COLS))

    def halo_copy():
        return pltpu.make_async_remote_copy(
            halo_send, halo_recv, halo_ssem, halo_rsem, device_id={"lat": lax.max(l - 1, 0)},
            device_id_type=pl.DeviceIdType.MESH)

    def fold_copy(dst, src):
        return pltpu.make_async_remote_copy(
            fold_send, fold_recv.at[src], fold_ssem.at[dst], fold_rsem.at[src],
            device_id={"lon": dst}, device_id_type=pl.DeviceIdType.MESH)

    def pfx_copy(dst, src):
        return pltpu.make_async_remote_copy(
            pfx_send, pfx_recv.at[src], pfx_ssem.at[dst], pfx_rsem.at[src],
            device_id={"lat": dst}, device_id_type=pl.DeviceIdType.MESH)

    def rs_copy(dst, src):
        return pltpu.make_async_remote_copy(
            rs_send.at[dst], rs_recv.at[src], rs_ssem.at[dst], rs_rsem.at[src],
            device_id={"lon": dst}, device_id_type=pl.DeviceIdType.MESH)

    def ag_copy(dst, src):
        return pltpu.make_async_remote_copy(
            ag_send, ag_recv.at[src], ag_ssem.at[dst], ag_rsem.at[src],
            device_id={"lon": dst}, device_id_type=pl.DeviceIdType.MESH)

    def others(count, me, act):
        def step(q, c):
            @pl.when(q != me)
            def _():
                act(q)
            return c
        lax.fori_loop(0, count, step, 0)

    def first_sends():
        pl.semaphore_wait(barrier, NLON - 1 + NLAT - 1)

        @pl.when(l > 0)
        def _():
            halo_copy().start()

        @pl.when(l == NLAT - 1)
        def _():
            others(NLON, o, lambda q: fold_copy(q, o).start())
            fold_recv[o] = fold_send[...]

        def north(q, c):
            @pl.when(q > l)
            def _():
                pfx_copy(q, l).start()
            return c
        lax.fori_loop(0, NLAT, north, 0)

    def north_row():
        @pl.when(l < NLAT - 1)
        def _():
            halo_copy().wait_recv()
            for k in range(TIERS):
                th[k, ROWS : ROWS + 1, :] = halo_recv[k : k + 1, :]
            tally[ROWS : ROWS + 1, :] = halo_recv[TIERS : TIERS + 1, :].astype(jnp.int32)

        @pl.when(l == NLAT - 1)
        def _():
            others(NLON, o, lambda q: fold_copy(o, q).wait_recv())
            first = seam_s[0]
            owner = lax.shift_right_logical(first, 8)
            at = jnp.bitwise_and(first, COLS - 1)
            high = fold_recv[owner]
            low = fold_recv[jnp.bitwise_and(owner + NLON - 1, NLON - 1)]
            for t in range(COLS // 128):
                i = lane8 + 128 * t
                spot = jnp.bitwise_and(at - i, COLS - 1)
                lane = jnp.bitwise_and(spot, 127)
                for r in range(3):
                    rows = slice(8 * r, 8 * r + 8)
                    pick = [
                        jnp.where(
                            spot >= 128,
                            jnp.take_along_axis(src[rows, 128:], lane, axis=1),
                            jnp.take_along_axis(src[rows, :128], lane, axis=1),
                        )
                        for src in (high, low)
                    ]
                    halo_recv[rows, 128 * t : 128 * t + 128] = jnp.where(i <= at, pick[0], pick[1])
            for k in range(TIERS):
                th[k, ROWS : ROWS + 1, :] = halo_recv[k : k + 1, :]
            tally[ROWS : ROWS + 1, :] = halo_recv[TIERS : TIERS + 1, :].astype(jnp.int32)

        def south(q, c):
            @pl.when(q < l)
            def _():
                pfx_copy(l, q).wait_recv()
            return c
        lax.fori_loop(0, NLAT, south, 0)

    sub8 = iota((8, COLS), 0)
    hi_iota = iota((HI, COLS), 0).astype(F32).astype(BF16)
    cl_iota = iota((REGIONS * LO, COLS), 0).astype(F32).astype(BF16)
    zero16 = jnp.zeros((HI, COLS), BF16)
    one32 = jnp.ones((REGIONS * LO, COLS), BF16)
    zero32 = jnp.zeros((REGIONS * LO, COLS), BF16)

    def group(g, carry):
        @pl.when(g == ROWS // GROUP - 1)
        def _():
            north_row()

        base = pl.multiple_of(g * GROUP, GROUP)
        here = pl.ds(base, GROUP)
        nxt = pl.ds(base + GROUP, 1)
        deep = tally[here, :]
        deep_n = jnp.where(sub8 == 7, tally[nxt, :], pltpu.roll(deep, 7, 0))
        face_depth = jnp.minimum(deep, deep_n)
        width = dx[here, :]
        reg = region[here, :]
        regf = reg.astype(F32)
        member = [reg == b for b in range(REGIONS)]
        heat = jnp.zeros((8, COLS), F32)
        theta_sum = jnp.zeros((8, COLS), F32)
        wet_sum = jnp.zeros((8, COLS), F32)
        stats = jnp.zeros((8, 128), F32)
        for k in range(TIERS):
            t = th[k, here, :]
            tn = jnp.where(sub8 == 7, th[k, nxt, :], pltpu.roll(t, 7, 0))
            face = 0.5 * (t + tn)
            vol = jnp.where(face_depth > k, dz_s[k] * width, 0.0)
            mass = vol * sp[k, here, :]
            pos = jnp.clip((face - (-2.0)) * (BINS / 32.0), 0.0, BINS - 1.0)
            low = jnp.minimum(jnp.floor(pos), BINS - 2.0)
            w = pos - low
            hi = jnp.floor(low * (1.0 / LO))
            bc[0, k] = hi
            bc[1, k] = (low - hi * LO) + regf * LO
            s0, s1 = two_terms(mass)
            bc[2, k] = s0
            bc[3, k] = s1
            s0, s1 = two_terms(mass * w)
            bc[4, k] = s0
            bc[5, k] = s1
            heat = heat + mass * face
            theta_sum = theta_sum + vol * face
            wet_sum = wet_sum + vol
            for b in range(REGIONS):
                red = jnp.sum(jnp.where(member[b], mass, 0.0), axis=1, keepdims=True)
                stats = jnp.where(lane8 == b * TIERS + k, red, stats)
        f = flux[here, :] * area[here, :]
        for b in range(REGIONS):
            red = jnp.sum(jnp.where(member[b], heat, 0.0), axis=1, keepdims=True)
            stats = jnp.where(lane8 == HEAT + b, red, stats)
            red = jnp.sum(jnp.where(member[b], f, 0.0), axis=1, keepdims=True)
            stats = jnp.where(lane8 == FLUX + b, red, stats)
        stats = jnp.where(lane8 == THETA, jnp.sum(theta_sum, axis=1, keepdims=True), stats)
        stats = jnp.where(lane8 == WET, jnp.sum(wet_sum, axis=1, keepdims=True), stats)
        for h in range(2):
            rs_send[2 * g + h, 16:20, :] = stats[4 * h : 4 * h + 4, :]

        @pl.when(g == ROWS // GROUP - 1)
        def _():
            def add(q, c):
                return c + jnp.where(q < l, pfx_recv[q], 0.0)
            south = lax.fori_loop(0, NLAT, add, jnp.zeros((8, 128), F32))
            rs_send[2 * g + 1, 16:24, :] = rs_send[2 * g + 1, 16:24, :] + south

        for jj in range(GROUP):
            total = None
            for k in range(TIERS):
                def row(n, rows):
                    return jnp.broadcast_to(bc[n, k, jj : jj + 1, :], (rows, COLS)).astype(BF16)
                mask = row(0, HI) == hi_iota
                lhs = jnp.concatenate(
                    [jnp.where(mask, row(n, HI), zero16) for n in (2, 3, 4, 5)], axis=0)
                rhs = jnp.where(row(1, REGIONS * LO) == cl_iota, one32, zero32)
                d = lax.dot_general(lhs, rhs, (((1,), (1,)), ((), ())), preferred_element_type=F32)
                total = d if total is None else total + d
            lanes = slice(32 * (jj % 4), 32 * (jj % 4) + 32)
            part[jj // 4, 0:HI, lanes] = total[0:HI] + total[HI : 2 * HI]
            part[jj // 4, HI : 2 * HI, lanes] = total[2 * HI : 3 * HI] + total[3 * HI :]
        lane16 = iota((HI, 128), 1)
        first_hi = iota((HI, 128), 0) == 0
        for h in range(2):
            s0 = part[h, 0:HI, :]
            s1 = part[h, HI : 2 * HI, :]
            up = jnp.where(first_hi, 0.0, pltpu.roll(pltpu.roll(s1, 128 - (LO - 1), 1), 1, 0))
            moved = jnp.where(jnp.bitwise_and(lane16, LO - 1) == 0, up, pltpu.roll(s1, 1, 1))
            rs_send[2 * g + h, 0:HI, :] = s0 - s1 + moved

        @pl.when(g == 0)
        def _():
            first_sends()

        for h in range(2):
            @pl.when(2 * g + h != o)
            def _():
                rs_copy(2 * g + h, o).start()
        return carry

    lax.fori_loop(0, ROWS // GROUP, group, 0)

    others(NLON, o, lambda q: rs_copy(o, q).wait_recv())

    def add(q, c):
        return c + jnp.where(q != o, rs_recv[q], 0.0)

    own = lax.fori_loop(0, NLON, add, rs_send[o])
    crow[...] = own[0:HI]
    sub = iota((8, 128), 0)
    block = lax.shift_right_logical(lane8, 3)
    for v in range(2):
        r = sub + 8 * v
        index = 32 * jnp.bitwise_and(r, 3) + 8 * lax.shift_right_logical(r, 2) + jnp.bitwise_and(lane8, LO - 1)
        res = jnp.zeros((8, 128), F32)
        for hi in range(HI):
            spread = jnp.broadcast_to(crow[hi : hi + 1, :], (8, 128))
            res = jnp.where(block == hi, jnp.take_along_axis(spread, index, axis=1), res)
        ag_send[8 * v : 8 * v + 8, :] = res
    ag_send[16:24, :] = own[16:24]
    others(NLON, o, lambda q: ag_copy(q, o).start())
    ag_recv[o] = ag_send[...]
    others(NLON, o, lambda q: ag_copy(o, q).wait_recv())

    for s in range(NLON):
        for b in range(REGIONS):
            out_class[b, 4 * s : 4 * s + 4, :] = UNIT * ag_recv[s, 4 * b : 4 * b + 4, :]
        sfin[4 * s : 4 * s + 4, :] = ag_recv[s, 16:20, :]
    sfin[ROWS:128, :] = jnp.zeros((128 - ROWS, 128), F32)
    rowsum = sfin[0:ROWS, :]
    lanes = iota((ROWS, 128), 1)
    x = rowsum
    for step in (1, 2, 4, 8):
        x = x + jnp.where(jnp.bitwise_and(lanes, 15) >= step, pltpu.roll(x, step, 1), 0.0)
    for b in range(REGIONS):
        out_over[b] = UNIT * x[:, 16 * b : 16 * b + 16]
    flipped = jnp.transpose(sfin[...])
    wet = flipped[WET : WET + 1, :]
    mean = flipped[THETA : THETA + 1, :] / jnp.where(iota((1, 128), 1) < ROWS, wet, 1.0)
    for b in range(REGIONS):
        vol = jnp.sum(flipped[16 * b : 16 * b + 16, :], axis=0, keepdims=True)
        res = (UNIT / 16.0) * (flipped[HEAT + b : HEAT + b + 1, :] - vol * mean)
        out_heat[b : b + 1, :] = res[:, 0:ROWS]
    c = flipped[FLUX : FLUX + 8, :]
    south = jnp.sum(jnp.where(lane8 == ROWS - 1, c, 0.0), axis=1, keepdims=True)
    for step in (1, 2, 4, 8, 16, 32):
        c = c + jnp.where(lane8 >= step, pltpu.roll(c, step, 1), 0.0)
    out_impl[...] = (IMPLIED * (c[0:4] + south[4:8]))[:, 0:ROWS]

    others(NLON, o, lambda q: rs_copy(q, o).wait_send())
    others(NLON, o, lambda q: ag_copy(q, o).wait_send())

    @pl.when(l > 0)
    def _():
        halo_copy().wait_send()

    @pl.when(l == NLAT - 1)
    def _():
        others(NLON, o, lambda q: fold_copy(q, o).wait_send())

    def north_done(q, c):
        @pl.when(q > l)
        def _():
            pfx_copy(q, l).wait_send()
        return c
    lax.fori_loop(0, NLAT, north_done, 0)


def body(speed, theta, dz, dx, area, flux, tally, region, seam):
    any_ = pl.BlockSpec(memory_space=pl.ANY)
    smem = pl.BlockSpec(memory_space=pltpu.SMEM)
    vmem = pl.BlockSpec(memory_space=pltpu.VMEM)
    dma = pltpu.SemaphoreType.DMA
    return pl.pallas_call(
        kernel,
        out_shape=(
            jax.ShapeDtypeStruct((REGIONS, ROWS, BINS), F32),
            jax.ShapeDtypeStruct((REGIONS, ROWS, TIERS), F32),
            jax.ShapeDtypeStruct((REGIONS, ROWS), F32),
            jax.ShapeDtypeStruct((REGIONS, ROWS), F32),
        ),
        in_specs=[any_, any_, smem, any_, any_, any_, any_, any_, smem],
        out_specs=(vmem, vmem, vmem, vmem),
        scratch_shapes=[
            pltpu.VMEM((TIERS, ROWS + 8, COLS), F32),
            pltpu.VMEM((TIERS, ROWS, COLS), F32),
            pltpu.VMEM((ROWS, COLS), F32),
            pltpu.VMEM((ROWS, COLS), F32),
            pltpu.VMEM((ROWS, COLS), F32),
            pltpu.VMEM((ROWS + 8, COLS), jnp.int32),
            pltpu.VMEM((ROWS, COLS), jnp.int32),
            pltpu.VMEM((6, TIERS, GROUP, COLS), F32),
            pltpu.VMEM((2, 2 * HI, 128), F32),
            pltpu.VMEM((HI, 128), F32),
            pltpu.VMEM((128, 128), F32),
            pltpu.VMEM((NLON, PAY, 128), F32),
            pltpu.VMEM((NLON, PAY, 128), F32),
            pltpu.VMEM((PAY, 128), F32),
            pltpu.VMEM((NLON, PAY, 128), F32),
            pltpu.VMEM((24, COLS), F32),
            pltpu.VMEM((24, COLS), F32),
            pltpu.VMEM((24, COLS), F32),
            pltpu.VMEM((NLON, 24, COLS), F32),
            pltpu.VMEM((8, 128), F32),
            pltpu.VMEM((NLAT, 8, 128), F32),
            dma((7,)),
            dma((NLON,)), dma((NLON,)), dma((NLON,)), dma((NLON,)), dma((NLON,)), dma((NLON,)),
            dma, dma,
            dma((NLAT,)), dma((NLAT,)),
        ],
        compiler_params=pltpu.CompilerParams(collective_id=0, has_side_effects=True),
    )(speed, theta, dz, dx, area, flux, tally, region, seam)


def solution(mesh):
    in_specs = (
        P(None, "lat", "lon"),
        P(None, "lat", "lon"),
        P(),
        P("lat", "lon"),
        P("lat", "lon"),
        P("lat", "lon"),
        P("lat", "lon"),
        P("lat", "lon"),
        P("lon"),
    )
    out_specs = (P(None, "lat", None), P(None, "lat", None), P(None, "lat"), P(None, "lat"))
    return jax.shard_map(body, mesh=mesh, in_specs=in_specs, out_specs=out_specs, check_vma=False)
```

```python
import math

import jax
import jax.numpy as jnp
from jax import lax
from jax.experimental import pallas as pl
from jax.experimental.pallas import tpu as pltpu
from jax.sharding import PartitionSpec as P

BINS = 128
REGIONS = 4
TIERS = 16
ROWS = 64
COLS = 256
NLON = 16
NLAT = 16
GROUP = 8
OWNED = ROWS // NLON
LO = 12
HI = 11
SIDE = REGIONS * LO

HEAT, THETA, WET, FLUX, SOUTH = 64, 68, 69, 72, 76

UNIT = math.sqrt(BINS / (COLS * NLON * TIERS))
IMPLIED = 2.0 / math.sqrt(COLS * NLON * ROWS * NLAT)
VMEM_LIMIT = 66_800_000
F32, BF16 = jnp.float32, jnp.bfloat16


def iota(shape, dim):
    return lax.broadcasted_iota(jnp.int32, shape, dim)


def two_terms(x):
    high = x.astype(BF16).astype(F32)
    return high, x - high


def kernel(
    speed_h, theta_h, dz_s, dx_h, area_h, flux_h, tally_h, region_h, seam_s,
    out_class, out_sums,
    th, sp, dx, area, flux, tally, region,
    hi_a, cl_a, val_a, part_a, hi_b, cl_b, val_b, part_b,
    rs_send, rs_recv, ag_send,
    halo_send, halo_recv, fold_send, fold_recv, pfx_send, pfx_recv,
    in_sem, rs_ssem, rs_rsem, ag_ssem, agc_rsem, ags_rsem, fold_ssem, fold_rsem,
    halo_ssem, halo_rsem, pfx_ssem, pfx_rsem,
):
    o = lax.axis_index("lon")
    l = lax.axis_index("lat")
    lane8 = iota((8, 128), 1)
    MESH = pl.DeviceIdType.MESH

    first, rest = pl.ds(0, 16), pl.ds(16, ROWS - 16)
    loads = [
        pltpu.make_async_copy(flux_h, flux, in_sem.at[0]),
        pltpu.make_async_copy(area_h, area, in_sem.at[1]),
        pltpu.make_async_copy(region_h, region, in_sem.at[2]),
        pltpu.make_async_copy(tally_h, tally.at[pl.ds(0, ROWS)], in_sem.at[3]),
        pltpu.make_async_copy(dx_h, dx, in_sem.at[4]),
        pltpu.make_async_copy(theta_h.at[:, first], th.at[:, first], in_sem.at[5]),
        pltpu.make_async_copy(speed_h.at[:, first], sp.at[:, first], in_sem.at[6]),
        pltpu.make_async_copy(theta_h.at[:, rest], th.at[:, rest], in_sem.at[7]),
        pltpu.make_async_copy(speed_h.at[:, rest], sp.at[:, rest], in_sem.at[8]),
    ]
    for load in loads:
        load.start()

    barrier = pltpu.get_barrier_semaphore()
    for d in range(1, NLON):
        pl.semaphore_signal(barrier, inc=1, device_id={"lon": lax.rem(o + d, NLON)}, device_id_type=MESH)
    for d in range(1, NLAT):
        pl.semaphore_signal(barrier, inc=1, device_id={"lat": lax.rem(l + d, NLAT)}, device_id_type=MESH)

    def halo_copy():
        return pltpu.make_async_remote_copy(
            halo_send, halo_recv, halo_ssem, halo_rsem, device_id={"lat": lax.max(l - 1, 0)}, device_id_type=MESH)

    def fold_copy(dst, src):
        return pltpu.make_async_remote_copy(
            fold_send, fold_recv.at[src], fold_ssem.at[dst], fold_rsem.at[src],
            device_id={"lon": dst}, device_id_type=MESH)

    def pfx_copy(dst, src):
        return pltpu.make_async_remote_copy(
            pfx_send, pfx_recv.at[src], pfx_ssem.at[dst], pfx_rsem.at[src],
            device_id={"lat": dst}, device_id_type=MESH)

    def owner(g, t):
        if t < REGIONS:
            return 4 * t + lax.rem(g, 4), lax.div(g, 4)
        return 4 * lax.div(g, 2) + lax.rem(g + 1, 4), 2

    def rs_copy(g, t, src):
        dst, slot = owner(g, t)
        return pltpu.make_async_remote_copy(
            rs_send.at[g, t], rs_recv.at[slot, src], rs_ssem.at[g, t], rs_rsem.at[slot, src],
            device_id={"lon": dst}, device_id_type=MESH)

    def class_copy(slot, b, g, dst):
        return pltpu.make_async_remote_copy(
            ag_send.at[slot], out_class.at[b, pl.ds(pl.multiple_of(8 * g, 8), 8)],
            ag_ssem.at[slot, dst], agc_rsem.at[b, g], device_id={"lon": dst}, device_id_type=MESH)

    def sums_copy(g, dst):
        return pltpu.make_async_remote_copy(
            ag_send.at[2], out_sums.at[pl.ds(pl.multiple_of(8 * g, 8), 8)],
            ag_ssem.at[2, dst], ags_rsem.at[g], device_id={"lon": dst}, device_id_type=MESH)

    def others(count, me, act):
        def step(q, c):
            @pl.when(q != me)
            def _():
                act(q)
            return c
        lax.fori_loop(0, count, step, 0)

    def flux_totals():
        acc = [jnp.zeros((8, COLS), F32) for _ in range(REGIONS)]
        for g in range(ROWS // 8):
            rows = slice(8 * g, 8 * g + 8)
            f = flux[rows, :] * area[rows, :]
            reg = region[rows, :]
            for b in range(REGIONS):
                acc[b] = acc[b] + jnp.where(reg == b, f, 0.0)
        totals = jnp.zeros((8, 128), F32)
        for b in range(REGIONS):
            t = jnp.sum(jnp.sum(acc[b], axis=0, keepdims=True), axis=1, keepdims=True)
            totals = jnp.where(lane8 == SOUTH + b, t, totals)
        pfx_send[...] = totals

    def edge_rows():
        for k in range(TIERS):
            halo_send[k : k + 1, :] = th[k, 0:1, :]
            fold_send[k : k + 1, :] = th[k, ROWS - 1 : ROWS, :]
        halo_send[TIERS:24, :] = jnp.broadcast_to(tally[0:1, :].astype(F32), (8, COLS))
        fold_send[TIERS:24, :] = jnp.broadcast_to(tally[ROWS - 1 : ROWS, :].astype(F32), (8, COLS))

    def first_sends():
        pl.semaphore_wait(barrier, NLON - 1 + NLAT - 1)

        @pl.when(l == NLAT - 1)
        def _():
            others(NLON, o, lambda q: fold_copy(q, o).start())
            fold_recv[o] = fold_send[...]

        @pl.when(l > 0)
        def _():
            halo_copy().start()

        def north(q, c):
            @pl.when(q > l)
            def _():
                pfx_copy(q, l).start()
            return c
        lax.fori_loop(0, NLAT, north, 0)

    def north_row():
        @pl.when(l < NLAT - 1)
        def _():
            halo_copy().wait_recv()

        @pl.when(l == NLAT - 1)
        def _():
            others(NLON, o, lambda q: fold_copy(o, q).wait_recv())
            first = seam_s[0]
            source = lax.shift_right_logical(first, 8)
            at = jnp.bitwise_and(first, COLS - 1)
            high = fold_recv[source]
            low = fold_recv[jnp.bitwise_and(source + NLON - 1, NLON - 1)]
            for t in range(COLS // 128):
                i = lane8 + 128 * t
                spot = jnp.bitwise_and(at - i, COLS - 1)
                lane = jnp.bitwise_and(spot, 127)
                for r in range(3):
                    rows = slice(8 * r, 8 * r + 8)
                    pick = [
                        jnp.where(
                            spot >= 128,
                            jnp.take_along_axis(src[rows, 128:], lane, axis=1),
                            jnp.take_along_axis(src[rows, :128], lane, axis=1),
                        )
                        for src in (high, low)
                    ]
                    halo_recv[rows, 128 * t : 128 * t + 128] = jnp.where(i <= at, pick[0], pick[1])

        for k in range(TIERS):
            th[k, ROWS : ROWS + 1, :] = halo_recv[k : k + 1, :]
        tally[ROWS : ROWS + 1, :] = halo_recv[TIERS : TIERS + 1, :].astype(jnp.int32)

        def south(q, c):
            @pl.when(q < l)
            def _():
                pfx_copy(l, q).wait_recv()
            return c
        lax.fori_loop(0, NLAT, south, 0)

    sub8 = iota((8, COLS), 0)
    hi_iota = lax.shift_right_logical(iota((SIDE, COLS), 0), 2).astype(F32).astype(BF16)
    cl_iota = iota((SIDE, COLS), 0).astype(F32).astype(BF16)
    zero = jnp.zeros((SIDE, COLS), BF16)
    one = jnp.ones((SIDE, COLS), BF16)

    def prepare(g, hi_r, cl_r, val_r, south=None):
        base = g * GROUP if isinstance(g, int) else pl.multiple_of(g * GROUP, GROUP)
        here = pl.ds(base, GROUP)
        nxt = pl.ds(base + GROUP, 1)
        deep = tally[here, :]
        face_depth = jnp.minimum(deep, jnp.where(sub8 == 7, tally[nxt, :], pltpu.roll(deep, 7, 0)))
        width = dx[here, :]
        reg = region[here, :]
        regf = reg.astype(F32) * LO
        member = [reg == b for b in range(REGIONS)]
        heat = theta_sum = wet_sum = jnp.zeros((8, COLS), F32)
        stats = jnp.zeros((8, 128), F32)
        for k in range(TIERS):
            t = th[k, here, :]
            face = 0.5 * (t + jnp.where(sub8 == 7, th[k, nxt, :], pltpu.roll(t, 7, 0)))
            vol = jnp.where(face_depth > k, dz_s[k] * width, 0.0)
            mass = vol * sp[k, here, :]
            pos = jnp.clip((face - (-2.0)) * (BINS / 32.0), 0.0, BINS - 1.0)
            low = jnp.minimum(jnp.floor(pos), BINS - 2.0)
            hi = jnp.floor((low + 0.5) * (1.0 / LO))
            hi_r[k] = hi
            cl_r[k] = (low - hi * LO) + regf
            for n, x in enumerate(two_terms(mass) + two_terms(mass * (pos - low))):
                for half in range(2):
                    val_r[k, half, pl.ds(n, 8, stride=8), :] = x[:, 128 * half : 128 * half + 128]
                    val_r[k, half, pl.ds(n + 4, 8, stride=8), :] = x[:, 128 * half : 128 * half + 128]
            heat = heat + mass * face
            theta_sum = theta_sum + vol * face
            wet_sum = wet_sum + vol
            for b in range(REGIONS):
                red = jnp.sum(jnp.where(member[b], mass, 0.0), axis=1, keepdims=True)
                stats = jnp.where(lane8 == b * TIERS + k, red, stats)
            yield
        f = flux[here, :] * area[here, :]
        for b in range(REGIONS):
            red = jnp.sum(jnp.where(member[b], heat, 0.0), axis=1, keepdims=True)
            stats = jnp.where(lane8 == HEAT + b, red, stats)
            red = jnp.sum(jnp.where(member[b], f, 0.0), axis=1, keepdims=True)
            stats = jnp.where(lane8 == FLUX + b, red, stats)
        stats = jnp.where(lane8 == THETA, jnp.sum(theta_sum, axis=1, keepdims=True), stats)
        stats = jnp.where(lane8 == WET, jnp.sum(wet_sum, axis=1, keepdims=True), stats)
        if south is not None:
            stats = stats + south
        rs_send[g, REGIONS] = stats
        yield

    def bin_rows(hi_r, cl_r, val_r, part_r):
        for jj in range(GROUP):
            total = None
            for k in range(TIERS):
                hi = jnp.broadcast_to(hi_r[k, jj : jj + 1, :], (SIDE, COLS)).astype(BF16)
                cl = jnp.broadcast_to(cl_r[k, jj : jj + 1, :], (SIDE, COLS)).astype(BF16)
                val = jnp.concatenate([val_r[k, half, 8 * jj : 8 * jj + 8, :] for half in range(2)], axis=1)
                val = jnp.concatenate([val] * (SIDE // 8), axis=0).astype(BF16)
                lhs = jnp.where(hi == hi_iota, val, zero)
                rhs = jnp.where(cl == cl_iota, one, zero)
                d = lax.dot_general(lhs, rhs, (((1,), (1,)), ((), ())), preferred_element_type=F32)
                total = d if total is None else total + d
            part_r[pl.ds(jj, SIDE, stride=8), 0:SIDE] = total
            yield

    bin_lane = lax.rem(lane8, LO)
    bin_block = lax.div(lane8, LO)

    def arrange(g, part_r):
        s0 = [jnp.zeros((8, 128), F32)] * REGIONS
        s1 = [jnp.zeros((8, 128), F32)] * REGIONS
        for hi in range(HI):
            rows = [part_r[32 * hi + 8 * n : 32 * hi + 8 * n + 8, :] for n in range(4)]
            wx = rows[2] + rows[3]
            x = rows[0] + rows[1] - wx
            for b in range(REGIONS):
                at = bin_lane + LO * b
                s0[b] = jnp.where(bin_block == hi, jnp.take_along_axis(x, at, axis=1), s0[b])
                s1[b] = jnp.where(bin_block == hi, jnp.take_along_axis(wx, at, axis=1), s1[b])
            yield
        for b in range(REGIONS):
            rs_send[g, b] = s0[b] + jnp.where(lane8 == 0, 0.0, pltpu.roll(s1[b], 1, 1))
        yield

    def together(*parts):
        parts = [p for p in parts if p is not None]
        done = object()
        lead, rest = parts[0], parts[1:]
        per = [2] * len(rest)
        while next(lead, done) is not done:
            for p, n in zip(rest, per):
                for _ in range(n):
                    next(p, done)
        for p in rest:
            while next(p, done) is not done:
                pass

    def send(g):
        for t in range(REGIONS + 1):
            dst, slot = owner(g, t)

            @pl.when(dst != o)
            def _():
                rs_copy(g, t, o).start()

    set_a = (hi_a, cl_a, val_a)
    set_b = (hi_b, cl_b, val_b)

    for load in loads[:3]:
        load.wait()
    flux_totals()
    for load in loads[3:7]:
        load.wait()
    together(prepare(0, *set_a))
    for load in loads[7:]:
        load.wait()
    edge_rows()

    def pair(i, carry):
        g = 2 * i
        together(bin_rows(*set_a, part_a), prepare(g + 1, *set_b), arrange(lax.max(g - 1, 0), part_b))

        @pl.when(i == 0)
        def _():
            first_sends()

        @pl.when(i > 0)
        def _():
            send(g - 1)
        together(bin_rows(*set_b, part_b), prepare(g + 2, *set_a), arrange(g, part_a))
        send(g)
        return carry

    lax.fori_loop(0, 3, pair, 0)
    together(bin_rows(*set_a, part_a), arrange(5, part_b))
    send(5)
    north_row()

    def add_south(q, c):
        return c + jnp.where(q < l, pfx_recv[q], 0.0)

    south = lax.fori_loop(0, NLAT, add_south, jnp.zeros((8, 128), F32))
    together(prepare(7, *set_b, south))
    together(bin_rows(*set_b, part_b), arrange(6, part_a))
    send(6)
    together(arrange(7, part_b))
    send(7)

    b_own, g_low = lax.div(o, 4), lax.rem(o, 4)

    def owned(slot, g, t, scale):
        others(NLON, o, lambda q: pltpu.make_async_remote_copy(
            rs_send.at[0, 0], rs_recv.at[slot, q], rs_ssem.at[0, 0], rs_rsem.at[slot, q],
            device_id={"lon": q}, device_id_type=MESH).wait_recv())
        acc = rs_send[g, t]
        for q in range(NLON):
            acc = acc + jnp.where(q != o, rs_recv[slot, q], 0.0)
        ag_send[slot] = acc * scale

    for slot in (0, 1):
        g = 4 * slot + g_low
        owned(slot, g, b_own, UNIT)
        others(NLON, o, lambda q: class_copy(slot, b_own, g, q).start())
        out_class[b_own, pl.ds(pl.multiple_of(8 * g, 8), 8), :] = ag_send[slot]
    odd = jnp.bitwise_and(o - 2 * b_own - 1, 3)
    g_sum = 2 * b_own + odd

    @pl.when(odd < 2)
    def _():
        owned(2, g_sum, REGIONS, 1.0)
        others(NLON, o, lambda q: sums_copy(g_sum, q).start())
        out_sums[pl.ds(pl.multiple_of(8 * g_sum, 8), 8), :] = ag_send[2]

    for g in range(ROWS // 8):
        for t in range(REGIONS + 1):
            dst, slot = owner(jnp.int32(g), t)

            @pl.when(dst != o)
            def _():
                (class_copy(0, t, g, 0) if t < REGIONS else sums_copy(g, 0)).wait_recv()

    for g in range(ROWS // 8):
        for t in range(REGIONS + 1):
            dst, slot = owner(jnp.int32(g), t)

            @pl.when(dst != o)
            def _():
                rs_copy(g, t, o).wait_send()
    for slot in (0, 1):
        others(NLON, o, lambda q: class_copy(slot, b_own, 4 * slot + g_low, q).wait_send())

    @pl.when(odd < 2)
    def _():
        others(NLON, o, lambda q: sums_copy(g_sum, q).wait_send())

    @pl.when(l > 0)
    def _():
        halo_copy().wait_send()

    @pl.when(l == NLAT - 1)
    def _():
        others(NLON, o, lambda q: fold_copy(q, o).wait_send())

    def north_done(q, c):
        @pl.when(q > l)
        def _():
            pfx_copy(q, l).wait_send()
        return c
    lax.fori_loop(0, NLAT, north_done, 0)


def finish(classes, sums, out_class, out_over, out_heat, out_impl, square):
    out_class[...] = classes[...]
    square[0:ROWS, :] = sums[...]
    square[ROWS:128, :] = jnp.zeros((128 - ROWS, 128), F32)
    flipped = jnp.transpose(square[...])
    lane8 = iota((8, 128), 1)
    sub = iota((TIERS, 128), 0)
    mean = flipped[THETA : THETA + 1, :] / jnp.where(iota((1, 128), 1) < ROWS, flipped[WET : WET + 1, :], 1.0)
    for b in range(REGIONS):
        x = flipped[TIERS * b : TIERS * b + TIERS, :]
        vol = jnp.sum(x, axis=0, keepdims=True)
        res = (UNIT / 16.0) * (flipped[HEAT + b : HEAT + b + 1, :] - vol * mean)
        out_heat[b : b + 1, :] = res[:, 0:ROWS]
        for step in (1, 2, 4, 8):
            x = x + jnp.where(sub >= step, pltpu.roll(x, step, 0), 0.0)
        out_over[b] = (UNIT * x)[:, 0:ROWS]
    c = flipped[FLUX : FLUX + 8, :]
    south = jnp.sum(jnp.where(lane8 == ROWS - 1, c, 0.0), axis=1, keepdims=True)
    for step in (1, 2, 4, 8, 16, 32):
        c = c + jnp.where(lane8 >= step, pltpu.roll(c, step, 1), 0.0)
    out_impl[...] = (IMPLIED * (c[0:4] + south[4:8]))[:, 0:ROWS]


def body(speed, theta, dz, dx, area, flux, tally, region, seam):
    any_ = pl.BlockSpec(memory_space=pltpu.HBM)
    smem = pl.BlockSpec(memory_space=pltpu.SMEM)
    vmem = pl.BlockSpec(memory_space=pltpu.VMEM)
    dma = pltpu.SemaphoreType.DMA
    rows = [pltpu.VMEM((TIERS, GROUP, COLS), F32)] * 2
    sets = (rows + [pltpu.VMEM((TIERS, 2, 8 * GROUP, 128), F32), pltpu.VMEM((8 * SIDE, 128), F32)]) * 2
    classes, sums = pl.pallas_call(
        kernel,
        out_shape=(
            jax.ShapeDtypeStruct((REGIONS, ROWS, BINS), F32),
            jax.ShapeDtypeStruct((ROWS, 128), F32),
        ),
        in_specs=[any_, any_, smem, any_, any_, any_, any_, any_, smem],
        out_specs=(vmem, vmem),
        scratch_shapes=[
            pltpu.VMEM((TIERS, ROWS + 8, COLS), F32),
            pltpu.VMEM((TIERS, ROWS, COLS), F32),
            pltpu.VMEM((ROWS, COLS), F32),
            pltpu.VMEM((ROWS, COLS), F32),
            pltpu.VMEM((ROWS, COLS), F32),
            pltpu.VMEM((ROWS + 8, COLS), jnp.int32),
            pltpu.VMEM((ROWS, COLS), jnp.int32),
            *sets,
            pltpu.VMEM((ROWS // 8, REGIONS + 1, 8, 128), F32),
            pltpu.VMEM((3, NLON, 8, 128), F32),
            pltpu.VMEM((3, 8, 128), F32),
            pltpu.VMEM((24, COLS), F32),
            pltpu.VMEM((24, COLS), F32),
            pltpu.VMEM((24, COLS), F32),
            pltpu.VMEM((NLON, 24, COLS), F32),
            pltpu.VMEM((8, 128), F32),
            pltpu.VMEM((NLAT, 8, 128), F32),
            dma((9,)),
            dma((ROWS // 8, REGIONS + 1)), dma((3, NLON)), dma((3, NLON)),
            dma((REGIONS, ROWS // 8)), dma((ROWS // 8,)),
            dma((NLON,)), dma((NLON,)),
            dma, dma,
            dma((NLAT,)), dma((NLAT,)),
        ],
        compiler_params=pltpu.CompilerParams(collective_id=0, has_side_effects=True, vmem_limit_bytes=VMEM_LIMIT),
    )(speed, theta, dz, dx, area, flux, tally, region, seam)
    out_class, over, heat, impl = pl.pallas_call(
        finish,
        out_shape=(
            jax.ShapeDtypeStruct((REGIONS, ROWS, BINS), F32),
            jax.ShapeDtypeStruct((REGIONS, TIERS, ROWS), F32),
            jax.ShapeDtypeStruct((REGIONS, ROWS), F32),
            jax.ShapeDtypeStruct((REGIONS, ROWS), F32),
        ),
        in_specs=[vmem, vmem],
        out_specs=(vmem,) * 4,
        scratch_shapes=[pltpu.VMEM((128, 128), F32)],
        compiler_params=pltpu.CompilerParams(vmem_limit_bytes=4 * 2**20),
    )(classes, sums)
    return out_class, jnp.transpose(over, (0, 2, 1)), heat, impl


def solution(mesh):
    in_specs = (
        P(None, "lat", "lon"),
        P(None, "lat", "lon"),
        P(),
        P("lat", "lon"),
        P("lat", "lon"),
        P("lat", "lon"),
        P("lat", "lon"),
        P("lat", "lon"),
        P("lon"),
    )
    out_specs = (P(None, "lat", None), P(None, "lat", None), P(None, "lat"), P(None, "lat"))
    return jax.shard_map(body, mesh=mesh, in_specs=in_specs, out_specs=out_specs, check_vma=False)
```

```python
import math

import jax
import jax.numpy as jnp
from jax import lax
from jax.experimental import pallas as pl
from jax.experimental.pallas import tpu as pltpu
from jax.sharding import PartitionSpec as P

BINS = 128
REGIONS = 4
TIERS = 16
ROWS = 64
COLS = 256
NLON = 16
NLAT = 16
GROUP = 8
OWNED = ROWS // NLON
LO = 12
HI = 11
SIDE = REGIONS * LO

HEAT, THETA, WET, FLUX, SOUTH = 64, 68, 69, 72, 76

UNIT = math.sqrt(BINS / (COLS * NLON * TIERS))
IMPLIED = 2.0 / math.sqrt(COLS * NLON * ROWS * NLAT)
VMEM_LIMIT = 32 * 2**20
F32, BF16 = jnp.float32, jnp.bfloat16


def iota(shape, dim):
    return lax.broadcasted_iota(jnp.int32, shape, dim)


def two_terms(x):
    high = x.astype(BF16).astype(F32)
    return high, x - high


def kernel(
    speed_h, theta_h, dz_h, dx_h, area_h, flux_h, tally_h, region_h, seam_h,
    out_class, out_sums,
    th, sp, dx, area, flux, tally, region, dz_s, seam_s,
    hi_a, cl_a, val_a, part_a, hi_b, cl_b, val_b, part_b,
    rs_send, rs_recv, ag_send,
    halo_send, halo_recv, fold_send, fold_recv, pfx_send, pfx_recv,
    in_sem, rs_ssem, rs_rsem, ag_ssem, agc_rsem, ags_rsem, fold_ssem, fold_rsem,
    halo_ssem, halo_rsem, pfx_ssem, pfx_rsem,
):
    o = lax.axis_index("lon")
    l = lax.axis_index("lat")
    lane8 = iota((8, 128), 1)
    MESH = pl.DeviceIdType.MESH

    first, rest = pl.ds(0, 16), pl.ds(16, ROWS - 16)
    loads = [
        pltpu.make_async_copy(flux_h, flux, in_sem.at[0]),
        pltpu.make_async_copy(area_h, area, in_sem.at[1]),
        pltpu.make_async_copy(region_h, region, in_sem.at[2]),
        pltpu.make_async_copy(tally_h, tally.at[pl.ds(0, ROWS)], in_sem.at[3]),
        pltpu.make_async_copy(dx_h, dx, in_sem.at[4]),
        pltpu.make_async_copy(dz_h, dz_s, in_sem.at[9]),
        pltpu.make_async_copy(theta_h.at[:, first], th.at[:, first], in_sem.at[5]),
        pltpu.make_async_copy(speed_h.at[:, first], sp.at[:, first], in_sem.at[6]),
        pltpu.make_async_copy(theta_h.at[:, rest], th.at[:, rest], in_sem.at[7]),
        pltpu.make_async_copy(speed_h.at[:, rest], sp.at[:, rest], in_sem.at[8]),
        pltpu.make_async_copy(seam_h, seam_s, in_sem.at[10]),
    ]
    for load in loads:
        load.start()

    barrier = pltpu.get_barrier_semaphore()
    for d in range(1, NLON):
        pl.semaphore_signal(barrier, inc=1, device_id={"lon": lax.rem(o + d, NLON)}, device_id_type=MESH)
    for d in range(1, NLAT):
        pl.semaphore_signal(barrier, inc=1, device_id={"lat": lax.rem(l + d, NLAT)}, device_id_type=MESH)

    def halo_copy():
        return pltpu.make_async_remote_copy(
            halo_send, halo_recv, halo_ssem, halo_rsem, device_id={"lat": lax.max(l - 1, 0)}, device_id_type=MESH)

    def fold_copy(dst, src):
        return pltpu.make_async_remote_copy(
            fold_send, fold_recv.at[src], fold_ssem.at[dst], fold_rsem.at[src],
            device_id={"lon": dst}, device_id_type=MESH)

    def pfx_copy(dst, src):
        return pltpu.make_async_remote_copy(
            pfx_send, pfx_recv.at[src], pfx_ssem.at[dst], pfx_rsem.at[src],
            device_id={"lat": dst}, device_id_type=MESH)

    def owner(g, t):
        if t < REGIONS:
            return 4 * t + lax.rem(g, 4), lax.div(g, 4)
        return 4 * lax.div(g, 2) + lax.rem(g + 1, 4), 2

    def rs_copy(g, t, src):
        dst, slot = owner(g, t)
        return pltpu.make_async_remote_copy(
            rs_send.at[g, t], rs_recv.at[slot, src], rs_ssem.at[g, t], rs_rsem.at[slot, src],
            device_id={"lon": dst}, device_id_type=MESH)

    def class_copy(slot, b, g, dst):
        return pltpu.make_async_remote_copy(
            ag_send.at[slot], out_class.at[b, pl.ds(pl.multiple_of(8 * g, 8), 8)],
            ag_ssem.at[slot, dst], agc_rsem.at[b, g], device_id={"lon": dst}, device_id_type=MESH)

    def sums_copy(g, dst):
        return pltpu.make_async_remote_copy(
            ag_send.at[2], out_sums.at[pl.ds(pl.multiple_of(8 * g, 8), 8)],
            ag_ssem.at[2, dst], ags_rsem.at[g], device_id={"lon": dst}, device_id_type=MESH)

    def others(count, me, act):
        def step(q, c):
            @pl.when(q != me)
            def _():
                act(q)
            return c
        lax.fori_loop(0, count, step, 0)

    def flux_totals():
        acc = [jnp.zeros((8, COLS), F32) for _ in range(REGIONS)]
        for g in range(ROWS // 8):
            rows = slice(8 * g, 8 * g + 8)
            f = flux[rows, :] * area[rows, :]
            reg = region[rows, :]
            for b in range(REGIONS):
                acc[b] = acc[b] + jnp.where(reg == b, f, 0.0)
        totals = jnp.zeros((8, 128), F32)
        for b in range(REGIONS):
            t = jnp.sum(jnp.sum(acc[b], axis=0, keepdims=True), axis=1, keepdims=True)
            totals = jnp.where(lane8 == SOUTH + b, t, totals)
        pfx_send[...] = totals

    def edge_rows():
        for k in range(TIERS):
            halo_send[k : k + 1, :] = th[k, 0:1, :]
            fold_send[k : k + 1, :] = th[k, ROWS - 1 : ROWS, :]
        halo_send[TIERS:24, :] = jnp.broadcast_to(tally[0:1, :].astype(F32), (8, COLS))
        fold_send[TIERS:24, :] = jnp.broadcast_to(tally[ROWS - 1 : ROWS, :].astype(F32), (8, COLS))

    def first_sends():
        pl.semaphore_wait(barrier, NLON - 1 + NLAT - 1)

        @pl.when(l == NLAT - 1)
        def _():
            others(NLON, o, lambda q: fold_copy(q, o).start())
            fold_recv[o] = fold_send[...]

        @pl.when(l > 0)
        def _():
            halo_copy().start()

        def north(q, c):
            @pl.when(q > l)
            def _():
                pfx_copy(q, l).start()
            return c
        lax.fori_loop(0, NLAT, north, 0)

    def north_row():
        @pl.when(l < NLAT - 1)
        def _():
            halo_copy().wait_recv()

        @pl.when(l == NLAT - 1)
        def _():
            others(NLON, o, lambda q: fold_copy(o, q).wait_recv())
            first = seam_s[0]
            source = lax.shift_right_logical(first, 8)
            at = jnp.bitwise_and(first, COLS - 1)
            high = fold_recv[source]
            low = fold_recv[jnp.bitwise_and(source + NLON - 1, NLON - 1)]
            for t in range(COLS // 128):
                i = lane8 + 128 * t
                spot = jnp.bitwise_and(at - i, COLS - 1)
                lane = jnp.bitwise_and(spot, 127)
                for r in range(3):
                    rows = slice(8 * r, 8 * r + 8)
                    pick = [
                        jnp.where(
                            spot >= 128,
                            jnp.take_along_axis(src[rows, 128:], lane, axis=1),
                            jnp.take_along_axis(src[rows, :128], lane, axis=1),
                        )
                        for src in (high, low)
                    ]
                    halo_recv[rows, 128 * t : 128 * t + 128] = jnp.where(i <= at, pick[0], pick[1])

        for k in range(TIERS):
            th[k, ROWS : ROWS + 1, :] = halo_recv[k : k + 1, :]
        tally[ROWS : ROWS + 1, :] = halo_recv[TIERS : TIERS + 1, :].astype(jnp.int32)

        def south(q, c):
            @pl.when(q < l)
            def _():
                pfx_copy(l, q).wait_recv()
            return c
        lax.fori_loop(0, NLAT, south, 0)

    sub8 = iota((8, COLS), 0)
    hi_iota = lax.shift_right_logical(iota((SIDE, COLS), 0), 2).astype(F32).astype(BF16)
    cl_iota = iota((SIDE, COLS), 0).astype(F32).astype(BF16)
    zero = jnp.zeros((SIDE, COLS), BF16)
    one = jnp.ones((SIDE, COLS), BF16)

    def prepare(g, hi_r, cl_r, val_r, south=None):
        base = g * GROUP if isinstance(g, int) else pl.multiple_of(g * GROUP, GROUP)
        here = pl.ds(base, GROUP)
        nxt = pl.ds(base + GROUP, 1)
        deep = tally[here, :]
        face_depth = jnp.minimum(deep, jnp.where(sub8 == 7, tally[nxt, :], pltpu.roll(deep, 7, 0)))
        width = dx[here, :]
        reg = region[here, :]
        regf = reg.astype(F32) * LO
        member = [reg == b for b in range(REGIONS)]
        heat = theta_sum = wet_sum = jnp.zeros((8, COLS), F32)
        stats = jnp.zeros((8, 128), F32)
        for k in range(TIERS):
            t = th[k, here, :]
            face = 0.5 * (t + jnp.where(sub8 == 7, th[k, nxt, :], pltpu.roll(t, 7, 0)))
            vol = jnp.where(face_depth > k, dz_s[k] * width, 0.0)
            mass = vol * sp[k, here, :]
            pos = jnp.clip((face - (-2.0)) * (BINS / 32.0), 0.0, BINS - 1.0)
            low = jnp.minimum(jnp.floor(pos), BINS - 2.0)
            hi = jnp.floor((low + 0.5) * (1.0 / LO))
            hi_r[k] = hi
            cl_r[k] = (low - hi * LO) + regf
            for n, x in enumerate(two_terms(mass) + two_terms(mass * (pos - low))):
                for half in range(2):
                    val_r[k, half, pl.ds(n, 8, stride=8), :] = x[:, 128 * half : 128 * half + 128]
                    val_r[k, half, pl.ds(n + 4, 8, stride=8), :] = x[:, 128 * half : 128 * half + 128]
            heat = heat + mass * face
            theta_sum = theta_sum + vol * face
            wet_sum = wet_sum + vol
            for b in range(REGIONS):
                red = jnp.sum(jnp.where(member[b], mass, 0.0), axis=1, keepdims=True)
                stats = jnp.where(lane8 == b * TIERS + k, red, stats)
            yield
        f = flux[here, :] * area[here, :]
        for b in range(REGIONS):
            red = jnp.sum(jnp.where(member[b], heat, 0.0), axis=1, keepdims=True)
            stats = jnp.where(lane8 == HEAT + b, red, stats)
            red = jnp.sum(jnp.where(member[b], f, 0.0), axis=1, keepdims=True)
            stats = jnp.where(lane8 == FLUX + b, red, stats)
        stats = jnp.where(lane8 == THETA, jnp.sum(theta_sum, axis=1, keepdims=True), stats)
        stats = jnp.where(lane8 == WET, jnp.sum(wet_sum, axis=1, keepdims=True), stats)
        if south is not None:
            stats = stats + south
        rs_send[g, REGIONS] = stats
        yield

    def bin_rows(hi_r, cl_r, val_r, part_r):
        for jj in range(GROUP):
            total = None
            for k in range(TIERS):
                hi = jnp.broadcast_to(hi_r[k, jj : jj + 1, :], (SIDE, COLS)).astype(BF16)
                cl = jnp.broadcast_to(cl_r[k, jj : jj + 1, :], (SIDE, COLS)).astype(BF16)
                val = jnp.concatenate([val_r[k, half, 8 * jj : 8 * jj + 8, :] for half in range(2)], axis=1)
                val = jnp.concatenate([val] * (SIDE // 8), axis=0).astype(BF16)
                lhs = jnp.where(hi == hi_iota, val, zero)
                rhs = jnp.where(cl == cl_iota, one, zero)
                d = lax.dot_general(lhs, rhs, (((1,), (1,)), ((), ())), preferred_element_type=F32)
                total = d if total is None else total + d
            part_r[pl.ds(jj, SIDE, stride=8), 0:SIDE] = total
            yield

    bin_lane = lax.rem(lane8, LO)
    bin_block = lax.div(lane8, LO)

    def arrange(g, part_r):
        s0 = [jnp.zeros((8, 128), F32)] * REGIONS
        s1 = [jnp.zeros((8, 128), F32)] * REGIONS
        for hi in range(HI):
            rows = [part_r[32 * hi + 8 * n : 32 * hi + 8 * n + 8, :] for n in range(4)]
            wx = rows[2] + rows[3]
            x = rows[0] + rows[1] - wx
            for b in range(REGIONS):
                at = bin_lane + LO * b
                s0[b] = jnp.where(bin_block == hi, jnp.take_along_axis(x, at, axis=1), s0[b])
                s1[b] = jnp.where(bin_block == hi, jnp.take_along_axis(wx, at, axis=1), s1[b])
            yield
        for b in range(REGIONS):
            rs_send[g, b] = s0[b] + jnp.where(lane8 == 0, 0.0, pltpu.roll(s1[b], 1, 1))
        yield

    def together(*parts):
        parts = [p for p in parts if p is not None]
        done = object()
        lead, rest = parts[0], parts[1:]
        per = [2] * len(rest)
        while next(lead, done) is not done:
            for p, n in zip(rest, per):
                for _ in range(n):
                    next(p, done)
        for p in rest:
            while next(p, done) is not done:
                pass

    def send(g):
        for t in range(REGIONS + 1):
            dst, slot = owner(g, t)

            @pl.when(dst != o)
            def _():
                rs_copy(g, t, o).start()

    set_a = (hi_a, cl_a, val_a)
    set_b = (hi_b, cl_b, val_b)

    for load in loads[:3]:
        load.wait()
    flux_totals()
    for load in loads[3:8]:
        load.wait()
    together(prepare(0, *set_a))
    for load in loads[8:]:
        load.wait()
    edge_rows()

    def pair(i, carry):
        g = 2 * i
        together(bin_rows(*set_a, part_a), prepare(g + 1, *set_b), arrange(lax.max(g - 1, 0), part_b))

        @pl.when(i == 0)
        def _():
            first_sends()

        @pl.when(i > 0)
        def _():
            send(g - 1)
        together(bin_rows(*set_b, part_b), prepare(g + 2, *set_a), arrange(g, part_a))
        send(g)
        return carry

    lax.fori_loop(0, 3, pair, 0)
    together(bin_rows(*set_a, part_a), arrange(5, part_b))
    send(5)
    north_row()

    def add_south(q, c):
        return c + jnp.where(q < l, pfx_recv[q], 0.0)

    south = lax.fori_loop(0, NLAT, add_south, jnp.zeros((8, 128), F32))
    together(prepare(7, *set_b, south))
    together(bin_rows(*set_b, part_b), arrange(6, part_a))
    send(6)
    together(arrange(7, part_b))
    send(7)

    b_own, g_low = lax.div(o, 4), lax.rem(o, 4)

    def owned(slot, g, t, scale):
        others(NLON, o, lambda q: pltpu.make_async_remote_copy(
            rs_send.at[0, 0], rs_recv.at[slot, q], rs_ssem.at[0, 0], rs_rsem.at[slot, q],
            device_id={"lon": q}, device_id_type=MESH).wait_recv())
        acc = rs_send[g, t]
        for q in range(NLON):
            acc = acc + jnp.where(q != o, rs_recv[slot, q], 0.0)
        ag_send[slot] = acc * scale

    for slot in (0, 1):
        g = 4 * slot + g_low
        owned(slot, g, b_own, UNIT)
        others(NLON, o, lambda q: class_copy(slot, b_own, g, q).start())
        out_class[b_own, pl.ds(pl.multiple_of(8 * g, 8), 8), :] = ag_send[slot]
    odd = jnp.bitwise_and(o - 2 * b_own - 1, 3)
    g_sum = 2 * b_own + odd

    @pl.when(odd < 2)
    def _():
        owned(2, g_sum, REGIONS, 1.0)
        others(NLON, o, lambda q: sums_copy(g_sum, q).start())
        out_sums[pl.ds(pl.multiple_of(8 * g_sum, 8), 8), :] = ag_send[2]

    for g in range(ROWS // 8):
        for t in range(REGIONS + 1):
            dst, slot = owner(jnp.int32(g), t)

            @pl.when(dst != o)
            def _():
                (class_copy(0, t, g, 0) if t < REGIONS else sums_copy(g, 0)).wait_recv()

    for g in range(ROWS // 8):
        for t in range(REGIONS + 1):
            dst, slot = owner(jnp.int32(g), t)

            @pl.when(dst != o)
            def _():
                rs_copy(g, t, o).wait_send()
    for slot in (0, 1):
        others(NLON, o, lambda q: class_copy(slot, b_own, 4 * slot + g_low, q).wait_send())

    @pl.when(odd < 2)
    def _():
        others(NLON, o, lambda q: sums_copy(g_sum, q).wait_send())

    @pl.when(l > 0)
    def _():
        halo_copy().wait_send()

    @pl.when(l == NLAT - 1)
    def _():
        others(NLON, o, lambda q: fold_copy(q, o).wait_send())

    def north_done(q, c):
        @pl.when(q > l)
        def _():
            pfx_copy(q, l).wait_send()
        return c
    lax.fori_loop(0, NLAT, north_done, 0)


def finish(classes, sums, out_class, out_over, out_heat, out_impl, square):
    out_class[...] = classes[...]
    square[0:ROWS, :] = sums[...]
    square[ROWS:128, :] = jnp.zeros((128 - ROWS, 128), F32)
    flipped = jnp.transpose(square[...])
    lane8 = iota((8, 128), 1)
    sub = iota((TIERS, 128), 0)
    mean = flipped[THETA : THETA + 1, :] / jnp.where(iota((1, 128), 1) < ROWS, flipped[WET : WET + 1, :], 1.0)
    for b in range(REGIONS):
        x = flipped[TIERS * b : TIERS * b + TIERS, :]
        vol = jnp.sum(x, axis=0, keepdims=True)
        res = (UNIT / 16.0) * (flipped[HEAT + b : HEAT + b + 1, :] - vol * mean)
        out_heat[b : b + 1, :] = res[:, 0:ROWS]
        for step in (1, 2, 4, 8):
            x = x + jnp.where(sub >= step, pltpu.roll(x, step, 0), 0.0)
        out_over[b] = (UNIT * x)[:, 0:ROWS]
    c = flipped[FLUX : FLUX + 8, :]
    south = jnp.sum(jnp.where(lane8 == ROWS - 1, c, 0.0), axis=1, keepdims=True)
    for step in (1, 2, 4, 8, 16, 32):
        c = c + jnp.where(lane8 >= step, pltpu.roll(c, step, 1), 0.0)
    out_impl[...] = (IMPLIED * (c[0:4] + south[4:8]))[:, 0:ROWS]


def body(speed, theta, dz, dx, area, flux, tally, region, seam):
    any_ = pl.BlockSpec(memory_space=pltpu.HBM)
    vmem = pl.BlockSpec(memory_space=pltpu.VMEM)
    dma = pltpu.SemaphoreType.DMA
    inputs = (speed, theta, dz, dx, area, flux, tally, region, seam)
    inputs = [pltpu.with_memory_space_constraint(x, pltpu.HBM) for x in inputs]
    rows = [pltpu.VMEM((TIERS, GROUP, COLS), F32)] * 2
    sets = (rows + [pltpu.VMEM((TIERS, 2, 8 * GROUP, 128), F32), pltpu.VMEM((8 * SIDE, 128), F32)]) * 2
    classes, sums = pl.pallas_call(
        kernel,
        out_shape=(
            jax.ShapeDtypeStruct((REGIONS, ROWS, BINS), F32),
            jax.ShapeDtypeStruct((ROWS, 128), F32),
        ),
        in_specs=[any_] * 9,
        out_specs=(vmem, vmem),
        scratch_shapes=[
            pltpu.VMEM((TIERS, ROWS + 8, COLS), F32),
            pltpu.VMEM((TIERS, ROWS, COLS), F32),
            pltpu.VMEM((ROWS, COLS), F32),
            pltpu.VMEM((ROWS, COLS), F32),
            pltpu.VMEM((ROWS, COLS), F32),
            pltpu.VMEM((ROWS + 8, COLS), jnp.int32),
            pltpu.VMEM((ROWS, COLS), jnp.int32),
            pltpu.SMEM((TIERS,), F32),
            pltpu.SMEM((COLS,), jnp.int32),
            *sets,
            pltpu.VMEM((ROWS // 8, REGIONS + 1, 8, 128), F32),
            pltpu.VMEM((3, NLON, 8, 128), F32),
            pltpu.VMEM((3, 8, 128), F32),
            pltpu.VMEM((24, COLS), F32),
            pltpu.VMEM((24, COLS), F32),
            pltpu.VMEM((24, COLS), F32),
            pltpu.VMEM((NLON, 24, COLS), F32),
            pltpu.VMEM((8, 128), F32),
            pltpu.VMEM((NLAT, 8, 128), F32),
            dma((11,)),
            dma((ROWS // 8, REGIONS + 1)), dma((3, NLON)), dma((3, NLON)),
            dma((REGIONS, ROWS // 8)), dma((ROWS // 8,)),
            dma((NLON,)), dma((NLON,)),
            dma, dma,
            dma((NLAT,)), dma((NLAT,)),
        ],
        compiler_params=pltpu.CompilerParams(collective_id=0, has_side_effects=True, vmem_limit_bytes=VMEM_LIMIT),
    )(*inputs)
    out_class, over, heat, impl = pl.pallas_call(
        finish,
        out_shape=(
            jax.ShapeDtypeStruct((REGIONS, ROWS, BINS), F32),
            jax.ShapeDtypeStruct((REGIONS, TIERS, ROWS), F32),
            jax.ShapeDtypeStruct((REGIONS, ROWS), F32),
            jax.ShapeDtypeStruct((REGIONS, ROWS), F32),
        ),
        in_specs=[vmem, vmem],
        out_specs=(vmem,) * 4,
        scratch_shapes=[pltpu.VMEM((128, 128), F32)],
        compiler_params=pltpu.CompilerParams(vmem_limit_bytes=4 * 2**20),
    )(classes, sums)
    return out_class, jnp.transpose(over, (0, 2, 1)), heat, impl


def solution(mesh):
    in_specs = (
        P(None, "lat", "lon"),
        P(None, "lat", "lon"),
        P(),
        P("lat", "lon"),
        P("lat", "lon"),
        P("lat", "lon"),
        P("lat", "lon"),
        P("lat", "lon"),
        P("lon"),
    )
    out_specs = (P(None, "lat", None), P(None, "lat", None), P(None, "lat"), P(None, "lat"))
    return jax.shard_map(body, mesh=mesh, in_specs=in_specs, out_specs=out_specs, check_vma=False)
```

```python
import math

import jax
import jax.numpy as jnp
from jax import lax
from jax.experimental import pallas as pl
from jax.experimental.pallas import tpu as pltpu
from jax.sharding import PartitionSpec as P

BINS = 128
REGIONS = 4
TIERS = 16
ROWS = 64
COLS = 256
NLON = 16
NLAT = 16
GROUP = 8
OWNED = ROWS // NLON
LO = 12
HI = 11
SIDE = REGIONS * LO

HEAT, THETA, WET, FLUX, SOUTH = 64, 68, 69, 72, 76

UNIT = math.sqrt(BINS / (COLS * NLON * TIERS))
IMPLIED = 2.0 / math.sqrt(COLS * NLON * ROWS * NLAT)
VMEM_LIMIT = 32 * 2**20
F32, BF16 = jnp.float32, jnp.bfloat16


def iota(shape, dim):
    return lax.broadcasted_iota(jnp.int32, shape, dim)


def two_terms(x):
    high = x.astype(BF16).astype(F32)
    return high, x - high


def kernel(
    speed_h, theta_h, dz_h, dx_h, area_h, flux_h, tally_h, region_h, seam_h,
    out_class, out_sums,
    th, sp, dx, area, flux, tally, region, dz_s, seam_s,
    hi_a, cl_a, val_a, part_a, hi_b, cl_b, val_b, part_b,
    rs_send, rs_recv, ag_send,
    halo_send, halo_recv, fold_send, fold_recv, own_flux, pair_flux, south_flux, north_flux,
    in_sem, rs_ssem, rs_rsem, ag_ssem, agc_rsem, ags_rsem, fold_ssem, fold_rsem,
    halo_ssem, halo_rsem, pair_ssem, pair_rsem, chain_ssem, chain_rsem,
):
    o = lax.axis_index("lon")
    l = lax.axis_index("lat")
    lane8 = iota((8, 128), 1)
    MESH = pl.DeviceIdType.MESH

    first, rest = pl.ds(0, 16), pl.ds(16, ROWS - 16)
    loads = [
        pltpu.make_async_copy(flux_h, flux, in_sem.at[0]),
        pltpu.make_async_copy(area_h, area, in_sem.at[1]),
        pltpu.make_async_copy(region_h, region, in_sem.at[2]),
        pltpu.make_async_copy(tally_h, tally.at[pl.ds(0, ROWS)], in_sem.at[3]),
        pltpu.make_async_copy(dx_h, dx, in_sem.at[4]),
        pltpu.make_async_copy(dz_h, dz_s, in_sem.at[9]),
        pltpu.make_async_copy(theta_h.at[:, first], th.at[:, first], in_sem.at[5]),
        pltpu.make_async_copy(speed_h.at[:, first], sp.at[:, first], in_sem.at[6]),
        pltpu.make_async_copy(theta_h.at[:, rest], th.at[:, rest], in_sem.at[7]),
        pltpu.make_async_copy(speed_h.at[:, rest], sp.at[:, rest], in_sem.at[8]),
        pltpu.make_async_copy(seam_h, seam_s, in_sem.at[10]),
    ]
    for load in loads:
        load.start()

    barrier = pltpu.get_barrier_semaphore()
    for d in range(1, NLON):
        pl.semaphore_signal(barrier, inc=1, device_id={"lon": lax.rem(o + d, NLON)}, device_id_type=MESH)
    near = (-2, -1, 1, 2)
    for d in near:
        @pl.when(jnp.logical_and(l + d >= 0, l + d < NLAT))
        def _():
            pl.semaphore_signal(barrier, inc=1, device_id={"lat": l + d}, device_id_type=MESH)

    def halo_copy():
        return pltpu.make_async_remote_copy(
            halo_send, halo_recv, halo_ssem, halo_rsem, device_id={"lat": lax.max(l - 1, 0)}, device_id_type=MESH)

    def fold_copy(dst, src):
        return pltpu.make_async_remote_copy(
            fold_send, fold_recv.at[src], fold_ssem.at[dst], fold_rsem.at[src],
            device_id={"lon": dst}, device_id_type=MESH)

    chip, core = lax.div(l, 2), lax.rem(l, 2)

    def pair_copy():
        return pltpu.make_async_remote_copy(
            own_flux, pair_flux, pair_ssem, pair_rsem, device_id={"lat": l + 1 - 2 * core}, device_id_type=MESH)

    def chain_copy():
        return pltpu.make_async_remote_copy(
            north_flux, south_flux, chain_ssem, chain_rsem,
            device_id={"lat": lax.min(l + 2, NLAT - 1)}, device_id_type=MESH)

    def chain_step():
        pair_copy().wait_recv()

        @pl.when(chip > 0)
        def _():
            chain_copy().wait_recv()

        @pl.when(chip < NLAT // 2 - 1)
        def _():
            north_flux[...] = south_flux[...] + own_flux[...] + pair_flux[...]
            chain_copy().start()

    def owner(g, t):
        if t < REGIONS:
            return 4 * t + lax.rem(g, 4), lax.div(g, 4)
        return 4 * lax.div(g, 2) + lax.rem(g + 1, 4), 2

    def rs_copy(g, t, src):
        dst, slot = owner(g, t)
        return pltpu.make_async_remote_copy(
            rs_send.at[g, t], rs_recv.at[slot, src], rs_ssem.at[g, t], rs_rsem.at[slot, src],
            device_id={"lon": dst}, device_id_type=MESH)

    def class_copy(slot, b, g, dst):
        return pltpu.make_async_remote_copy(
            ag_send.at[slot], out_class.at[b, pl.ds(pl.multiple_of(8 * g, 8), 8)],
            ag_ssem.at[slot, dst], agc_rsem.at[b, g], device_id={"lon": dst}, device_id_type=MESH)

    def sums_copy(g, dst):
        return pltpu.make_async_remote_copy(
            ag_send.at[2], out_sums.at[pl.ds(pl.multiple_of(8 * g, 8), 8)],
            ag_ssem.at[2, dst], ags_rsem.at[g], device_id={"lon": dst}, device_id_type=MESH)

    def others(count, me, act):
        def step(q, c):
            @pl.when(q != me)
            def _():
                act(q)
            return c
        lax.fori_loop(0, count, step, 0)

    def flux_totals():
        acc = [jnp.zeros((8, COLS), F32) for _ in range(REGIONS)]
        for g in range(ROWS // 8):
            rows = slice(8 * g, 8 * g + 8)
            f = flux[rows, :] * area[rows, :]
            reg = region[rows, :]
            for b in range(REGIONS):
                acc[b] = acc[b] + jnp.where(reg == b, f, 0.0)
        totals = jnp.zeros((8, 128), F32)
        for b in range(REGIONS):
            t = jnp.sum(jnp.sum(acc[b], axis=0, keepdims=True), axis=1, keepdims=True)
            totals = jnp.where(lane8 == SOUTH + b, t, totals)
        own_flux[...] = totals

        @pl.when(chip == 0)
        def _():
            south_flux[...] = jnp.zeros((8, 128), F32)

    def edge_rows():
        for k in range(TIERS):
            halo_send[k : k + 1, :] = th[k, 0:1, :]
            fold_send[k : k + 1, :] = th[k, ROWS - 1 : ROWS, :]
        halo_send[TIERS:24, :] = jnp.broadcast_to(tally[0:1, :].astype(F32), (8, COLS))
        fold_send[TIERS:24, :] = jnp.broadcast_to(tally[ROWS - 1 : ROWS, :].astype(F32), (8, COLS))

    def first_sends():
        known = NLON - 1
        for d in near:
            known = known + jnp.where(jnp.logical_and(l + d >= 0, l + d < NLAT), 1, 0)
        pl.semaphore_wait(barrier, known)
        pair_copy().start()

        @pl.when(l == NLAT - 1)
        def _():
            others(NLON, o, lambda q: fold_copy(q, o).start())
            fold_recv[o] = fold_send[...]

        @pl.when(l > 0)
        def _():
            halo_copy().start()

    def north_row():
        @pl.when(l < NLAT - 1)
        def _():
            halo_copy().wait_recv()

        @pl.when(l == NLAT - 1)
        def _():
            others(NLON, o, lambda q: fold_copy(o, q).wait_recv())
            first = seam_s[0]
            source = lax.shift_right_logical(first, 8)
            at = jnp.bitwise_and(first, COLS - 1)
            high = fold_recv[source]
            low = fold_recv[jnp.bitwise_and(source + NLON - 1, NLON - 1)]
            for t in range(COLS // 128):
                i = lane8 + 128 * t
                spot = jnp.bitwise_and(at - i, COLS - 1)
                lane = jnp.bitwise_and(spot, 127)
                for r in range(3):
                    rows = slice(8 * r, 8 * r + 8)
                    pick = [
                        jnp.where(
                            spot >= 128,
                            jnp.take_along_axis(src[rows, 128:], lane, axis=1),
                            jnp.take_along_axis(src[rows, :128], lane, axis=1),
                        )
                        for src in (high, low)
                    ]
                    halo_recv[rows, 128 * t : 128 * t + 128] = jnp.where(i <= at, pick[0], pick[1])

        for k in range(TIERS):
            th[k, ROWS : ROWS + 1, :] = halo_recv[k : k + 1, :]
        tally[ROWS : ROWS + 1, :] = halo_recv[TIERS : TIERS + 1, :].astype(jnp.int32)

    sub8 = iota((8, COLS), 0)
    hi_iota = lax.shift_right_logical(iota((SIDE, COLS), 0), 2).astype(F32).astype(BF16)
    cl_iota = iota((SIDE, COLS), 0).astype(F32).astype(BF16)
    zero = jnp.zeros((SIDE, COLS), BF16)
    one = jnp.ones((SIDE, COLS), BF16)

    def prepare(g, hi_r, cl_r, val_r):
        base = g * GROUP if isinstance(g, int) else pl.multiple_of(g * GROUP, GROUP)
        here = pl.ds(base, GROUP)
        nxt = pl.ds(base + GROUP, 1)
        deep = tally[here, :]
        face_depth = jnp.minimum(deep, jnp.where(sub8 == 7, tally[nxt, :], pltpu.roll(deep, 7, 0)))
        width = dx[here, :]
        reg = region[here, :]
        regf = reg.astype(F32) * LO
        member = [reg == b for b in range(REGIONS)]
        heat = theta_sum = wet_sum = jnp.zeros((8, COLS), F32)
        stats = jnp.zeros((8, 128), F32)
        for k in range(TIERS):
            t = th[k, here, :]
            face = 0.5 * (t + jnp.where(sub8 == 7, th[k, nxt, :], pltpu.roll(t, 7, 0)))
            vol = jnp.where(face_depth > k, dz_s[k] * width, 0.0)
            mass = vol * sp[k, here, :]
            pos = jnp.clip((face - (-2.0)) * (BINS / 32.0), 0.0, BINS - 1.0)
            low = jnp.minimum(jnp.floor(pos), BINS - 2.0)
            hi = jnp.floor((low + 0.5) * (1.0 / LO))
            hi_r[k] = hi
            cl_r[k] = (low - hi * LO) + regf
            for n, x in enumerate(two_terms(mass) + two_terms(mass * (pos - low))):
                for half in range(2):
                    val_r[k, half, pl.ds(n, 8, stride=8), :] = x[:, 128 * half : 128 * half + 128]
                    val_r[k, half, pl.ds(n + 4, 8, stride=8), :] = x[:, 128 * half : 128 * half + 128]
            heat = heat + mass * face
            theta_sum = theta_sum + vol * face
            wet_sum = wet_sum + vol
            for b in range(REGIONS):
                red = jnp.sum(jnp.where(member[b], mass, 0.0), axis=1, keepdims=True)
                stats = jnp.where(lane8 == b * TIERS + k, red, stats)
            yield
        f = flux[here, :] * area[here, :]
        for b in range(REGIONS):
            red = jnp.sum(jnp.where(member[b], heat, 0.0), axis=1, keepdims=True)
            stats = jnp.where(lane8 == HEAT + b, red, stats)
            red = jnp.sum(jnp.where(member[b], f, 0.0), axis=1, keepdims=True)
            stats = jnp.where(lane8 == FLUX + b, red, stats)
        stats = jnp.where(lane8 == THETA, jnp.sum(theta_sum, axis=1, keepdims=True), stats)
        stats = jnp.where(lane8 == WET, jnp.sum(wet_sum, axis=1, keepdims=True), stats)
        rs_send[g, REGIONS] = stats
        yield

    def bin_rows(hi_r, cl_r, val_r, part_r):
        for jj in range(GROUP):
            total = None
            for k in range(TIERS):
                hi = jnp.broadcast_to(hi_r[k, jj : jj + 1, :], (SIDE, COLS)).astype(BF16)
                cl = jnp.broadcast_to(cl_r[k, jj : jj + 1, :], (SIDE, COLS)).astype(BF16)
                val = jnp.concatenate([val_r[k, half, 8 * jj : 8 * jj + 8, :] for half in range(2)], axis=1)
                val = jnp.concatenate([val] * (SIDE // 8), axis=0).astype(BF16)
                lhs = jnp.where(hi == hi_iota, val, zero)
                rhs = jnp.where(cl == cl_iota, one, zero)
                d = lax.dot_general(lhs, rhs, (((1,), (1,)), ((), ())), preferred_element_type=F32)
                total = d if total is None else total + d
            part_r[pl.ds(jj, SIDE, stride=8), 0:SIDE] = total
            yield

    bin_lane = lax.rem(lane8, LO)
    bin_block = lax.div(lane8, LO)

    def arrange(g, part_r):
        s0 = [jnp.zeros((8, 128), F32)] * REGIONS
        s1 = [jnp.zeros((8, 128), F32)] * REGIONS
        for hi in range(HI):
            rows = [part_r[32 * hi + 8 * n : 32 * hi + 8 * n + 8, :] for n in range(4)]
            wx = rows[2] + rows[3]
            x = rows[0] + rows[1] - wx
            for b in range(REGIONS):
                at = bin_lane + LO * b
                s0[b] = jnp.where(bin_block == hi, jnp.take_along_axis(x, at, axis=1), s0[b])
                s1[b] = jnp.where(bin_block == hi, jnp.take_along_axis(wx, at, axis=1), s1[b])
            yield
        for b in range(REGIONS):
            rs_send[g, b] = s0[b] + jnp.where(lane8 == 0, 0.0, pltpu.roll(s1[b], 1, 1))
        yield

    def together(*parts):
        parts = [p for p in parts if p is not None]
        done = object()
        lead, rest = parts[0], parts[1:]
        per = [2] * len(rest)
        while next(lead, done) is not done:
            for p, n in zip(rest, per):
                for _ in range(n):
                    next(p, done)
        for p in rest:
            while next(p, done) is not done:
                pass

    def send(g):
        for t in range(REGIONS + 1):
            dst, slot = owner(g, t)

            @pl.when(dst != o)
            def _():
                rs_copy(g, t, o).start()

    set_a = (hi_a, cl_a, val_a)
    set_b = (hi_b, cl_b, val_b)

    for load in loads[:3]:
        load.wait()
    flux_totals()
    for load in loads[3:8]:
        load.wait()
    together(prepare(0, *set_a))
    for load in loads[8:]:
        load.wait()
    edge_rows()

    def pair(i, carry):
        g = 2 * i
        together(bin_rows(*set_a, part_a), prepare(g + 1, *set_b), arrange(lax.max(g - 1, 0), part_b))

        @pl.when(i == 0)
        def _():
            first_sends()

        @pl.when(jnp.logical_and(i > 0, chip == 2 * i - 1))
        def _():
            chain_step()

        @pl.when(i > 0)
        def _():
            send(g - 1)
        together(bin_rows(*set_b, part_b), prepare(g + 2, *set_a), arrange(g, part_a))

        @pl.when(chip == 2 * i)
        def _():
            chain_step()
        send(g)
        return carry

    lax.fori_loop(0, 3, pair, 0)
    together(bin_rows(*set_a, part_a), arrange(5, part_b))
    send(5)
    north_row()

    @pl.when(jnp.logical_or(chip == 5, chip == 6))
    def _():
        chain_step()
    together(prepare(7, *set_b))
    together(bin_rows(*set_b, part_b), arrange(6, part_a))
    send(6)

    @pl.when(chip == 7)
    def _():
        chain_step()
    rs_send[7, REGIONS] = rs_send[7, REGIONS] + south_flux[...] + jnp.where(core == 1, pair_flux[...], 0.0)
    together(arrange(7, part_b))
    send(7)

    b_own, g_low = lax.div(o, 4), lax.rem(o, 4)

    def owned(slot, g, t, scale):
        others(NLON, o, lambda q: pltpu.make_async_remote_copy(
            rs_send.at[0, 0], rs_recv.at[slot, q], rs_ssem.at[0, 0], rs_rsem.at[slot, q],
            device_id={"lon": q}, device_id_type=MESH).wait_recv())
        acc = rs_send[g, t]
        for q in range(NLON):
            acc = acc + jnp.where(q != o, rs_recv[slot, q], 0.0)
        ag_send[slot] = acc * scale

    for slot in (0, 1):
        g = 4 * slot + g_low
        owned(slot, g, b_own, UNIT)
        others(NLON, o, lambda q: class_copy(slot, b_own, g, q).start())
        out_class[b_own, pl.ds(pl.multiple_of(8 * g, 8), 8), :] = ag_send[slot]
    odd = jnp.bitwise_and(o - 2 * b_own - 1, 3)
    g_sum = 2 * b_own + odd

    @pl.when(odd < 2)
    def _():
        owned(2, g_sum, REGIONS, 1.0)
        others(NLON, o, lambda q: sums_copy(g_sum, q).start())
        out_sums[pl.ds(pl.multiple_of(8 * g_sum, 8), 8), :] = ag_send[2]

    for g in range(ROWS // 8):
        for t in range(REGIONS + 1):
            dst, slot = owner(jnp.int32(g), t)

            @pl.when(dst != o)
            def _():
                (class_copy(0, t, g, 0) if t < REGIONS else sums_copy(g, 0)).wait_recv()

    for g in range(ROWS // 8):
        for t in range(REGIONS + 1):
            dst, slot = owner(jnp.int32(g), t)

            @pl.when(dst != o)
            def _():
                rs_copy(g, t, o).wait_send()
    for slot in (0, 1):
        others(NLON, o, lambda q: class_copy(slot, b_own, 4 * slot + g_low, q).wait_send())

    @pl.when(odd < 2)
    def _():
        others(NLON, o, lambda q: sums_copy(g_sum, q).wait_send())

    @pl.when(l > 0)
    def _():
        halo_copy().wait_send()

    @pl.when(l == NLAT - 1)
    def _():
        others(NLON, o, lambda q: fold_copy(q, o).wait_send())

    pair_copy().wait_send()

    @pl.when(chip < NLAT // 2 - 1)
    def _():
        chain_copy().wait_send()


def finish(classes, sums, out_class, out_over, out_heat, out_impl, square):
    out_class[...] = classes[...]
    square[0:ROWS, :] = sums[...]
    square[ROWS:128, :] = jnp.zeros((128 - ROWS, 128), F32)
    flipped = jnp.transpose(square[...])
    lane8 = iota((8, 128), 1)
    sub = iota((TIERS, 128), 0)
    mean = flipped[THETA : THETA + 1, :] / jnp.where(iota((1, 128), 1) < ROWS, flipped[WET : WET + 1, :], 1.0)
    for b in range(REGIONS):
        x = flipped[TIERS * b : TIERS * b + TIERS, :]
        vol = jnp.sum(x, axis=0, keepdims=True)
        res = (UNIT / 16.0) * (flipped[HEAT + b : HEAT + b + 1, :] - vol * mean)
        out_heat[b : b + 1, :] = res[:, 0:ROWS]
        for step in (1, 2, 4, 8):
            x = x + jnp.where(sub >= step, pltpu.roll(x, step, 0), 0.0)
        out_over[b] = (UNIT * x)[:, 0:ROWS]
    c = flipped[FLUX : FLUX + 8, :]
    south = jnp.sum(jnp.where(lane8 == ROWS - 1, c, 0.0), axis=1, keepdims=True)
    for step in (1, 2, 4, 8, 16, 32):
        c = c + jnp.where(lane8 >= step, pltpu.roll(c, step, 1), 0.0)
    out_impl[...] = (IMPLIED * (c[0:4] + south[4:8]))[:, 0:ROWS]


def body(speed, theta, dz, dx, area, flux, tally, region, seam):
    any_ = pl.BlockSpec(memory_space=pltpu.HBM)
    vmem = pl.BlockSpec(memory_space=pltpu.VMEM)
    dma = pltpu.SemaphoreType.DMA
    inputs = (speed, theta, dz, dx, area, flux, tally, region, seam)
    inputs = [pltpu.with_memory_space_constraint(x, pltpu.HBM) for x in inputs]
    rows = [pltpu.VMEM((TIERS, GROUP, COLS), F32)] * 2
    sets = (rows + [pltpu.VMEM((TIERS, 2, 8 * GROUP, 128), F32), pltpu.VMEM((8 * SIDE, 128), F32)]) * 2
    classes, sums = pl.pallas_call(
        kernel,
        out_shape=(
            jax.ShapeDtypeStruct((REGIONS, ROWS, BINS), F32),
            jax.ShapeDtypeStruct((ROWS, 128), F32),
        ),
        in_specs=[any_] * 9,
        out_specs=(vmem, vmem),
        scratch_shapes=[
            pltpu.VMEM((TIERS, ROWS + 8, COLS), F32),
            pltpu.VMEM((TIERS, ROWS, COLS), F32),
            pltpu.VMEM((ROWS, COLS), F32),
            pltpu.VMEM((ROWS, COLS), F32),
            pltpu.VMEM((ROWS, COLS), F32),
            pltpu.VMEM((ROWS + 8, COLS), jnp.int32),
            pltpu.VMEM((ROWS, COLS), jnp.int32),
            pltpu.SMEM((TIERS,), F32),
            pltpu.SMEM((COLS,), jnp.int32),
            *sets,
            pltpu.VMEM((ROWS // 8, REGIONS + 1, 8, 128), F32),
            pltpu.VMEM((3, NLON, 8, 128), F32),
            pltpu.VMEM((3, 8, 128), F32),
            pltpu.VMEM((24, COLS), F32),
            pltpu.VMEM((24, COLS), F32),
            pltpu.VMEM((24, COLS), F32),
            pltpu.VMEM((NLON, 24, COLS), F32),
            *([pltpu.VMEM((8, 128), F32)] * 4),
            dma((11,)),
            dma((ROWS // 8, REGIONS + 1)), dma((3, NLON)), dma((3, NLON)),
            dma((REGIONS, ROWS // 8)), dma((ROWS // 8,)),
            dma((NLON,)), dma((NLON,)),
            *([dma] * 6),
        ],
        compiler_params=pltpu.CompilerParams(collective_id=0, has_side_effects=True, vmem_limit_bytes=VMEM_LIMIT),
    )(*inputs)
    out_class, over, heat, impl = pl.pallas_call(
        finish,
        out_shape=(
            jax.ShapeDtypeStruct((REGIONS, ROWS, BINS), F32),
            jax.ShapeDtypeStruct((REGIONS, TIERS, ROWS), F32),
            jax.ShapeDtypeStruct((REGIONS, ROWS), F32),
            jax.ShapeDtypeStruct((REGIONS, ROWS), F32),
        ),
        in_specs=[vmem, vmem],
        out_specs=(vmem,) * 4,
        scratch_shapes=[pltpu.VMEM((128, 128), F32)],
        compiler_params=pltpu.CompilerParams(vmem_limit_bytes=4 * 2**20),
    )(classes, sums)
    return out_class, jnp.transpose(over, (0, 2, 1)), heat, impl


def solution(mesh):
    in_specs = (
        P(None, "lat", "lon"),
        P(None, "lat", "lon"),
        P(),
        P("lat", "lon"),
        P("lat", "lon"),
        P("lat", "lon"),
        P("lat", "lon"),
        P("lat", "lon"),
        P("lon"),
    )
    out_specs = (P(None, "lat", None), P(None, "lat", None), P(None, "lat"), P(None, "lat"))
    return jax.shard_map(body, mesh=mesh, in_specs=in_specs, out_specs=out_specs, check_vma=False)
```

```python
import math

import jax
import jax.numpy as jnp
from jax import lax
from jax.experimental import pallas as pl
from jax.experimental.pallas import tpu as pltpu
from jax.sharding import PartitionSpec as P

BINS = 128
REGIONS = 4
TIERS = 16
ROWS = 64
COLS = 256
NLON = 16
NLAT = 16
GROUP = 8
OWNED = ROWS // NLON
LO = 12
HI = 11
SIDE = REGIONS * LO

HEAT, THETA, WET, FLUX, SOUTH = 64, 68, 69, 72, 76

UNIT = math.sqrt(BINS / (COLS * NLON * TIERS))
IMPLIED = 2.0 / math.sqrt(COLS * NLON * ROWS * NLAT)
VMEM_LIMIT = 32 * 2**20
F32, BF16 = jnp.float32, jnp.bfloat16


def iota(shape, dim):
    return lax.broadcasted_iota(jnp.int32, shape, dim)


def two_terms(x):
    high = x.astype(BF16).astype(F32)
    return high, x - high


def kernel(
    speed_h, theta_h, dz_h, dx_h, area_h, flux_h, tally_h, region_h, seam_h,
    out_class, out_sums,
    th, sp, dx, area, flux, tally, region, dz_s, seam_s,
    hi_a, cl_a, val_a, part_a, hi_b, cl_b, val_b, part_b,
    rs_send, rs_recv, ag_send,
    halo_send, halo_recv, fold_send, fold_recv, own_flux, pair_flux, south_flux, north_flux, offset, offsets,
    in_sem, rs_ssem, rs_rsem, ag_ssem, agc_rsem, ags_rsem, fold_ssem, fold_rsem,
    halo_ssem, halo_rsem, pair_ssem, pair_rsem, chain_ssem, chain_rsem, off_ssem, off_rsem,
):
    o = lax.axis_index("lon")
    l = lax.axis_index("lat")
    lane8 = iota((8, 128), 1)
    MESH = pl.DeviceIdType.MESH

    first, rest = pl.ds(0, 16), pl.ds(16, ROWS - 16)
    loads = [
        pltpu.make_async_copy(flux_h, flux, in_sem.at[0]),
        pltpu.make_async_copy(area_h, area, in_sem.at[1]),
        pltpu.make_async_copy(region_h, region, in_sem.at[2]),
        pltpu.make_async_copy(tally_h, tally.at[pl.ds(0, ROWS)], in_sem.at[3]),
        pltpu.make_async_copy(dx_h, dx, in_sem.at[4]),
        pltpu.make_async_copy(dz_h, dz_s, in_sem.at[9]),
        pltpu.make_async_copy(theta_h.at[:, first], th.at[:, first], in_sem.at[5]),
        pltpu.make_async_copy(speed_h.at[:, first], sp.at[:, first], in_sem.at[6]),
        pltpu.make_async_copy(theta_h.at[:, rest], th.at[:, rest], in_sem.at[7]),
        pltpu.make_async_copy(speed_h.at[:, rest], sp.at[:, rest], in_sem.at[8]),
        pltpu.make_async_copy(seam_h, seam_s, in_sem.at[10]),
    ]
    for load in loads:
        load.start()

    barrier = pltpu.get_barrier_semaphore()
    for d in range(1, NLON):
        pl.semaphore_signal(barrier, inc=1, device_id={"lon": lax.rem(o + d, NLON)}, device_id_type=MESH)
    near = (-2, -1, 1, 2)
    for d in near:
        @pl.when(jnp.logical_and(l + d >= 0, l + d < NLAT))
        def _():
            pl.semaphore_signal(barrier, inc=1, device_id={"lat": l + d}, device_id_type=MESH)

    def halo_copy():
        return pltpu.make_async_remote_copy(
            halo_send, halo_recv, halo_ssem, halo_rsem, device_id={"lat": lax.max(l - 1, 0)}, device_id_type=MESH)

    def fold_copy(dst, src):
        return pltpu.make_async_remote_copy(
            fold_send, fold_recv.at[src], fold_ssem.at[dst], fold_rsem.at[src],
            device_id={"lon": dst}, device_id_type=MESH)

    chip, core = lax.div(l, 2), lax.rem(l, 2)

    def pair_copy():
        return pltpu.make_async_remote_copy(
            own_flux, pair_flux, pair_ssem, pair_rsem, device_id={"lat": l + 1 - 2 * core}, device_id_type=MESH)

    def down_copy():
        return pltpu.make_async_remote_copy(
            south_flux, pair_flux, pair_ssem, pair_rsem, device_id={"lat": l + 1 - 2 * core}, device_id_type=MESH)

    def chain_copy():
        return pltpu.make_async_remote_copy(
            north_flux, south_flux, chain_ssem, chain_rsem,
            device_id={"lat": lax.min(l + 2, NLAT - 1)}, device_id_type=MESH)

    def offset_copy(dst, src):
        return pltpu.make_async_remote_copy(
            offset, offsets.at[src], off_ssem.at[dst], off_rsem.at[src],
            device_id={"lon": dst}, device_id_type=MESH)

    def chain_step(turn):
        @pl.when(jnp.logical_and(turn, core == 1))
        def _():
            pair_copy().wait_recv()

            @pl.when(chip > 0)
            def _():
                chain_copy().wait_recv()
                down_copy().start()

            @pl.when(chip < NLAT // 2 - 1)
            def _():
                north_flux[...] = south_flux[...] + own_flux[...] + pair_flux[...]
                chain_copy().start()

    def owner(g, t):
        if t < REGIONS:
            return 4 * t + lax.rem(g, 4), lax.div(g, 4)
        return 4 * lax.div(g, 2) + lax.rem(g + 1, 4), 2

    def rs_copy(g, t, src):
        dst, slot = owner(g, t)
        return pltpu.make_async_remote_copy(
            rs_send.at[g, t], rs_recv.at[slot, src], rs_ssem.at[g, t], rs_rsem.at[slot, src],
            device_id={"lon": dst}, device_id_type=MESH)

    def class_copy(slot, b, g, dst):
        return pltpu.make_async_remote_copy(
            ag_send.at[slot], out_class.at[b, pl.ds(pl.multiple_of(8 * g, 8), 8)],
            ag_ssem.at[slot, dst], agc_rsem.at[b, g], device_id={"lon": dst}, device_id_type=MESH)

    def sums_copy(g, dst):
        return pltpu.make_async_remote_copy(
            ag_send.at[2], out_sums.at[pl.ds(pl.multiple_of(8 * g, 8), 8)],
            ag_ssem.at[2, dst], ags_rsem.at[g], device_id={"lon": dst}, device_id_type=MESH)

    def others(count, me, act):
        def step(q, c):
            @pl.when(q != me)
            def _():
                act(q)
            return c
        lax.fori_loop(0, count, step, 0)

    def flux_totals():
        acc = [jnp.zeros((8, COLS), F32) for _ in range(REGIONS)]
        for g in range(ROWS // 8):
            rows = slice(8 * g, 8 * g + 8)
            f = flux[rows, :] * area[rows, :]
            reg = region[rows, :]
            for b in range(REGIONS):
                acc[b] = acc[b] + jnp.where(reg == b, f, 0.0)
        totals = jnp.zeros((8, 128), F32)
        for b in range(REGIONS):
            t = jnp.sum(jnp.sum(acc[b], axis=0, keepdims=True), axis=1, keepdims=True)
            totals = jnp.where(lane8 == SOUTH + b, t, totals)
        own_flux[...] = totals

        @pl.when(chip == 0)
        def _():
            south_flux[...] = jnp.zeros((8, 128), F32)

            @pl.when(core == 0)
            def _():
                pair_flux[...] = jnp.zeros((8, 128), F32)

    def edge_rows():
        for k in range(TIERS):
            halo_send[k : k + 1, :] = th[k, 0:1, :]
            fold_send[k : k + 1, :] = th[k, ROWS - 1 : ROWS, :]
        halo_send[TIERS:24, :] = jnp.broadcast_to(tally[0:1, :].astype(F32), (8, COLS))
        fold_send[TIERS:24, :] = jnp.broadcast_to(tally[ROWS - 1 : ROWS, :].astype(F32), (8, COLS))

    def first_sends():
        known = NLON - 1
        for d in near:
            known = known + jnp.where(jnp.logical_and(l + d >= 0, l + d < NLAT), 1, 0)
        pl.semaphore_wait(barrier, known)

        @pl.when(core == 0)
        def _():
            pair_copy().start()

        @pl.when(l == NLAT - 1)
        def _():
            others(NLON, o, lambda q: fold_copy(q, o).start())
            fold_recv[o] = fold_send[...]

        @pl.when(l > 0)
        def _():
            halo_copy().start()

    def north_row():
        @pl.when(l < NLAT - 1)
        def _():
            halo_copy().wait_recv()

        @pl.when(l == NLAT - 1)
        def _():
            others(NLON, o, lambda q: fold_copy(o, q).wait_recv())
            first = seam_s[0]
            source = lax.shift_right_logical(first, 8)
            at = jnp.bitwise_and(first, COLS - 1)
            high = fold_recv[source]
            low = fold_recv[jnp.bitwise_and(source + NLON - 1, NLON - 1)]
            for t in range(COLS // 128):
                i = lane8 + 128 * t
                spot = jnp.bitwise_and(at - i, COLS - 1)
                lane = jnp.bitwise_and(spot, 127)
                for r in range(3):
                    rows = slice(8 * r, 8 * r + 8)
                    pick = [
                        jnp.where(
                            spot >= 128,
                            jnp.take_along_axis(src[rows, 128:], lane, axis=1),
                            jnp.take_along_axis(src[rows, :128], lane, axis=1),
                        )
                        for src in (high, low)
                    ]
                    halo_recv[rows, 128 * t : 128 * t + 128] = jnp.where(i <= at, pick[0], pick[1])

        for k in range(TIERS):
            th[k, ROWS : ROWS + 1, :] = halo_recv[k : k + 1, :]
        tally[ROWS : ROWS + 1, :] = halo_recv[TIERS : TIERS + 1, :].astype(jnp.int32)

    sub8 = iota((8, COLS), 0)
    hi_iota = lax.shift_right_logical(iota((SIDE, COLS), 0), 2).astype(F32).astype(BF16)
    cl_iota = iota((SIDE, COLS), 0).astype(F32).astype(BF16)
    zero = jnp.zeros((SIDE, COLS), BF16)
    one = jnp.ones((SIDE, COLS), BF16)

    def prepare(g, hi_r, cl_r, val_r):
        base = g * GROUP if isinstance(g, int) else pl.multiple_of(g * GROUP, GROUP)
        here = pl.ds(base, GROUP)
        nxt = pl.ds(base + GROUP, 1)
        deep = tally[here, :]
        face_depth = jnp.minimum(deep, jnp.where(sub8 == 7, tally[nxt, :], pltpu.roll(deep, 7, 0)))
        width = dx[here, :]
        reg = region[here, :]
        regf = reg.astype(F32) * LO
        member = [reg == b for b in range(REGIONS)]
        heat = theta_sum = wet_sum = jnp.zeros((8, COLS), F32)
        stats = jnp.zeros((8, 128), F32)
        for k in range(TIERS):
            t = th[k, here, :]
            face = 0.5 * (t + jnp.where(sub8 == 7, th[k, nxt, :], pltpu.roll(t, 7, 0)))
            vol = jnp.where(face_depth > k, dz_s[k] * width, 0.0)
            mass = vol * sp[k, here, :]
            pos = jnp.clip((face - (-2.0)) * (BINS / 32.0), 0.0, BINS - 1.0)
            low = jnp.minimum(jnp.floor(pos), BINS - 2.0)
            hi = jnp.floor((low + 0.5) * (1.0 / LO))
            hi_r[k] = hi
            cl_r[k] = (low - hi * LO) + regf
            for n, x in enumerate(two_terms(mass) + two_terms(mass * (pos - low))):
                for half in range(2):
                    val_r[k, half, pl.ds(n, 8, stride=8), :] = x[:, 128 * half : 128 * half + 128]
                    val_r[k, half, pl.ds(n + 4, 8, stride=8), :] = x[:, 128 * half : 128 * half + 128]
            heat = heat + mass * face
            theta_sum = theta_sum + vol * face
            wet_sum = wet_sum + vol
            for b in range(REGIONS):
                red = jnp.sum(jnp.where(member[b], mass, 0.0), axis=1, keepdims=True)
                stats = jnp.where(lane8 == b * TIERS + k, red, stats)
            yield
        f = flux[here, :] * area[here, :]
        for b in range(REGIONS):
            red = jnp.sum(jnp.where(member[b], heat, 0.0), axis=1, keepdims=True)
            stats = jnp.where(lane8 == HEAT + b, red, stats)
            red = jnp.sum(jnp.where(member[b], f, 0.0), axis=1, keepdims=True)
            stats = jnp.where(lane8 == FLUX + b, red, stats)
        stats = jnp.where(lane8 == THETA, jnp.sum(theta_sum, axis=1, keepdims=True), stats)
        stats = jnp.where(lane8 == WET, jnp.sum(wet_sum, axis=1, keepdims=True), stats)
        rs_send[g, REGIONS] = stats
        yield

    def bin_rows(hi_r, cl_r, val_r, part_r):
        for jj in range(GROUP):
            total = None
            for k in range(TIERS):
                hi = jnp.broadcast_to(hi_r[k, jj : jj + 1, :], (SIDE, COLS)).astype(BF16)
                cl = jnp.broadcast_to(cl_r[k, jj : jj + 1, :], (SIDE, COLS)).astype(BF16)
                val = jnp.concatenate([val_r[k, half, 8 * jj : 8 * jj + 8, :] for half in range(2)], axis=1)
                val = jnp.concatenate([val] * (SIDE // 8), axis=0).astype(BF16)
                lhs = jnp.where(hi == hi_iota, val, zero)
                rhs = jnp.where(cl == cl_iota, one, zero)
                d = lax.dot_general(lhs, rhs, (((1,), (1,)), ((), ())), preferred_element_type=F32)
                total = d if total is None else total + d
            part_r[pl.ds(jj, SIDE, stride=8), 0:SIDE] = total
            yield

    bin_lane = lax.rem(lane8, LO)
    bin_block = lax.div(lane8, LO)

    def arrange(g, part_r):
        s0 = [jnp.zeros((8, 128), F32)] * REGIONS
        s1 = [jnp.zeros((8, 128), F32)] * REGIONS
        for hi in range(HI):
            rows = [part_r[32 * hi + 8 * n : 32 * hi + 8 * n + 8, :] for n in range(4)]
            wx = rows[2] + rows[3]
            x = rows[0] + rows[1] - wx
            for b in range(REGIONS):
                at = bin_lane + LO * b
                s0[b] = jnp.where(bin_block == hi, jnp.take_along_axis(x, at, axis=1), s0[b])
                s1[b] = jnp.where(bin_block == hi, jnp.take_along_axis(wx, at, axis=1), s1[b])
            yield
        for b in range(REGIONS):
            rs_send[g, b] = s0[b] + jnp.where(lane8 == 0, 0.0, pltpu.roll(s1[b], 1, 1))
        yield

    def together(*parts):
        parts = [p for p in parts if p is not None]
        done = object()
        lead, rest = parts[0], parts[1:]
        per = [2] * len(rest)
        while next(lead, done) is not done:
            for p, n in zip(rest, per):
                for _ in range(n):
                    next(p, done)
        for p in rest:
            while next(p, done) is not done:
                pass

    def send(g):
        for t in range(REGIONS + 1):
            dst, slot = owner(g, t)

            @pl.when(dst != o)
            def _():
                rs_copy(g, t, o).start()

    set_a = (hi_a, cl_a, val_a)
    set_b = (hi_b, cl_b, val_b)

    for load in loads[:3]:
        load.wait()
    flux_totals()
    for load in loads[3:8]:
        load.wait()
    together(prepare(0, *set_a))
    for load in loads[8:]:
        load.wait()
    edge_rows()

    def pair(i, carry):
        g = 2 * i
        together(bin_rows(*set_a, part_a), prepare(g + 1, *set_b), arrange(lax.max(g - 1, 0), part_b))

        @pl.when(i == 0)
        def _():
            first_sends()

        chain_step(jnp.logical_and(i > 0, chip == 2 * i - 1))

        @pl.when(i > 0)
        def _():
            send(g - 1)
        together(bin_rows(*set_b, part_b), prepare(g + 2, *set_a), arrange(g, part_a))

        chain_step(chip == 2 * i)
        send(g)
        return carry

    lax.fori_loop(0, 3, pair, 0)
    together(bin_rows(*set_a, part_a), arrange(5, part_b))
    send(5)
    north_row()

    chain_step(chip == 5)
    together(prepare(7, *set_b))
    together(bin_rows(*set_b, part_b), arrange(6, part_a))
    send(6)

    together(arrange(7, part_b))
    send(7)

    chain_step(chip >= 6)

    @pl.when(jnp.logical_and(core == 0, chip > 0))
    def _():
        down_copy().wait_recv()
    offset[...] = pair_flux[...] + jnp.where(core == 1, south_flux[...], 0.0)
    others(NLON, o, lambda q: offset_copy(q, o).start())

    b_own, g_low = lax.div(o, 4), lax.rem(o, 4)

    def owned(slot, g, t, scale):
        others(NLON, o, lambda q: pltpu.make_async_remote_copy(
            rs_send.at[0, 0], rs_recv.at[slot, q], rs_ssem.at[0, 0], rs_rsem.at[slot, q],
            device_id={"lon": q}, device_id_type=MESH).wait_recv())
        acc = rs_send[g, t]
        for q in range(NLON):
            acc = acc + jnp.where(q != o, rs_recv[slot, q], 0.0)
        ag_send[slot] = acc * scale

    for slot in (0, 1):
        g = 4 * slot + g_low
        owned(slot, g, b_own, UNIT)
        others(NLON, o, lambda q: class_copy(slot, b_own, g, q).start())
        out_class[b_own, pl.ds(pl.multiple_of(8 * g, 8), 8), :] = ag_send[slot]
    odd = jnp.bitwise_and(o - 2 * b_own - 1, 3)
    g_sum = 2 * b_own + odd

    @pl.when(odd < 2)
    def _():
        owned(2, g_sum, REGIONS, 1.0)
        others(NLON, o, lambda q: sums_copy(g_sum, q).start())
        out_sums[pl.ds(pl.multiple_of(8 * g_sum, 8), 8), :] = ag_send[2]

    for g in range(ROWS // 8):
        for t in range(REGIONS + 1):
            dst, slot = owner(jnp.int32(g), t)

            @pl.when(dst != o)
            def _():
                (class_copy(0, t, g, 0) if t < REGIONS else sums_copy(g, 0)).wait_recv()

    others(NLON, o, lambda q: offset_copy(o, q).wait_recv())
    south = offset[...]
    for q in range(NLON):
        south = south + jnp.where(q != o, offsets[q], 0.0)
    out_sums[ROWS - 8 : ROWS, :] = out_sums[ROWS - 8 : ROWS, :] + south

    for g in range(ROWS // 8):
        for t in range(REGIONS + 1):
            dst, slot = owner(jnp.int32(g), t)

            @pl.when(dst != o)
            def _():
                rs_copy(g, t, o).wait_send()
    for slot in (0, 1):
        others(NLON, o, lambda q: class_copy(slot, b_own, 4 * slot + g_low, q).wait_send())

    @pl.when(odd < 2)
    def _():
        others(NLON, o, lambda q: sums_copy(g_sum, q).wait_send())

    @pl.when(l > 0)
    def _():
        halo_copy().wait_send()

    @pl.when(l == NLAT - 1)
    def _():
        others(NLON, o, lambda q: fold_copy(q, o).wait_send())

    others(NLON, o, lambda q: offset_copy(q, o).wait_send())

    @pl.when(jnp.logical_or(core == 0, chip > 0))
    def _():
        pair_copy().wait_send()

    @pl.when(jnp.logical_and(core == 1, chip < NLAT // 2 - 1))
    def _():
        chain_copy().wait_send()


def finish(classes, sums, out_class, out_over, out_heat, out_impl, square):
    out_class[...] = classes[...]
    square[0:ROWS, :] = sums[...]
    square[ROWS:128, :] = jnp.zeros((128 - ROWS, 128), F32)
    flipped = jnp.transpose(square[...])
    lane8 = iota((8, 128), 1)
    sub = iota((TIERS, 128), 0)
    mean = flipped[THETA : THETA + 1, :] / jnp.where(iota((1, 128), 1) < ROWS, flipped[WET : WET + 1, :], 1.0)
    for b in range(REGIONS):
        x = flipped[TIERS * b : TIERS * b + TIERS, :]
        vol = jnp.sum(x, axis=0, keepdims=True)
        res = (UNIT / 16.0) * (flipped[HEAT + b : HEAT + b + 1, :] - vol * mean)
        out_heat[b : b + 1, :] = res[:, 0:ROWS]
        for step in (1, 2, 4, 8):
            x = x + jnp.where(sub >= step, pltpu.roll(x, step, 0), 0.0)
        out_over[b] = (UNIT * x)[:, 0:ROWS]
    c = flipped[FLUX : FLUX + 8, :]
    south = jnp.sum(jnp.where(lane8 == ROWS - 1, c, 0.0), axis=1, keepdims=True)
    for step in (1, 2, 4, 8, 16, 32):
        c = c + jnp.where(lane8 >= step, pltpu.roll(c, step, 1), 0.0)
    out_impl[...] = (IMPLIED * (c[0:4] + south[4:8]))[:, 0:ROWS]


def body(speed, theta, dz, dx, area, flux, tally, region, seam):
    any_ = pl.BlockSpec(memory_space=pltpu.HBM)
    vmem = pl.BlockSpec(memory_space=pltpu.VMEM)
    dma = pltpu.SemaphoreType.DMA
    inputs = (speed, theta, dz, dx, area, flux, tally, region, seam)
    inputs = [pltpu.with_memory_space_constraint(x, pltpu.HBM) for x in inputs]
    rows = [pltpu.VMEM((TIERS, GROUP, COLS), F32)] * 2
    sets = (rows + [pltpu.VMEM((TIERS, 2, 8 * GROUP, 128), F32), pltpu.VMEM((8 * SIDE, 128), F32)]) * 2
    classes, sums = pl.pallas_call(
        kernel,
        out_shape=(
            jax.ShapeDtypeStruct((REGIONS, ROWS, BINS), F32),
            jax.ShapeDtypeStruct((ROWS, 128), F32),
        ),
        in_specs=[any_] * 9,
        out_specs=(vmem, vmem),
        scratch_shapes=[
            pltpu.VMEM((TIERS, ROWS + 8, COLS), F32),
            pltpu.VMEM((TIERS, ROWS, COLS), F32),
            pltpu.VMEM((ROWS, COLS), F32),
            pltpu.VMEM((ROWS, COLS), F32),
            pltpu.VMEM((ROWS, COLS), F32),
            pltpu.VMEM((ROWS + 8, COLS), jnp.int32),
            pltpu.VMEM((ROWS, COLS), jnp.int32),
            pltpu.SMEM((TIERS,), F32),
            pltpu.SMEM((COLS,), jnp.int32),
            *sets,
            pltpu.VMEM((ROWS // 8, REGIONS + 1, 8, 128), F32),
            pltpu.VMEM((3, NLON, 8, 128), F32),
            pltpu.VMEM((3, 8, 128), F32),
            pltpu.VMEM((24, COLS), F32),
            pltpu.VMEM((24, COLS), F32),
            pltpu.VMEM((24, COLS), F32),
            pltpu.VMEM((NLON, 24, COLS), F32),
            *([pltpu.VMEM((8, 128), F32)] * 5),
            pltpu.VMEM((NLON, 8, 128), F32),
            dma((11,)),
            dma((ROWS // 8, REGIONS + 1)), dma((3, NLON)), dma((3, NLON)),
            dma((REGIONS, ROWS // 8)), dma((ROWS // 8,)),
            dma((NLON,)), dma((NLON,)),
            *([dma] * 6), dma((NLON,)), dma((NLON,)),
        ],
        compiler_params=pltpu.CompilerParams(collective_id=0, has_side_effects=True, vmem_limit_bytes=VMEM_LIMIT),
    )(*inputs)
    out_class, over, heat, impl = pl.pallas_call(
        finish,
        out_shape=(
            jax.ShapeDtypeStruct((REGIONS, ROWS, BINS), F32),
            jax.ShapeDtypeStruct((REGIONS, TIERS, ROWS), F32),
            jax.ShapeDtypeStruct((REGIONS, ROWS), F32),
            jax.ShapeDtypeStruct((REGIONS, ROWS), F32),
        ),
        in_specs=[vmem, vmem],
        out_specs=(vmem,) * 4,
        scratch_shapes=[pltpu.VMEM((128, 128), F32)],
        compiler_params=pltpu.CompilerParams(vmem_limit_bytes=4 * 2**20),
    )(classes, sums)
    return out_class, jnp.transpose(over, (0, 2, 1)), heat, impl


def solution(mesh):
    in_specs = (
        P(None, "lat", "lon"),
        P(None, "lat", "lon"),
        P(),
        P("lat", "lon"),
        P("lat", "lon"),
        P("lat", "lon"),
        P("lat", "lon"),
        P("lat", "lon"),
        P("lon"),
    )
    out_specs = (P(None, "lat", None), P(None, "lat", None), P(None, "lat"), P(None, "lat"))
    return jax.shard_map(body, mesh=mesh, in_specs=in_specs, out_specs=out_specs, check_vma=False)
```

```python
import math

import jax
import jax.numpy as jnp
from jax import lax
from jax.experimental import pallas as pl
from jax.experimental.pallas import tpu as pltpu
from jax.sharding import PartitionSpec as P

BINS = 128
REGIONS = 4
TIERS = 16
ROWS = 64
COLS = 256
NLON = 16
NLAT = 16
GROUP = 8
OWNED = ROWS // NLON
LO = 12
HI = 11
SIDE = REGIONS * LO

HEAT, THETA, WET, FLUX, SOUTH = 64, 68, 69, 72, 76

UNIT = math.sqrt(BINS / (COLS * NLON * TIERS))
IMPLIED = 2.0 / math.sqrt(COLS * NLON * ROWS * NLAT)
VMEM_LIMIT = 32 * 2**20
F32, BF16 = jnp.float32, jnp.bfloat16


def iota(shape, dim):
    return lax.broadcasted_iota(jnp.int32, shape, dim)


def two_terms(x):
    high = x.astype(BF16).astype(F32)
    return high, x - high


def kernel(
    speed_h, theta_h, dz_h, dx_h, area_h, flux_h, tally_h, region_h, seam_h,
    out_class, out_sums,
    th, sp, dx, area, flux, tally, region, dz_s, seam_s,
    hi_a, cl_a, val_a, part_a, hi_b, cl_b, val_b, part_b,
    rs_send, rs_recv, ag_send,
    halo_send, halo_recv, fold_send, fold_recv, own_flux, pair_flux, south_flux, north_flux, offset, offsets,
    in_sem, rs_ssem, rs_rsem, ag_ssem, ag_rsem, fold_ssem, fold_rsem,
    halo_ssem, halo_rsem, pair_ssem, pair_rsem, chain_ssem, chain_rsem, off_ssem, off_rsem,
):
    o = lax.axis_index("lon")
    l = lax.axis_index("lat")
    lane8 = iota((8, 128), 1)
    MESH = pl.DeviceIdType.MESH

    first, rest = pl.ds(0, 16), pl.ds(16, ROWS - 16)
    loads = [
        pltpu.make_async_copy(tally_h, tally.at[pl.ds(0, ROWS)], in_sem.at[3]),
        pltpu.make_async_copy(dx_h, dx, in_sem.at[4]),
        pltpu.make_async_copy(region_h, region, in_sem.at[2]),
        pltpu.make_async_copy(dz_h, dz_s, in_sem.at[9]),
        pltpu.make_async_copy(theta_h.at[:, first], th.at[:, first], in_sem.at[5]),
        pltpu.make_async_copy(speed_h.at[:, first], sp.at[:, first], in_sem.at[6]),
        pltpu.make_async_copy(flux_h, flux, in_sem.at[0]),
        pltpu.make_async_copy(area_h, area, in_sem.at[1]),
        pltpu.make_async_copy(theta_h.at[:, rest], th.at[:, rest], in_sem.at[7]),
        pltpu.make_async_copy(speed_h.at[:, rest], sp.at[:, rest], in_sem.at[8]),
        pltpu.make_async_copy(seam_h, seam_s, in_sem.at[10]),
    ]
    for load in loads:
        load.start()

    barrier = pltpu.get_barrier_semaphore()
    for d in range(1, NLON):
        pl.semaphore_signal(barrier, inc=1, device_id={"lon": lax.rem(o + d, NLON)}, device_id_type=MESH)
    chip, core = lax.div(l, 2), lax.rem(l, 2)
    sibling = l + 1 - 2 * core
    for q in range(NLON):
        pl.semaphore_signal(barrier, inc=1, device_id={"lon": q, "lat": sibling}, device_id_type=MESH)
    near = (l - 2, l + 2, l - 1 + 2 * core)
    for n in near:
        @pl.when(jnp.logical_and(n >= 0, n < NLAT))
        def _():
            pl.semaphore_signal(barrier, inc=1, device_id={"lat": n}, device_id_type=MESH)

    def halo_copy():
        return pltpu.make_async_remote_copy(
            halo_send, halo_recv, halo_ssem, halo_rsem, device_id={"lat": lax.max(l - 1, 0)}, device_id_type=MESH)

    def fold_copy(dst):
        return pltpu.make_async_remote_copy(
            fold_send, fold_recv.at[o], fold_ssem, fold_rsem, device_id={"lon": dst}, device_id_type=MESH)

    def pair_copy():
        return pltpu.make_async_remote_copy(
            own_flux, pair_flux, pair_ssem, pair_rsem, device_id={"lat": sibling}, device_id_type=MESH)

    def down_copy():
        return pltpu.make_async_remote_copy(
            south_flux, pair_flux, pair_ssem, pair_rsem, device_id={"lat": sibling}, device_id_type=MESH)

    def chain_copy():
        return pltpu.make_async_remote_copy(
            north_flux, south_flux, chain_ssem, chain_rsem,
            device_id={"lat": lax.min(l + 2, NLAT - 1)}, device_id_type=MESH)

    def offset_copy(dst):
        return pltpu.make_async_remote_copy(
            offset, offsets.at[o], off_ssem, off_rsem, device_id={"lon": dst}, device_id_type=MESH)

    def chain_step(turn):
        @pl.when(jnp.logical_and(turn, core == 1))
        def _():
            pair_copy().wait_recv()

            @pl.when(chip > 0)
            def _():
                chain_copy().wait_recv()
                down_copy().start()

            @pl.when(chip < NLAT // 2 - 1)
            def _():
                north_flux[...] = south_flux[...] + own_flux[...] + pair_flux[...]
                chain_copy().start()

    def owner(g, t):
        if t < REGIONS:
            return 4 * t + lax.rem(g, 4), lax.div(g, 4)
        return 4 * lax.div(g, 2) + lax.rem(g + 1, 4), 2

    def rs_copy(g, t):
        dst, slot = owner(g, t)
        return pltpu.make_async_remote_copy(
            rs_send.at[g, t], rs_recv.at[(3 * core + slot) * NLON + o], rs_ssem, rs_rsem.at[core, slot],
            device_id={"lon": dst, "lat": 2 * chip + 1}, device_id_type=MESH)

    def remote_tile(g, t):
        dst, _ = owner(g, t)
        return jnp.logical_or(core == 0, dst != o)

    steps = [(dx, dy) for dx in range(4) for dy in range(4)]
    steps.sort(key=lambda d: -(min(d[0], 4 - d[0]) + min(d[1], 4 - d[1])))
    b_own, g_low = lax.div(o, 4), lax.rem(o, 4)
    peers = [4 * lax.rem(b_own + dx, 4) + lax.rem(g_low + dy, 4) for dx, dy in steps]

    def landed(ref, sem):
        pltpu.make_async_copy(ref, ref, sem).wait()

    def flux_totals():
        acc = [jnp.zeros((8, COLS), F32) for _ in range(REGIONS)]
        for g in range(ROWS // 8):
            rows = slice(8 * g, 8 * g + 8)
            f = flux[rows, :] * area[rows, :]
            reg = region[rows, :]
            for b in range(REGIONS):
                acc[b] = acc[b] + jnp.where(reg == b, f, 0.0)
        totals = jnp.zeros((8, 128), F32)
        for b in range(REGIONS):
            t = jnp.sum(jnp.sum(acc[b], axis=0, keepdims=True), axis=1, keepdims=True)
            totals = jnp.where(lane8 == SOUTH + b, t, totals)
        own_flux[...] = totals

        @pl.when(chip == 0)
        def _():
            south_flux[...] = jnp.zeros((8, 128), F32)

            @pl.when(core == 0)
            def _():
                pair_flux[...] = jnp.zeros((8, 128), F32)

    def edge_rows():
        for k in range(TIERS):
            halo_send[k : k + 1, :] = th[k, 0:1, :]
            fold_send[k : k + 1, :] = th[k, ROWS - 1 : ROWS, :]
        halo_send[TIERS:24, :] = jnp.broadcast_to(tally[0:1, :].astype(F32), (8, COLS))
        fold_send[TIERS:24, :] = jnp.broadcast_to(tally[ROWS - 1 : ROWS, :].astype(F32), (8, COLS))

    def first_sends():
        known = 2 * NLON - 1
        for n in near:
            known = known + jnp.where(jnp.logical_and(n >= 0, n < NLAT), 1, 0)
        pl.semaphore_wait(barrier, known)

        @pl.when(core == 0)
        def _():
            pair_copy().start()

        @pl.when(l == NLAT - 1)
        def _():
            for q in peers[:-1]:
                fold_copy(q).start()
            fold_recv[o] = fold_send[...]

        @pl.when(l > 0)
        def _():
            halo_copy().start()

    def north_row():
        @pl.when(l < NLAT - 1)
        def _():
            halo_copy().wait_recv()

        @pl.when(l == NLAT - 1)
        def _():
            landed(fold_recv.at[pl.ds(0, NLON - 1)], fold_rsem)
            first = seam_s[0]
            source = lax.shift_right_logical(first, 8)
            at = jnp.bitwise_and(first, COLS - 1)
            high = fold_recv[source]
            low = fold_recv[jnp.bitwise_and(source + NLON - 1, NLON - 1)]
            for t in range(COLS // 128):
                i = lane8 + 128 * t
                spot = jnp.bitwise_and(at - i, COLS - 1)
                lane = jnp.bitwise_and(spot, 127)
                for r in range(3):
                    rows = slice(8 * r, 8 * r + 8)
                    pick = [
                        jnp.where(
                            spot >= 128,
                            jnp.take_along_axis(src[rows, 128:], lane, axis=1),
                            jnp.take_along_axis(src[rows, :128], lane, axis=1),
                        )
                        for src in (high, low)
                    ]
                    halo_recv[rows, 128 * t : 128 * t + 128] = jnp.where(i <= at, pick[0], pick[1])

        for k in range(TIERS):
            th[k, ROWS : ROWS + 1, :] = halo_recv[k : k + 1, :]
        tally[ROWS : ROWS + 1, :] = halo_recv[TIERS : TIERS + 1, :].astype(jnp.int32)

    sub8 = iota((8, COLS), 0)
    hi_iota = lax.shift_right_logical(iota((SIDE, COLS), 0), 2).astype(F32).astype(BF16)
    cl_iota = iota((SIDE, COLS), 0).astype(F32).astype(BF16)
    zero = jnp.zeros((SIDE, COLS), BF16)
    one = jnp.ones((SIDE, COLS), BF16)

    def prepare(g, hi_r, cl_r, val_r):
        base = g * GROUP if isinstance(g, int) else pl.multiple_of(g * GROUP, GROUP)
        here = pl.ds(base, GROUP)
        nxt = pl.ds(base + GROUP, 1)
        deep = tally[here, :]
        face_depth = jnp.minimum(deep, jnp.where(sub8 == 7, tally[nxt, :], pltpu.roll(deep, 7, 0)))
        width = dx[here, :]
        reg = region[here, :]
        regf = reg.astype(F32) * LO
        member = [reg == b for b in range(REGIONS)]
        heat = theta_sum = wet_sum = jnp.zeros((8, COLS), F32)
        stats = jnp.zeros((8, 128), F32)
        for k in range(TIERS):
            t = th[k, here, :]
            face = 0.5 * (t + jnp.where(sub8 == 7, th[k, nxt, :], pltpu.roll(t, 7, 0)))
            vol = jnp.where(face_depth > k, dz_s[k] * width, 0.0)
            mass = vol * sp[k, here, :]
            pos = jnp.clip((face - (-2.0)) * (BINS / 32.0), 0.0, BINS - 1.0)
            low = jnp.minimum(jnp.floor(pos), BINS - 2.0)
            hi = jnp.floor((low + 0.5) * (1.0 / LO))
            hi_r[k] = hi
            cl_r[k] = (low - hi * LO) + regf
            for n, x in enumerate(two_terms(mass) + two_terms(mass * (pos - low))):
                for half in range(2):
                    val_r[k, half, pl.ds(n, 8, stride=8), :] = x[:, 128 * half : 128 * half + 128]
                    val_r[k, half, pl.ds(n + 4, 8, stride=8), :] = x[:, 128 * half : 128 * half + 128]
            heat = heat + mass * face
            theta_sum = theta_sum + vol * face
            wet_sum = wet_sum + vol
            for b in range(REGIONS):
                red = jnp.sum(jnp.where(member[b], mass, 0.0), axis=1, keepdims=True)
                stats = jnp.where(lane8 == b * TIERS + k, red, stats)
            yield
        f = flux[here, :] * area[here, :]
        for b in range(REGIONS):
            red = jnp.sum(jnp.where(member[b], heat, 0.0), axis=1, keepdims=True)
            stats = jnp.where(lane8 == HEAT + b, red, stats)
            red = jnp.sum(jnp.where(member[b], f, 0.0), axis=1, keepdims=True)
            stats = jnp.where(lane8 == FLUX + b, red, stats)
        stats = jnp.where(lane8 == THETA, jnp.sum(theta_sum, axis=1, keepdims=True), stats)
        stats = jnp.where(lane8 == WET, jnp.sum(wet_sum, axis=1, keepdims=True), stats)
        rs_send[g, REGIONS] = stats
        yield

    def bin_rows(hi_r, cl_r, val_r, part_r):
        for jj in range(GROUP):
            total = None
            for k in range(TIERS):
                hi = jnp.broadcast_to(hi_r[k, jj : jj + 1, :], (SIDE, COLS)).astype(BF16)
                cl = jnp.broadcast_to(cl_r[k, jj : jj + 1, :], (SIDE, COLS)).astype(BF16)
                val = jnp.concatenate([val_r[k, half, 8 * jj : 8 * jj + 8, :] for half in range(2)], axis=1)
                val = jnp.concatenate([val] * (SIDE // 8), axis=0).astype(BF16)
                lhs = jnp.where(hi == hi_iota, val, zero)
                rhs = jnp.where(cl == cl_iota, one, zero)
                d = lax.dot_general(lhs, rhs, (((1,), (1,)), ((), ())), preferred_element_type=F32)
                total = d if total is None else total + d
            part_r[pl.ds(jj, SIDE, stride=8), 0:SIDE] = total
            yield

    bin_lane = lax.rem(lane8, LO)
    bin_block = lax.div(lane8, LO)

    def arrange(g, part_r):
        s0 = [jnp.zeros((8, 128), F32)] * REGIONS
        s1 = [jnp.zeros((8, 128), F32)] * REGIONS
        for hi in range(HI):
            rows = [part_r[32 * hi + 8 * n : 32 * hi + 8 * n + 8, :] for n in range(4)]
            wx = rows[2] + rows[3]
            x = rows[0] + rows[1] - wx
            for b in range(REGIONS):
                at = bin_lane + LO * b
                s0[b] = jnp.where(bin_block == hi, jnp.take_along_axis(x, at, axis=1), s0[b])
                s1[b] = jnp.where(bin_block == hi, jnp.take_along_axis(wx, at, axis=1), s1[b])
            yield
        for b in range(REGIONS):
            rs_send[g, b] = s0[b] + jnp.where(lane8 == 0, 0.0, pltpu.roll(s1[b], 1, 1))
        yield

    def together(*parts):
        parts = [p for p in parts if p is not None]
        done = object()
        lead, rest = parts[0], parts[1:]
        per = [2] * len(rest)
        while next(lead, done) is not done:
            for p, n in zip(rest, per):
                for _ in range(n):
                    next(p, done)
        for p in rest:
            while next(p, done) is not done:
                pass

    def send(g):
        for t in range(REGIONS + 1):
            @pl.when(remote_tile(g, t))
            def _():
                rs_copy(g, t).start()

    set_a = (hi_a, cl_a, val_a)
    set_b = (hi_b, cl_b, val_b)

    for load in loads[:8]:
        load.wait()
    flux_totals()
    together(prepare(0, *set_a))
    for load in loads[8:]:
        load.wait()
    edge_rows()

    def pair(i, carry):
        g = 2 * i
        together(bin_rows(*set_a, part_a), prepare(g + 1, *set_b), arrange(lax.max(g - 1, 0), part_b))

        @pl.when(i == 0)
        def _():
            first_sends()

        chain_step(jnp.logical_and(i > 0, chip == 2 * i - 1))

        @pl.when(i > 0)
        def _():
            send(g - 1)
        together(bin_rows(*set_b, part_b), prepare(g + 2, *set_a), arrange(g, part_a))

        chain_step(chip == 2 * i)
        send(g)
        return carry

    lax.fori_loop(0, 3, pair, 0)
    together(bin_rows(*set_a, part_a), arrange(5, part_b))
    send(5)
    north_row()

    chain_step(chip == 5)
    together(prepare(7, *set_b))
    together(bin_rows(*set_b, part_b), arrange(6, part_a))
    send(6)

    together(arrange(7, part_b))
    send(7)

    chain_step(chip >= 6)

    @pl.when(jnp.logical_and(core == 0, chip > 0))
    def _():
        down_copy().wait_recv()
    offset[...] = pair_flux[...] + jnp.where(core == 1, south_flux[...], 0.0)
    for q in peers[:-1]:
        offset_copy(q).start()

    tiles = NLON * 2 + NLON // 2

    def owned(slot, g, t, scale, put):
        for c in (0, 1):
            at = 3 * c + slot
            landed(rs_recv.at[pl.ds(0, NLON - c)], rs_rsem.at[c, slot])
            parts = [rs_recv[at * NLON + q] for q in range(NLON)]
            if c == 1:
                parts = [jnp.where(q != o, p, 0.0) for q, p in enumerate(parts)] + [rs_send[g, t]]
            while len(parts) > 1:
                parts = [sum(parts[i : i + 2]) for i in range(0, len(parts), 2)]
            ag_send[at] = parts[0] * scale
            to = put(slot, g)
            for q in peers[: NLON - c]:
                pltpu.make_async_remote_copy(
                    ag_send.at[at], to, ag_ssem, ag_rsem,
                    device_id={"lon": q, "lat": 2 * chip + c}, device_id_type=MESH).start()
        to[...] = ag_send[at]

    def put_class(slot, g):
        return out_class.at[b_own, pl.ds(pl.multiple_of(8 * g, 8), 8)]

    def put_sums(slot, g):
        return out_sums.at[pl.ds(pl.multiple_of(8 * g, 8), 8)]

    odd = jnp.bitwise_and(o - 2 * b_own - 1, 3)
    g_sum = 2 * b_own + odd

    @pl.when(core == 1)
    def _():
        owned(0, g_low, b_own, UNIT, put_class)

        @pl.when(jnp.logical_and(odd < 2, g_sum < 7))
        def _():
            owned(2, g_sum, REGIONS, 1.0, put_sums)
        owned(1, 4 + g_low, b_own, UNIT, put_class)

        @pl.when(jnp.logical_and(odd < 2, g_sum == 7))
        def _():
            owned(2, g_sum, REGIONS, 1.0, put_sums)

    @pl.when(core == 0)
    def _():
        landed(rs_recv.at[pl.ds(0, tiles)], rs_ssem)
        pair_copy().wait_send()

    @pl.when(core == 1)
    def _():
        @pl.when(odd < 2)
        def _():
            landed(rs_recv.at[pl.ds(0, tiles - 3)], rs_ssem)
            landed(rs_recv.at[pl.ds(0, 3 * (2 * NLON - 1))], ag_ssem)

        @pl.when(odd >= 2)
        def _():
            landed(rs_recv.at[pl.ds(0, tiles - 2)], rs_ssem)
            landed(rs_recv.at[pl.ds(0, 2 * (2 * NLON - 1))], ag_ssem)

        @pl.when(chip > 0)
        def _():
            pair_copy().wait_send()

        @pl.when(chip < NLAT // 2 - 1)
        def _():
            chain_copy().wait_send()

    landed(rs_recv.at[pl.ds(0, NLON - 1)], off_ssem)

    @pl.when(l > 0)
    def _():
        halo_copy().wait_send()

    @pl.when(l == NLAT - 1)
    def _():
        landed(fold_recv.at[pl.ds(0, NLON - 1)], fold_ssem)

    landed(offsets.at[pl.ds(0, NLON - 1)], off_rsem)
    south = offset[...]
    for q in range(NLON):
        south = south + jnp.where(q != o, offsets[q], 0.0)

    @pl.when(core == 0)
    def _():
        landed(rs_recv.at[pl.ds(0, tiles)], ag_rsem)

    @pl.when(core == 1)
    def _():
        @pl.when(odd < 2)
        def _():
            landed(rs_recv.at[pl.ds(0, tiles - 3)], ag_rsem)

        @pl.when(odd >= 2)
        def _():
            landed(rs_recv.at[pl.ds(0, tiles - 2)], ag_rsem)
    out_sums[ROWS - 8 : ROWS, :] = out_sums[ROWS - 8 : ROWS, :] + south


def finish(classes, sums, out_class, out_over, out_heat, out_impl, square, sem):
    whole = pltpu.make_async_copy(classes, out_class, sem)
    whole.start()
    square[0:ROWS, :] = sums[...]
    square[ROWS:128, :] = jnp.zeros((128 - ROWS, 128), F32)
    flipped = jnp.transpose(square[...])
    lane8 = iota((8, 128), 1)
    sub = iota((TIERS, 128), 0)
    mean = flipped[THETA : THETA + 1, :] / jnp.where(iota((1, 128), 1) < ROWS, flipped[WET : WET + 1, :], 1.0)
    for b in range(REGIONS):
        x = flipped[TIERS * b : TIERS * b + TIERS, :]
        vol = jnp.sum(x, axis=0, keepdims=True)
        res = (UNIT / 16.0) * (flipped[HEAT + b : HEAT + b + 1, :] - vol * mean)
        out_heat[b : b + 1, :] = res[:, 0:ROWS]
        for step in (1, 2, 4, 8):
            x = x + jnp.where(sub >= step, pltpu.roll(x, step, 0), 0.0)
        out_over[b] = (UNIT * x)[:, 0:ROWS]
    c = flipped[FLUX : FLUX + 8, :]
    south = jnp.sum(jnp.where(lane8 == ROWS - 1, c, 0.0), axis=1, keepdims=True)
    for step in (1, 2, 4, 8, 16, 32):
        c = c + jnp.where(lane8 >= step, pltpu.roll(c, step, 1), 0.0)
    out_impl[...] = (IMPLIED * (c[0:4] + south[4:8]))[:, 0:ROWS]
    whole.wait()


def body(speed, theta, dz, dx, area, flux, tally, region, seam):
    any_ = pl.BlockSpec(memory_space=pltpu.HBM)
    vmem = pl.BlockSpec(memory_space=pltpu.VMEM)
    dma = pltpu.SemaphoreType.DMA
    inputs = (speed, theta, dz, dx, area, flux, tally, region, seam)
    inputs = [pltpu.with_memory_space_constraint(x, pltpu.HBM) for x in inputs]
    rows = [pltpu.VMEM((TIERS, GROUP, COLS), F32)] * 2
    sets = (rows + [pltpu.VMEM((TIERS, 2, 8 * GROUP, 128), F32), pltpu.VMEM((8 * SIDE, 128), F32)]) * 2
    classes, sums = pl.pallas_call(
        kernel,
        out_shape=(
            jax.ShapeDtypeStruct((REGIONS, ROWS, BINS), F32),
            jax.ShapeDtypeStruct((ROWS, 128), F32),
        ),
        in_specs=[any_] * 9,
        out_specs=(vmem, vmem),
        scratch_shapes=[
            pltpu.VMEM((TIERS, ROWS + 8, COLS), F32),
            pltpu.VMEM((TIERS, ROWS, COLS), F32),
            pltpu.VMEM((ROWS, COLS), F32),
            pltpu.VMEM((ROWS, COLS), F32),
            pltpu.VMEM((ROWS, COLS), F32),
            pltpu.VMEM((ROWS + 8, COLS), jnp.int32),
            pltpu.VMEM((ROWS, COLS), jnp.int32),
            pltpu.SMEM((TIERS,), F32),
            pltpu.SMEM((COLS,), jnp.int32),
            *sets,
            pltpu.VMEM((ROWS // 8, REGIONS + 1, 8, 128), F32),
            pltpu.VMEM((2 * 3 * NLON, 8, 128), F32),
            pltpu.VMEM((2 * 3, 8, 128), F32),
            pltpu.VMEM((24, COLS), F32),
            pltpu.VMEM((24, COLS), F32),
            pltpu.VMEM((24, COLS), F32),
            pltpu.VMEM((NLON, 24, COLS), F32),
            *([pltpu.VMEM((8, 128), F32)] * 5),
            pltpu.VMEM((NLON, 8, 128), F32),
            dma((11,)),
            dma, dma((2, 3)), dma, dma,
            dma, dma,
            *([dma] * 8),
        ],
        compiler_params=pltpu.CompilerParams(collective_id=0, has_side_effects=True, vmem_limit_bytes=VMEM_LIMIT),
    )(*inputs)
    out_class, over, heat, impl = pl.pallas_call(
        finish,
        out_shape=(
            jax.ShapeDtypeStruct((REGIONS, ROWS, BINS), F32),
            jax.ShapeDtypeStruct((REGIONS, TIERS, ROWS), F32),
            jax.ShapeDtypeStruct((REGIONS, ROWS), F32),
            jax.ShapeDtypeStruct((REGIONS, ROWS), F32),
        ),
        in_specs=[vmem, vmem],
        out_specs=(any_, vmem, vmem, vmem),
        scratch_shapes=[pltpu.VMEM((128, 128), F32), dma],
        compiler_params=pltpu.CompilerParams(vmem_limit_bytes=4 * 2**20),
    )(classes, sums)
    return out_class, jnp.transpose(over, (0, 2, 1)), heat, impl


def solution(mesh):
    in_specs = (
        P(None, "lat", "lon"),
        P(None, "lat", "lon"),
        P(),
        P("lat", "lon"),
        P("lat", "lon"),
        P("lat", "lon"),
        P("lat", "lon"),
        P("lat", "lon"),
        P("lon"),
    )
    out_specs = (P(None, "lat", None), P(None, "lat", None), P(None, "lat"), P(None, "lat"))
    return jax.shard_map(body, mesh=mesh, in_specs=in_specs, out_specs=out_specs, check_vma=False)
```

```python
import math

import jax
import jax.numpy as jnp
from jax import lax
from jax.experimental import pallas as pl
from jax.experimental.pallas import tpu as pltpu
from jax.sharding import PartitionSpec as P

BINS = 128
REGIONS = 4
TIERS = 16
ROWS = 64
COLS = 256
NLON = 16
NLAT = 16
GROUP = 8
OWNED = ROWS // NLON
LO = 12
HI = 11
SIDE = REGIONS * LO

HEAT, THETA, WET, FLUX, SOUTH = 64, 68, 69, 72, 76

UNIT = math.sqrt(BINS / (COLS * NLON * TIERS))
IMPLIED = 2.0 / math.sqrt(COLS * NLON * ROWS * NLAT)
VMEM_LIMIT = 32 * 2**20
F32, BF16 = jnp.float32, jnp.bfloat16


def iota(shape, dim):
    return lax.broadcasted_iota(jnp.int32, shape, dim)


def two_terms(x):
    high = x.astype(BF16).astype(F32)
    return high, x - high


def kernel(
    speed_h, theta_h, dz_h, dx_h, area_h, flux_h, tally_h, region_h, seam_h,
    out_class, out_sums,
    th, sp, dx, area, flux, tally, region, dz_s, seam_s,
    hi_a, cl_a, val_a, part_a, hi_b, cl_b, val_b, part_b,
    rs_send, rs_recv, ag_send,
    halo_send, halo_recv, fold_send, fold_recv, own_flux, pair_flux, south_flux, north_flux, offset, offsets,
    in_sem, rs_ssem, rs_rsem, ag_ssem, ag_rsem, fold_ssem, fold_rsem,
    halo_ssem, halo_rsem, pair_ssem, pair_rsem, chain_ssem, chain_rsem, off_ssem, off_rsem,
):
    o = lax.axis_index("lon")
    l = lax.axis_index("lat")
    lane8 = iota((8, 128), 1)
    MESH = pl.DeviceIdType.MESH

    first, rest = pl.ds(0, 16), pl.ds(16, ROWS - 16)
    loads = [
        pltpu.make_async_copy(tally_h, tally.at[pl.ds(0, ROWS)], in_sem.at[3]),
        pltpu.make_async_copy(dx_h, dx, in_sem.at[4]),
        pltpu.make_async_copy(region_h, region, in_sem.at[2]),
        pltpu.make_async_copy(dz_h, dz_s, in_sem.at[9]),
        pltpu.make_async_copy(theta_h.at[:, first], th.at[:, first], in_sem.at[5]),
        pltpu.make_async_copy(speed_h.at[:, first], sp.at[:, first], in_sem.at[6]),
        pltpu.make_async_copy(flux_h, flux, in_sem.at[0]),
        pltpu.make_async_copy(area_h, area, in_sem.at[1]),
        pltpu.make_async_copy(theta_h.at[:, rest], th.at[:, rest], in_sem.at[7]),
        pltpu.make_async_copy(speed_h.at[:, rest], sp.at[:, rest], in_sem.at[8]),
        pltpu.make_async_copy(seam_h, seam_s, in_sem.at[10]),
    ]
    for load in loads:
        load.start()

    barrier = pltpu.get_barrier_semaphore()
    for d in range(1, NLON):
        pl.semaphore_signal(barrier, inc=1, device_id={"lon": lax.rem(o + d, NLON)}, device_id_type=MESH)
    chip, core = lax.div(l, 2), lax.rem(l, 2)
    sibling = l + 1 - 2 * core
    for q in range(NLON):
        pl.semaphore_signal(barrier, inc=1, device_id={"lon": q, "lat": sibling}, device_id_type=MESH)
    near = (l - 2, l + 2, l - 1 + 2 * core)
    for n in near:
        @pl.when(jnp.logical_and(n >= 0, n < NLAT))
        def _():
            pl.semaphore_signal(barrier, inc=1, device_id={"lat": n}, device_id_type=MESH)

    def halo_copy():
        return pltpu.make_async_remote_copy(
            halo_send, halo_recv, halo_ssem, halo_rsem, device_id={"lat": lax.max(l - 1, 0)}, device_id_type=MESH)

    def fold_copy(dst):
        return pltpu.make_async_remote_copy(
            fold_send, fold_recv.at[o], fold_ssem, fold_rsem, device_id={"lon": dst}, device_id_type=MESH)

    def pair_copy():
        return pltpu.make_async_remote_copy(
            own_flux, pair_flux, pair_ssem, pair_rsem, device_id={"lat": sibling}, device_id_type=MESH)

    def down_copy():
        return pltpu.make_async_remote_copy(
            south_flux, pair_flux, pair_ssem, pair_rsem, device_id={"lat": sibling}, device_id_type=MESH)

    def chain_copy():
        return pltpu.make_async_remote_copy(
            north_flux, south_flux, chain_ssem, chain_rsem,
            device_id={"lat": lax.min(l + 2, NLAT - 1)}, device_id_type=MESH)

    def offset_copy(dst):
        return pltpu.make_async_remote_copy(
            offset, offsets.at[o], off_ssem, off_rsem, device_id={"lon": dst}, device_id_type=MESH)

    def chain_step(turn):
        @pl.when(jnp.logical_and(turn, core == 1))
        def _():
            pair_copy().wait_recv()

            @pl.when(chip > 0)
            def _():
                chain_copy().wait_recv()
                down_copy().start()

            @pl.when(chip < NLAT // 2 - 1)
            def _():
                north_flux[...] = south_flux[...] + own_flux[...] + pair_flux[...]
                chain_copy().start()

    def owner(g, t):
        turn = lax.rem(g, 4)
        wide_x, wide_y = lax.div(turn, 2), lax.rem(turn, 2)
        late = lax.div(g, 4)
        b = t if t < REGIONS else 3 * (1 - late)
        x, y = (b // 2, b % 2) if t < REGIONS else (1 - late, 1 - late)
        x = jnp.where(wide_x == 1, 3 * x, 1 + x)
        y = jnp.where(wide_y == 1, 3 * y, 1 + y)
        return 4 * x + y, (late if t < REGIONS else 2)

    def rs_copy(g, t):
        dst, slot = owner(g, t)
        return pltpu.make_async_remote_copy(
            rs_send.at[g, t], rs_recv.at[(3 * core + slot) * NLON + o], rs_ssem, rs_rsem.at[core, slot],
            device_id={"lon": dst, "lat": 2 * chip + 1}, device_id_type=MESH)

    def remote_tile(g, t):
        dst, _ = owner(g, t)
        return jnp.logical_or(core == 0, dst != o)

    x_own, y_own = lax.div(o, 4), lax.rem(o, 4)
    wide = [jnp.where(jnp.logical_or(v == 0, v == 3), 1, 0) for v in (x_own, y_own)]
    turn = 2 * wide[0] + wide[1]
    b_own = 2 * jnp.where(x_own >= 2, 1, 0) + jnp.where(y_own >= 2, 1, 0)
    peers = (0, 4, 1, 5, 8, 12, 2, 9, 3, 6, 13, 7, 10, 11, 14, 15)

    def to_peers(act, all_of_them=False):
        for q in peers:
            if all_of_them:
                act(q)
            else:
                @pl.when(o != q)
                def _():
                    act(q)

    def landed(ref, sem):
        pltpu.make_async_copy(ref, ref, sem).wait()

    def flux_totals():
        acc = [jnp.zeros((8, COLS), F32) for _ in range(REGIONS)]
        for g in range(ROWS // 8):
            rows = slice(8 * g, 8 * g + 8)
            f = flux[rows, :] * area[rows, :]
            reg = region[rows, :]
            for b in range(REGIONS):
                acc[b] = acc[b] + jnp.where(reg == b, f, 0.0)
        totals = jnp.zeros((8, 128), F32)
        for b in range(REGIONS):
            t = jnp.sum(jnp.sum(acc[b], axis=0, keepdims=True), axis=1, keepdims=True)
            totals = jnp.where(lane8 == SOUTH + b, t, totals)
        own_flux[...] = totals

        @pl.when(chip == 0)
        def _():
            south_flux[...] = jnp.zeros((8, 128), F32)

            @pl.when(core == 0)
            def _():
                pair_flux[...] = jnp.zeros((8, 128), F32)

    def edge_rows():
        for k in range(TIERS):
            halo_send[k : k + 1, :] = th[k, 0:1, :]
            fold_send[k : k + 1, :] = th[k, ROWS - 1 : ROWS, :]
        halo_send[TIERS:24, :] = jnp.broadcast_to(tally[0:1, :].astype(F32), (8, COLS))
        fold_send[TIERS:24, :] = jnp.broadcast_to(tally[ROWS - 1 : ROWS, :].astype(F32), (8, COLS))

    def first_sends():
        known = 2 * NLON - 1
        for n in near:
            known = known + jnp.where(jnp.logical_and(n >= 0, n < NLAT), 1, 0)
        pl.semaphore_wait(barrier, known)

        @pl.when(core == 0)
        def _():
            pair_copy().start()

        @pl.when(l == NLAT - 1)
        def _():
            to_peers(lambda q: fold_copy(q).start())
            fold_recv[o] = fold_send[...]

        @pl.when(l > 0)
        def _():
            halo_copy().start()

    def north_row():
        @pl.when(l < NLAT - 1)
        def _():
            halo_copy().wait_recv()

        @pl.when(l == NLAT - 1)
        def _():
            landed(fold_recv.at[pl.ds(0, NLON - 1)], fold_rsem)
            first = seam_s[0]
            source = lax.shift_right_logical(first, 8)
            at = jnp.bitwise_and(first, COLS - 1)
            high = fold_recv[source]
            low = fold_recv[jnp.bitwise_and(source + NLON - 1, NLON - 1)]
            for t in range(COLS // 128):
                i = lane8 + 128 * t
                spot = jnp.bitwise_and(at - i, COLS - 1)
                lane = jnp.bitwise_and(spot, 127)
                for r in range(3):
                    rows = slice(8 * r, 8 * r + 8)
                    pick = [
                        jnp.where(
                            spot >= 128,
                            jnp.take_along_axis(src[rows, 128:], lane, axis=1),
                            jnp.take_along_axis(src[rows, :128], lane, axis=1),
                        )
                        for src in (high, low)
                    ]
                    halo_recv[rows, 128 * t : 128 * t + 128] = jnp.where(i <= at, pick[0], pick[1])

        for k in range(TIERS):
            th[k, ROWS : ROWS + 1, :] = halo_recv[k : k + 1, :]
        tally[ROWS : ROWS + 1, :] = halo_recv[TIERS : TIERS + 1, :].astype(jnp.int32)

    sub8 = iota((8, COLS), 0)
    hi_iota = lax.shift_right_logical(iota((SIDE, COLS), 0), 2).astype(F32).astype(BF16)
    cl_iota = iota((SIDE, COLS), 0).astype(F32).astype(BF16)
    zero = jnp.zeros((SIDE, COLS), BF16)
    one = jnp.ones((SIDE, COLS), BF16)

    def prepare(g, hi_r, cl_r, val_r):
        base = g * GROUP if isinstance(g, int) else pl.multiple_of(g * GROUP, GROUP)
        here = pl.ds(base, GROUP)
        nxt = pl.ds(base + GROUP, 1)
        deep = tally[here, :]
        face_depth = jnp.minimum(deep, jnp.where(sub8 == 7, tally[nxt, :], pltpu.roll(deep, 7, 0)))
        width = dx[here, :]
        reg = region[here, :]
        regf = reg.astype(F32) * LO
        member = [reg == b for b in range(REGIONS)]
        heat = theta_sum = wet_sum = jnp.zeros((8, COLS), F32)
        stats = jnp.zeros((8, 128), F32)
        for k in range(TIERS):
            t = th[k, here, :]
            face = 0.5 * (t + jnp.where(sub8 == 7, th[k, nxt, :], pltpu.roll(t, 7, 0)))
            vol = jnp.where(face_depth > k, dz_s[k] * width, 0.0)
            mass = vol * sp[k, here, :]
            pos = jnp.clip((face - (-2.0)) * (BINS / 32.0), 0.0, BINS - 1.0)
            low = jnp.minimum(jnp.floor(pos), BINS - 2.0)
            hi = jnp.floor((low + 0.5) * (1.0 / LO))
            hi_r[k] = hi
            cl_r[k] = (low - hi * LO) + regf
            for n, x in enumerate(two_terms(mass) + two_terms(mass * (pos - low))):
                for half in range(2):
                    val_r[k, half, pl.ds(n, 8, stride=8), :] = x[:, 128 * half : 128 * half + 128]
                    val_r[k, half, pl.ds(n + 4, 8, stride=8), :] = x[:, 128 * half : 128 * half + 128]
            heat = heat + mass * face
            theta_sum = theta_sum + vol * face
            wet_sum = wet_sum + vol
            for b in range(REGIONS):
                red = jnp.sum(jnp.where(member[b], mass, 0.0), axis=1, keepdims=True)
                stats = jnp.where(lane8 == b * TIERS + k, red, stats)
            yield
        f = flux[here, :] * area[here, :]
        for b in range(REGIONS):
            red = jnp.sum(jnp.where(member[b], heat, 0.0), axis=1, keepdims=True)
            stats = jnp.where(lane8 == HEAT + b, red, stats)
            red = jnp.sum(jnp.where(member[b], f, 0.0), axis=1, keepdims=True)
            stats = jnp.where(lane8 == FLUX + b, red, stats)
        stats = jnp.where(lane8 == THETA, jnp.sum(theta_sum, axis=1, keepdims=True), stats)
        stats = jnp.where(lane8 == WET, jnp.sum(wet_sum, axis=1, keepdims=True), stats)
        rs_send[g, REGIONS] = stats
        yield

    def bin_rows(hi_r, cl_r, val_r, part_r):
        for jj in range(GROUP):
            total = None
            for k in range(TIERS):
                hi = jnp.broadcast_to(hi_r[k, jj : jj + 1, :], (SIDE, COLS)).astype(BF16)
                cl = jnp.broadcast_to(cl_r[k, jj : jj + 1, :], (SIDE, COLS)).astype(BF16)
                val = jnp.concatenate([val_r[k, half, 8 * jj : 8 * jj + 8, :] for half in range(2)], axis=1)
                val = jnp.concatenate([val] * (SIDE // 8), axis=0).astype(BF16)
                lhs = jnp.where(hi == hi_iota, val, zero)
                rhs = jnp.where(cl == cl_iota, one, zero)
                d = lax.dot_general(lhs, rhs, (((1,), (1,)), ((), ())), preferred_element_type=F32)
                total = d if total is None else total + d
            part_r[pl.ds(jj, SIDE, stride=8), 0:SIDE] = total
            yield

    bin_lane = lax.rem(lane8, LO)
    bin_block = lax.div(lane8, LO)

    def arrange(g, part_r):
        s0 = [jnp.zeros((8, 128), F32)] * REGIONS
        s1 = [jnp.zeros((8, 128), F32)] * REGIONS
        for hi in range(HI):
            rows = [part_r[32 * hi + 8 * n : 32 * hi + 8 * n + 8, :] for n in range(4)]
            wx = rows[2] + rows[3]
            x = rows[0] + rows[1] - wx
            for b in range(REGIONS):
                at = bin_lane + LO * b
                s0[b] = jnp.where(bin_block == hi, jnp.take_along_axis(x, at, axis=1), s0[b])
                s1[b] = jnp.where(bin_block == hi, jnp.take_along_axis(wx, at, axis=1), s1[b])
            yield
        for b in range(REGIONS):
            rs_send[g, b] = s0[b] + jnp.where(lane8 == 0, 0.0, pltpu.roll(s1[b], 1, 1))
        yield

    def together(*parts):
        parts = [p for p in parts if p is not None]
        done = object()
        lead, rest = parts[0], parts[1:]
        per = [2] * len(rest)
        while next(lead, done) is not done:
            for p, n in zip(rest, per):
                for _ in range(n):
                    next(p, done)
        for p in rest:
            while next(p, done) is not done:
                pass

    def send(g):
        for t in range(REGIONS + 1):
            @pl.when(remote_tile(g, t))
            def _():
                rs_copy(g, t).start()

    set_a = (hi_a, cl_a, val_a)
    set_b = (hi_b, cl_b, val_b)

    for load in loads[:8]:
        load.wait()
    flux_totals()
    together(prepare(0, *set_a))
    for load in loads[8:]:
        load.wait()
    edge_rows()

    def pair(i, carry):
        g = 2 * i
        together(bin_rows(*set_a, part_a), prepare(g + 1, *set_b), arrange(lax.max(g - 1, 0), part_b))

        @pl.when(i == 0)
        def _():
            first_sends()

        chain_step(jnp.logical_and(i > 0, chip == 2 * i - 1))

        @pl.when(i > 0)
        def _():
            send(g - 1)
        together(bin_rows(*set_b, part_b), prepare(g + 2, *set_a), arrange(g, part_a))

        chain_step(chip == 2 * i)
        send(g)
        return carry

    lax.fori_loop(0, 3, pair, 0)
    together(bin_rows(*set_a, part_a), arrange(5, part_b))
    send(5)
    north_row()

    chain_step(chip == 5)
    together(prepare(7, *set_b))
    together(bin_rows(*set_b, part_b), arrange(6, part_a))
    send(6)

    together(arrange(7, part_b))
    send(7)

    chain_step(chip >= 6)

    @pl.when(jnp.logical_and(core == 0, chip > 0))
    def _():
        down_copy().wait_recv()
    offset[...] = pair_flux[...] + jnp.where(core == 1, south_flux[...], 0.0)
    to_peers(lambda q: offset_copy(q).start())

    tiles = NLON * 2 + NLON // 2

    def owned(slot, g, t, scale, put):
        for c in (0, 1):
            at = 3 * c + slot
            landed(rs_recv.at[pl.ds(0, NLON - c)], rs_rsem.at[c, slot])
            parts = [rs_recv[at * NLON + q] for q in range(NLON)]
            if c == 1:
                parts = [jnp.where(q != o, p, 0.0) for q, p in enumerate(parts)] + [rs_send[g, t]]
            while len(parts) > 1:
                parts = [sum(parts[i : i + 2]) for i in range(0, len(parts), 2)]
            ag_send[at] = parts[0] * scale
            to = put(slot, g)
            to_peers(lambda q: pltpu.make_async_remote_copy(
                ag_send.at[at], to, ag_ssem, ag_rsem,
                device_id={"lon": q, "lat": 2 * chip + c}, device_id_type=MESH).start(), c == 0)
        to[...] = ag_send[at]

    def put_class(slot, g):
        return out_class.at[b_own, pl.ds(pl.multiple_of(8 * g, 8), 8)]

    def put_sums(slot, g):
        return out_sums.at[pl.ds(pl.multiple_of(8 * g, 8), 8)]

    has_sums = jnp.logical_or(b_own == 0, b_own == 3)
    no_sums = jnp.logical_not(has_sums)
    g_sum = turn + jnp.where(b_own == 0, 4, 0)

    @pl.when(core == 1)
    def _():
        owned(0, turn, b_own, UNIT, put_class)

        @pl.when(jnp.logical_and(has_sums, g_sum < 7))
        def _():
            owned(2, g_sum, REGIONS, 1.0, put_sums)
        owned(1, 4 + turn, b_own, UNIT, put_class)

        @pl.when(jnp.logical_and(has_sums, g_sum == 7))
        def _():
            owned(2, g_sum, REGIONS, 1.0, put_sums)

    @pl.when(core == 0)
    def _():
        landed(rs_recv.at[pl.ds(0, tiles)], rs_ssem)
        pair_copy().wait_send()

    @pl.when(core == 1)
    def _():
        @pl.when(has_sums)
        def _():
            landed(rs_recv.at[pl.ds(0, tiles - 3)], rs_ssem)
            landed(rs_recv.at[pl.ds(0, 3 * (2 * NLON - 1))], ag_ssem)

        @pl.when(no_sums)
        def _():
            landed(rs_recv.at[pl.ds(0, tiles - 2)], rs_ssem)
            landed(rs_recv.at[pl.ds(0, 2 * (2 * NLON - 1))], ag_ssem)

        @pl.when(chip > 0)
        def _():
            pair_copy().wait_send()

        @pl.when(chip < NLAT // 2 - 1)
        def _():
            chain_copy().wait_send()

    landed(rs_recv.at[pl.ds(0, NLON - 1)], off_ssem)

    @pl.when(l > 0)
    def _():
        halo_copy().wait_send()

    @pl.when(l == NLAT - 1)
    def _():
        landed(fold_recv.at[pl.ds(0, NLON - 1)], fold_ssem)

    landed(offsets.at[pl.ds(0, NLON - 1)], off_rsem)
    south = offset[...]
    for q in range(NLON):
        south = south + jnp.where(q != o, offsets[q], 0.0)

    @pl.when(core == 0)
    def _():
        landed(rs_recv.at[pl.ds(0, tiles)], ag_rsem)

    @pl.when(core == 1)
    def _():
        @pl.when(has_sums)
        def _():
            landed(rs_recv.at[pl.ds(0, tiles - 3)], ag_rsem)

        @pl.when(no_sums)
        def _():
            landed(rs_recv.at[pl.ds(0, tiles - 2)], ag_rsem)
    out_sums[ROWS - 8 : ROWS, :] = out_sums[ROWS - 8 : ROWS, :] + south


def finish(classes, sums, out_class, out_over, out_heat, out_impl, square):
    out_class[...] = classes[...]
    square[0:ROWS, :] = sums[...]
    square[ROWS:128, :] = jnp.zeros((128 - ROWS, 128), F32)
    flipped = jnp.transpose(square[...])
    lane8 = iota((8, 128), 1)
    sub = iota((TIERS, 128), 0)
    mean = flipped[THETA : THETA + 1, :] / jnp.where(iota((1, 128), 1) < ROWS, flipped[WET : WET + 1, :], 1.0)
    for b in range(REGIONS):
        x = flipped[TIERS * b : TIERS * b + TIERS, :]
        vol = jnp.sum(x, axis=0, keepdims=True)
        res = (UNIT / 16.0) * (flipped[HEAT + b : HEAT + b + 1, :] - vol * mean)
        out_heat[b : b + 1, :] = res[:, 0:ROWS]
        for step in (1, 2, 4, 8):
            x = x + jnp.where(sub >= step, pltpu.roll(x, step, 0), 0.0)
        out_over[b] = (UNIT * x)[:, 0:ROWS]
    c = flipped[FLUX : FLUX + 8, :]
    south = jnp.sum(jnp.where(lane8 == ROWS - 1, c, 0.0), axis=1, keepdims=True)
    for step in (1, 2, 4, 8, 16, 32):
        c = c + jnp.where(lane8 >= step, pltpu.roll(c, step, 1), 0.0)
    out_impl[...] = (IMPLIED * (c[0:4] + south[4:8]))[:, 0:ROWS]


def body(speed, theta, dz, dx, area, flux, tally, region, seam):
    any_ = pl.BlockSpec(memory_space=pltpu.HBM)
    vmem = pl.BlockSpec(memory_space=pltpu.VMEM)
    dma = pltpu.SemaphoreType.DMA
    inputs = (speed, theta, dz, dx, area, flux, tally, region, seam)
    inputs = [pltpu.with_memory_space_constraint(x, pltpu.HBM) for x in inputs]
    rows = [pltpu.VMEM((TIERS, GROUP, COLS), F32)] * 2
    sets = (rows + [pltpu.VMEM((TIERS, 2, 8 * GROUP, 128), F32), pltpu.VMEM((8 * SIDE, 128), F32)]) * 2
    classes, sums = pl.pallas_call(
        kernel,
        out_shape=(
            jax.ShapeDtypeStruct((REGIONS, ROWS, BINS), F32),
            jax.ShapeDtypeStruct((ROWS, 128), F32),
        ),
        in_specs=[any_] * 9,
        out_specs=(vmem, vmem),
        scratch_shapes=[
            pltpu.VMEM((TIERS, ROWS + 8, COLS), F32),
            pltpu.VMEM((TIERS, ROWS, COLS), F32),
            pltpu.VMEM((ROWS, COLS), F32),
            pltpu.VMEM((ROWS, COLS), F32),
            pltpu.VMEM((ROWS, COLS), F32),
            pltpu.VMEM((ROWS + 8, COLS), jnp.int32),
            pltpu.VMEM((ROWS, COLS), jnp.int32),
            pltpu.SMEM((TIERS,), F32),
            pltpu.SMEM((COLS,), jnp.int32),
            *sets,
            pltpu.VMEM((ROWS // 8, REGIONS + 1, 8, 128), F32),
            pltpu.VMEM((2 * 3 * NLON, 8, 128), F32),
            pltpu.VMEM((2 * 3, 8, 128), F32),
            pltpu.VMEM((24, COLS), F32),
            pltpu.VMEM((24, COLS), F32),
            pltpu.VMEM((24, COLS), F32),
            pltpu.VMEM((NLON, 24, COLS), F32),
            *([pltpu.VMEM((8, 128), F32)] * 5),
            pltpu.VMEM((NLON, 8, 128), F32),
            dma((11,)),
            dma, dma((2, 3)), dma, dma,
            dma, dma,
            *([dma] * 8),
        ],
        compiler_params=pltpu.CompilerParams(collective_id=0, has_side_effects=True, vmem_limit_bytes=VMEM_LIMIT),
    )(*inputs)
    out_class, over, heat, impl = pl.pallas_call(
        finish,
        out_shape=(
            jax.ShapeDtypeStruct((REGIONS, ROWS, BINS), F32),
            jax.ShapeDtypeStruct((REGIONS, TIERS, ROWS), F32),
            jax.ShapeDtypeStruct((REGIONS, ROWS), F32),
            jax.ShapeDtypeStruct((REGIONS, ROWS), F32),
        ),
        in_specs=[vmem, vmem],
        out_specs=(vmem,) * 4,
        scratch_shapes=[pltpu.VMEM((128, 128), F32)],
        compiler_params=pltpu.CompilerParams(vmem_limit_bytes=4 * 2**20),
    )(classes, sums)
    return out_class, jnp.transpose(over, (0, 2, 1)), heat, impl


def solution(mesh):
    in_specs = (
        P(None, "lat", "lon"),
        P(None, "lat", "lon"),
        P(),
        P("lat", "lon"),
        P("lat", "lon"),
        P("lat", "lon"),
        P("lat", "lon"),
        P("lat", "lon"),
        P("lon"),
    )
    out_specs = (P(None, "lat", None), P(None, "lat", None), P(None, "lat"), P(None, "lat"))
    return jax.shard_map(body, mesh=mesh, in_specs=in_specs, out_specs=out_specs, check_vma=False)
```

```python
import math

import jax
import jax.numpy as jnp
from jax import lax
from jax.experimental import pallas as pl
from jax.experimental.pallas import tpu as pltpu
from jax.sharding import PartitionSpec as P

BINS = 128
REGIONS = 4
TIERS = 16
ROWS = 64
COLS = 256
NLON = 16
NLAT = 16
GROUP = 8
OWNED = ROWS // NLON
LO = 12
HI = 11
SIDE = REGIONS * LO

HEAT, THETA, WET, FLUX, SOUTH = 64, 68, 69, 72, 76

UNIT = math.sqrt(BINS / (COLS * NLON * TIERS))
IMPLIED = 2.0 / math.sqrt(COLS * NLON * ROWS * NLAT)
VMEM_LIMIT = 32 * 2**20
F32, BF16 = jnp.float32, jnp.bfloat16


def iota(shape, dim):
    return lax.broadcasted_iota(jnp.int32, shape, dim)


def two_terms(x):
    high = x.astype(BF16).astype(F32)
    return high, x - high


def kernel(
    speed_h, theta_h, dz_h, dx_h, area_h, flux_h, tally_h, region_h, seam_h,
    out_class, out_sums,
    th, sp, dx, area, flux, tally, region, dz_s, seam_s,
    hi_a, cl_a, val_a, part_a, hi_b, cl_b, val_b, part_b,
    rs_send, rs_recv, ag_send,
    halo_send, halo_recv, fold_send, fold_recv, own_flux, pair_flux, south_flux, north_flux, offset, offsets,
    in_sem, rs_ssem, rs_rsem, ag_ssem, ag_rsem, fold_ssem, fold_rsem,
    halo_ssem, halo_rsem, pair_ssem, pair_rsem, chain_ssem, chain_rsem, off_ssem, off_rsem,
):
    o = lax.axis_index("lon")
    l = lax.axis_index("lat")
    lane8 = iota((8, 128), 1)
    MESH = pl.DeviceIdType.MESH

    first, rest = pl.ds(0, 24), pl.ds(24, ROWS - 24)
    loads = [
        pltpu.make_async_copy(tally_h, tally.at[pl.ds(0, ROWS)], in_sem.at[3]),
        pltpu.make_async_copy(dx_h, dx, in_sem.at[4]),
        pltpu.make_async_copy(region_h, region, in_sem.at[2]),
        pltpu.make_async_copy(dz_h, dz_s, in_sem.at[9]),
        pltpu.make_async_copy(theta_h.at[:, first], th.at[:, first], in_sem.at[5]),
        pltpu.make_async_copy(speed_h.at[:, first], sp.at[:, first], in_sem.at[6]),
        pltpu.make_async_copy(flux_h, flux, in_sem.at[0]),
        pltpu.make_async_copy(area_h, area, in_sem.at[1]),
        pltpu.make_async_copy(theta_h.at[:, rest], th.at[:, rest], in_sem.at[7]),
        pltpu.make_async_copy(speed_h.at[:, rest], sp.at[:, rest], in_sem.at[8]),
        pltpu.make_async_copy(seam_h, seam_s, in_sem.at[10]),
    ]
    for load in loads:
        load.start()

    barrier = pltpu.get_barrier_semaphore()
    for d in range(1, NLON):
        pl.semaphore_signal(barrier, inc=1, device_id={"lon": lax.rem(o + d, NLON)}, device_id_type=MESH)
    chip, core = lax.div(l, 2), lax.rem(l, 2)
    sibling = l + 1 - 2 * core
    for q in range(NLON):
        pl.semaphore_signal(barrier, inc=1, device_id={"lon": q, "lat": sibling}, device_id_type=MESH)
    near = (l - 2, l + 2, l - 1 + 2 * core)
    for n in near:
        @pl.when(jnp.logical_and(n >= 0, n < NLAT))
        def _():
            pl.semaphore_signal(barrier, inc=1, device_id={"lat": n}, device_id_type=MESH)

    def halo_copy():
        return pltpu.make_async_remote_copy(
            halo_send, halo_recv, halo_ssem, halo_rsem, device_id={"lat": lax.max(l - 1, 0)}, device_id_type=MESH)

    def fold_copy(dst):
        return pltpu.make_async_remote_copy(
            fold_send, fold_recv.at[o], fold_ssem, fold_rsem, device_id={"lon": dst}, device_id_type=MESH)

    def pair_copy():
        return pltpu.make_async_remote_copy(
            own_flux, pair_flux, pair_ssem, pair_rsem, device_id={"lat": sibling}, device_id_type=MESH)

    def down_copy():
        return pltpu.make_async_remote_copy(
            south_flux, pair_flux, pair_ssem, pair_rsem, device_id={"lat": sibling}, device_id_type=MESH)

    def chain_copy():
        return pltpu.make_async_remote_copy(
            north_flux, south_flux, chain_ssem, chain_rsem,
            device_id={"lat": lax.min(l + 2, NLAT - 1)}, device_id_type=MESH)

    def offset_copy(dst):
        return pltpu.make_async_remote_copy(
            offset, offsets.at[o], off_ssem, off_rsem, device_id={"lon": dst}, device_id_type=MESH)

    def chain_step(turn):
        @pl.when(jnp.logical_and(turn, core == 1))
        def _():
            pair_copy().wait_recv()

            @pl.when(chip > 0)
            def _():
                chain_copy().wait_recv()
                down_copy().start()

            @pl.when(chip < NLAT // 2 - 1)
            def _():
                north_flux[...] = south_flux[...] + own_flux[...] + pair_flux[...]
                chain_copy().start()

    def owner(g, t):
        turn = lax.rem(g if t < REGIONS else g + 3, 4)
        wide_x, wide_y = lax.div(turn, 2), lax.rem(turn, 2)
        late = lax.div(g, 4)
        b = t if t < REGIONS else 3 * (1 - late)
        x, y = (b // 2, b % 2) if t < REGIONS else (1 - late, 1 - late)
        x = jnp.where(wide_x == 1, 3 * x, 1 + x)
        y = jnp.where(wide_y == 1, 3 * y, 1 + y)
        return 4 * x + y, (late if t < REGIONS else 2)

    def rs_copy(g, t):
        dst, slot = owner(g, t)
        return pltpu.make_async_remote_copy(
            rs_send.at[g, t], rs_recv.at[(3 * core + slot) * NLON + o], rs_ssem, rs_rsem.at[core, slot],
            device_id={"lon": dst, "lat": 2 * chip + 1}, device_id_type=MESH)

    def remote_tile(g, t):
        dst, _ = owner(g, t)
        return jnp.logical_or(core == 0, dst != o)

    x_own, y_own = lax.div(o, 4), lax.rem(o, 4)
    wide = [jnp.where(jnp.logical_or(v == 0, v == 3), 1, 0) for v in (x_own, y_own)]
    turn = 2 * wide[0] + wide[1]
    b_own = 2 * jnp.where(x_own >= 2, 1, 0) + jnp.where(y_own >= 2, 1, 0)
    peers = (0, 4, 1, 5, 8, 12, 2, 9, 3, 6, 13, 7, 10, 11, 14, 15)

    def to_peers(act, all_of_them=False):
        for q in peers:
            if all_of_them:
                act(q)
            else:
                @pl.when(o != q)
                def _():
                    act(q)

    def landed(ref, sem):
        pltpu.make_async_copy(ref, ref, sem).wait()

    def flux_totals():
        acc = [jnp.zeros((8, COLS), F32) for _ in range(REGIONS)]
        for g in range(ROWS // 8):
            rows = slice(8 * g, 8 * g + 8)
            f = flux[rows, :] * area[rows, :]
            reg = region[rows, :]
            for b in range(REGIONS):
                acc[b] = acc[b] + jnp.where(reg == b, f, 0.0)
        totals = jnp.zeros((8, 128), F32)
        for b in range(REGIONS):
            t = jnp.sum(jnp.sum(acc[b], axis=0, keepdims=True), axis=1, keepdims=True)
            totals = jnp.where(lane8 == SOUTH + b, t, totals)
        own_flux[...] = totals

        @pl.when(chip == 0)
        def _():
            south_flux[...] = jnp.zeros((8, 128), F32)

            @pl.when(core == 0)
            def _():
                pair_flux[...] = jnp.zeros((8, 128), F32)

    def edge_rows():
        for k in range(TIERS):
            halo_send[k : k + 1, :] = th[k, 0:1, :]
            fold_send[k : k + 1, :] = th[k, ROWS - 1 : ROWS, :]
        halo_send[TIERS:24, :] = jnp.broadcast_to(tally[0:1, :].astype(F32), (8, COLS))
        fold_send[TIERS:24, :] = jnp.broadcast_to(tally[ROWS - 1 : ROWS, :].astype(F32), (8, COLS))

    def first_sends():
        known = 2 * NLON - 1
        for n in near:
            known = known + jnp.where(jnp.logical_and(n >= 0, n < NLAT), 1, 0)
        pl.semaphore_wait(barrier, known)

        @pl.when(core == 0)
        def _():
            pair_copy().start()

        @pl.when(l == NLAT - 1)
        def _():
            to_peers(lambda q: fold_copy(q).start())
            fold_recv[o] = fold_send[...]

        @pl.when(l > 0)
        def _():
            halo_copy().start()

    def put_north():
        for k in range(TIERS):
            th[k, ROWS : ROWS + 1, :] = halo_recv[k : k + 1, :]
        tally[ROWS : ROWS + 1, :] = halo_recv[TIERS : TIERS + 1, :].astype(jnp.int32)

    def north_row():
        halo_copy().wait_recv()
        put_north()

    def fold_row():
        landed(fold_recv.at[pl.ds(0, NLON - 1)], fold_rsem)
        first = seam_s[0]
        source = lax.shift_right_logical(first, 8)
        at = jnp.bitwise_and(first, COLS - 1)
        high = fold_recv[source]
        low = fold_recv[jnp.bitwise_and(source + NLON - 1, NLON - 1)]
        for t in range(COLS // 128):
            i = lane8 + 128 * t
            spot = jnp.bitwise_and(at - i, COLS - 1)
            lane = jnp.bitwise_and(spot, 127)
            for r in range(3):
                rows = slice(8 * r, 8 * r + 8)
                pick = [
                    jnp.where(
                        spot >= 128,
                        jnp.take_along_axis(src[rows, 128:], lane, axis=1),
                        jnp.take_along_axis(src[rows, :128], lane, axis=1),
                    )
                    for src in (high, low)
                ]
                halo_recv[rows, 128 * t : 128 * t + 128] = jnp.where(i <= at, pick[0], pick[1])
        put_north()

    sub8 = iota((8, COLS), 0)
    hi_iota = lax.shift_right_logical(iota((SIDE, COLS), 0), 2).astype(F32).astype(BF16)
    cl_iota = iota((SIDE, COLS), 0).astype(F32).astype(BF16)
    zero = jnp.zeros((SIDE, COLS), BF16)
    one = jnp.ones((SIDE, COLS), BF16)

    def prepare(g, hi_r, cl_r, val_r):
        base = g * GROUP if isinstance(g, int) else pl.multiple_of(g * GROUP, GROUP)
        here = pl.ds(base, GROUP)
        nxt = pl.ds(base + GROUP, 1)
        deep = tally[here, :]
        face_depth = jnp.minimum(deep, jnp.where(sub8 == 7, tally[nxt, :], pltpu.roll(deep, 7, 0)))
        width = dx[here, :]
        reg = region[here, :]
        regf = reg.astype(F32) * LO
        member = [reg == b for b in range(REGIONS)]
        heat = theta_sum = wet_sum = jnp.zeros((8, COLS), F32)
        stats = jnp.zeros((8, 128), F32)
        for k in range(TIERS):
            t = th[k, here, :]
            face = 0.5 * (t + jnp.where(sub8 == 7, th[k, nxt, :], pltpu.roll(t, 7, 0)))
            vol = jnp.where(face_depth > k, dz_s[k] * width, 0.0)
            mass = vol * sp[k, here, :]
            pos = jnp.clip((face - (-2.0)) * (BINS / 32.0), 0.0, BINS - 1.0)
            low = jnp.minimum(jnp.floor(pos), BINS - 2.0)
            hi = jnp.floor((low + 0.5) * (1.0 / LO))
            hi_r[k] = hi
            cl_r[k] = (low - hi * LO) + regf
            for n, x in enumerate(two_terms(mass) + two_terms(mass * (pos - low))):
                for half in range(2):
                    val_r[k, half, pl.ds(n, 8, stride=8), :] = x[:, 128 * half : 128 * half + 128]
                    val_r[k, half, pl.ds(n + 4, 8, stride=8), :] = x[:, 128 * half : 128 * half + 128]
            heat = heat + mass * face
            theta_sum = theta_sum + vol * face
            wet_sum = wet_sum + vol
            for b in range(REGIONS):
                red = jnp.sum(jnp.where(member[b], mass, 0.0), axis=1, keepdims=True)
                stats = jnp.where(lane8 == b * TIERS + k, red, stats)
            yield
        f = flux[here, :] * area[here, :]
        for b in range(REGIONS):
            red = jnp.sum(jnp.where(member[b], heat, 0.0), axis=1, keepdims=True)
            stats = jnp.where(lane8 == HEAT + b, red, stats)
            red = jnp.sum(jnp.where(member[b], f, 0.0), axis=1, keepdims=True)
            stats = jnp.where(lane8 == FLUX + b, red, stats)
        stats = jnp.where(lane8 == THETA, jnp.sum(theta_sum, axis=1, keepdims=True), stats)
        stats = jnp.where(lane8 == WET, jnp.sum(wet_sum, axis=1, keepdims=True), stats)
        rs_send[g, REGIONS] = stats
        yield

    def bin_rows(hi_r, cl_r, val_r, part_r):
        for jj in range(GROUP):
            total = None
            for k in range(TIERS):
                hi = jnp.broadcast_to(hi_r[k, jj : jj + 1, :], (SIDE, COLS)).astype(BF16)
                cl = jnp.broadcast_to(cl_r[k, jj : jj + 1, :], (SIDE, COLS)).astype(BF16)
                val = jnp.concatenate([val_r[k, half, 8 * jj : 8 * jj + 8, :] for half in range(2)], axis=1)
                val = jnp.concatenate([val] * (SIDE // 8), axis=0).astype(BF16)
                lhs = jnp.where(hi == hi_iota, val, zero)
                rhs = jnp.where(cl == cl_iota, one, zero)
                d = lax.dot_general(lhs, rhs, (((1,), (1,)), ((), ())), preferred_element_type=F32)
                total = d if total is None else total + d
            part_r[pl.ds(jj, SIDE, stride=8), 0:SIDE] = total
            yield

    bin_lane = lax.rem(lane8, LO)
    bin_block = lax.div(lane8, LO)

    def arrange(g, part_r):
        s0 = [jnp.zeros((8, 128), F32)] * REGIONS
        s1 = [jnp.zeros((8, 128), F32)] * REGIONS
        for hi in range(HI):
            rows = [part_r[32 * hi + 8 * n : 32 * hi + 8 * n + 8, :] for n in range(4)]
            wx = rows[2] + rows[3]
            x = rows[0] + rows[1] - wx
            for b in range(REGIONS):
                at = bin_lane + LO * b
                s0[b] = jnp.where(bin_block == hi, jnp.take_along_axis(x, at, axis=1), s0[b])
                s1[b] = jnp.where(bin_block == hi, jnp.take_along_axis(wx, at, axis=1), s1[b])
            yield
        for b in range(REGIONS):
            rs_send[g, b] = s0[b] + jnp.where(lane8 == 0, 0.0, pltpu.roll(s1[b], 1, 1))
        yield

    def together(*parts):
        parts = [p for p in parts if p is not None]
        done = object()
        lead, rest = parts[0], parts[1:]
        per = [2] * len(rest)
        while next(lead, done) is not done:
            for p, n in zip(rest, per):
                for _ in range(n):
                    next(p, done)
        for p in rest:
            while next(p, done) is not done:
                pass

    def send(g):
        for t in range(REGIONS + 1):
            @pl.when(remote_tile(g, t))
            def _():
                rs_copy(g, t).start()

    set_a = (hi_a, cl_a, val_a)
    set_b = (hi_b, cl_b, val_b)

    for load in loads[:8]:
        load.wait()
    together(prepare(0, *set_a))

    def pair(i, carry):
        g = 2 * i
        together(bin_rows(*set_a, part_a), prepare(g + 1, *set_b), arrange(lax.max(g - 1, 0), part_b))

        @pl.when(i == 0)
        def _():
            for load in loads[8:]:
                load.wait()
            flux_totals()
            edge_rows()
            first_sends()

        chain_step(jnp.logical_and(i > 0, chip == 2 * i - 1))

        @pl.when(i > 0)
        def _():
            send(g - 1)
        together(bin_rows(*set_b, part_b), prepare(g + 2, *set_a), arrange(g, part_a))

        chain_step(chip == 2 * i)
        send(g)
        return carry

    lax.fori_loop(0, 3, pair, 0)
    @pl.when(l < NLAT - 1)
    def _():
        north_row()
        together(bin_rows(*set_a, part_a), prepare(7, *set_b), arrange(5, part_b))

    @pl.when(l == NLAT - 1)
    def _():
        together(bin_rows(*set_a, part_a), arrange(5, part_b))
        fold_row()
        together(prepare(7, *set_b))
    send(5)
    chain_step(chip == 5)
    together(bin_rows(*set_b, part_b), arrange(6, part_a))
    send(6)

    together(arrange(7, part_b))
    send(7)

    chain_step(chip >= 6)

    @pl.when(jnp.logical_and(core == 0, chip > 0))
    def _():
        down_copy().wait_recv()
    offset[...] = pair_flux[...] + jnp.where(core == 1, south_flux[...], 0.0)
    to_peers(lambda q: offset_copy(q).start())

    tiles = NLON * 2 + NLON // 2

    def owned(slot, g, t, scale, put):
        for c in (0, 1):
            at = 3 * c + slot
            landed(rs_recv.at[pl.ds(0, NLON - c)], rs_rsem.at[c, slot])
            parts = [rs_recv[at * NLON + q] for q in range(NLON)]
            if c == 1:
                parts = [jnp.where(q != o, p, 0.0) for q, p in enumerate(parts)] + [rs_send[g, t]]
            while len(parts) > 1:
                parts = [sum(parts[i : i + 2]) for i in range(0, len(parts), 2)]
            ag_send[at] = parts[0] * scale
            to = put(slot, g)
            to_peers(lambda q: pltpu.make_async_remote_copy(
                ag_send.at[at], to, ag_ssem, ag_rsem,
                device_id={"lon": q, "lat": 2 * chip + c}, device_id_type=MESH).start(), c == 0)
        to[...] = ag_send[at]

    def put_class(slot, g):
        return out_class.at[b_own, pl.ds(pl.multiple_of(8 * g, 8), 8)]

    def put_sums(slot, g):
        return out_sums.at[pl.ds(pl.multiple_of(8 * g, 8), 8)]

    has_sums = jnp.logical_or(b_own == 0, b_own == 3)
    no_sums = jnp.logical_not(has_sums)
    g_sum = lax.rem(turn + 1, 4) + jnp.where(b_own == 0, 4, 0)

    @pl.when(core == 1)
    def _():
        owned(0, turn, b_own, UNIT, put_class)

        @pl.when(jnp.logical_and(has_sums, g_sum < 7))
        def _():
            owned(2, g_sum, REGIONS, 1.0, put_sums)
        owned(1, 4 + turn, b_own, UNIT, put_class)

        @pl.when(jnp.logical_and(has_sums, g_sum == 7))
        def _():
            owned(2, g_sum, REGIONS, 1.0, put_sums)

    @pl.when(core == 0)
    def _():
        landed(rs_recv.at[pl.ds(0, tiles)], rs_ssem)
        pair_copy().wait_send()

    @pl.when(core == 1)
    def _():
        @pl.when(has_sums)
        def _():
            landed(rs_recv.at[pl.ds(0, tiles - 3)], rs_ssem)
            landed(rs_recv.at[pl.ds(0, 3 * (2 * NLON - 1))], ag_ssem)

        @pl.when(no_sums)
        def _():
            landed(rs_recv.at[pl.ds(0, tiles - 2)], rs_ssem)
            landed(rs_recv.at[pl.ds(0, 2 * (2 * NLON - 1))], ag_ssem)

        @pl.when(chip > 0)
        def _():
            pair_copy().wait_send()

        @pl.when(chip < NLAT // 2 - 1)
        def _():
            chain_copy().wait_send()

    landed(rs_recv.at[pl.ds(0, NLON - 1)], off_ssem)

    @pl.when(l > 0)
    def _():
        halo_copy().wait_send()

    @pl.when(l == NLAT - 1)
    def _():
        landed(fold_recv.at[pl.ds(0, NLON - 1)], fold_ssem)

    landed(offsets.at[pl.ds(0, NLON - 1)], off_rsem)
    south = offset[...]
    for q in range(NLON):
        south = south + jnp.where(q != o, offsets[q], 0.0)

    @pl.when(core == 0)
    def _():
        landed(rs_recv.at[pl.ds(0, tiles)], ag_rsem)

    @pl.when(core == 1)
    def _():
        @pl.when(has_sums)
        def _():
            landed(rs_recv.at[pl.ds(0, tiles - 3)], ag_rsem)

        @pl.when(no_sums)
        def _():
            landed(rs_recv.at[pl.ds(0, tiles - 2)], ag_rsem)
    out_sums[ROWS - 8 : ROWS, :] = out_sums[ROWS - 8 : ROWS, :] + south


def finish(classes, sums, out_class, out_over, out_heat, out_impl):
    out_class[...] = classes[...]
    row, lane = iota((88, 128), 0), iota((88, 128), 1)
    upto = (row < HEAT) & (lane <= row) & (lax.div(lane, TIERS) == lax.div(row, TIERS))
    volume = (row >= HEAT) & (row < HEAT + 4) & (lax.div(lane, TIERS) == row - HEAT)
    same = (row >= 72) & (lane == row - 8)
    pick = jnp.where(upto | volume | same, 1.0, 0.0)
    res = lax.dot_general(
        pick, sums[...], (((1,), (1,)), ((), ())), precision=lax.Precision.HIGHEST, preferred_element_type=F32)
    for b in range(REGIONS):
        out_over[b] = UNIT * res[TIERS * b : TIERS * b + TIERS]
    at = HEAT + 8
    mean = res[at + 4 : at + 5] / res[at + 5 : at + 6]
    out_heat[...] = (UNIT / 16.0) * (res[at : at + 4] - res[HEAT : HEAT + 4] * mean)
    flux = res[FLUX + 8 : FLUX + 16]
    south_of = jnp.where(iota((ROWS, ROWS), 0) <= iota((ROWS, ROWS), 1), 1.0, 0.0)
    c = jnp.dot(flux, south_of, precision=lax.Precision.HIGHEST, preferred_element_type=F32)
    out_impl[...] = IMPLIED * (c[0:4] + flux[4:8, ROWS - 1 : ROWS])


def body(speed, theta, dz, dx, area, flux, tally, region, seam):
    any_ = pl.BlockSpec(memory_space=pltpu.HBM)
    vmem = pl.BlockSpec(memory_space=pltpu.VMEM)
    dma = pltpu.SemaphoreType.DMA
    inputs = (speed, theta, dz, dx, area, flux, tally, region, seam)
    inputs = [pltpu.with_memory_space_constraint(x, pltpu.HBM) for x in inputs]
    rows = [pltpu.VMEM((TIERS, GROUP, COLS), F32)] * 2
    sets = (rows + [pltpu.VMEM((TIERS, 2, 8 * GROUP, 128), F32), pltpu.VMEM((8 * SIDE, 128), F32)]) * 2
    classes, sums = pl.pallas_call(
        kernel,
        out_shape=(
            jax.ShapeDtypeStruct((REGIONS, ROWS, BINS), F32),
            jax.ShapeDtypeStruct((ROWS, 128), F32),
        ),
        in_specs=[any_] * 9,
        out_specs=(vmem, vmem),
        scratch_shapes=[
            pltpu.VMEM((TIERS, ROWS + 8, COLS), F32),
            pltpu.VMEM((TIERS, ROWS, COLS), F32),
            pltpu.VMEM((ROWS, COLS), F32),
            pltpu.VMEM((ROWS, COLS), F32),
            pltpu.VMEM((ROWS, COLS), F32),
            pltpu.VMEM((ROWS + 8, COLS), jnp.int32),
            pltpu.VMEM((ROWS, COLS), jnp.int32),
            pltpu.SMEM((TIERS,), F32),
            pltpu.SMEM((COLS,), jnp.int32),
            *sets,
            pltpu.VMEM((ROWS // 8, REGIONS + 1, 8, 128), F32),
            pltpu.VMEM((2 * 3 * NLON, 8, 128), F32),
            pltpu.VMEM((2 * 3, 8, 128), F32),
            pltpu.VMEM((24, COLS), F32),
            pltpu.VMEM((24, COLS), F32),
            pltpu.VMEM((24, COLS), F32),
            pltpu.VMEM((NLON, 24, COLS), F32),
            *([pltpu.VMEM((8, 128), F32)] * 5),
            pltpu.VMEM((NLON, 8, 128), F32),
            dma((11,)),
            dma, dma((2, 3)), dma, dma,
            dma, dma,
            *([dma] * 8),
        ],
        compiler_params=pltpu.CompilerParams(collective_id=0, has_side_effects=True, vmem_limit_bytes=VMEM_LIMIT),
    )(*inputs)
    out_class, over, heat, impl = pl.pallas_call(
        finish,
        out_shape=(
            jax.ShapeDtypeStruct((REGIONS, ROWS, BINS), F32),
            jax.ShapeDtypeStruct((REGIONS, TIERS, ROWS), F32),
            jax.ShapeDtypeStruct((REGIONS, ROWS), F32),
            jax.ShapeDtypeStruct((REGIONS, ROWS), F32),
        ),
        in_specs=[vmem, vmem],
        out_specs=(vmem,) * 4,
        compiler_params=pltpu.CompilerParams(vmem_limit_bytes=4 * 2**20),
    )(classes, sums)
    return out_class, jnp.transpose(over, (0, 2, 1)), heat, impl


def solution(mesh):
    in_specs = (
        P(None, "lat", "lon"),
        P(None, "lat", "lon"),
        P(),
        P("lat", "lon"),
        P("lat", "lon"),
        P("lat", "lon"),
        P("lat", "lon"),
        P("lat", "lon"),
        P("lon"),
    )
    out_specs = (P(None, "lat", None), P(None, "lat", None), P(None, "lat"), P(None, "lat"))
    return jax.shard_map(body, mesh=mesh, in_specs=in_specs, out_specs=out_specs, check_vma=False)
```

```python
import math

import jax
import jax.numpy as jnp
from jax import lax
from jax.experimental import pallas as pl
from jax.experimental.pallas import tpu as pltpu
from jax.sharding import PartitionSpec as P

BINS = 128
REGIONS = 4
TIERS = 16
ROWS = 64
COLS = 256
NLON = 16
NLAT = 16
GROUP = 8
OWNED = ROWS // NLON
LO = 12
HI = 11
SIDE = REGIONS * LO

HEAT, THETA, WET, FLUX, SOUTH = 64, 68, 69, 72, 76

UNIT = math.sqrt(BINS / (COLS * NLON * TIERS))
IMPLIED = 2.0 / math.sqrt(COLS * NLON * ROWS * NLAT)
VMEM_LIMIT = 32 * 2**20
F32, BF16 = jnp.float32, jnp.bfloat16


def iota(shape, dim):
    return lax.broadcasted_iota(jnp.int32, shape, dim)


def two_terms(x):
    high = x.astype(BF16).astype(F32)
    return high, x - high


def kernel(
    speed_h, theta_h, dz_h, dx_h, area_h, flux_h, tally_h, region_h, seam_h,
    out_class, out_sums,
    th, sp, dx, area, flux, tally, region, dz_s, seam_s,
    hi_a, cl_a, val_a, part_a, hi_b, cl_b, val_b, part_b,
    rs_send, rs_recv, ag_send,
    halo_send, halo_recv, fold_send, fold_recv, own_flux, pair_flux, south_flux, north_flux, offset, offsets,
    in_sem, rs_ssem, rs_rsem, ag_ssem, ag_rsem, fold_ssem, fold_rsem,
    halo_ssem, halo_rsem, pair_ssem, pair_rsem, chain_ssem, chain_rsem, off_ssem, off_rsem,
):
    o = lax.axis_index("lon")
    l = lax.axis_index("lat")
    lane8 = iota((8, 128), 1)
    MESH = pl.DeviceIdType.MESH

    first, rest = pl.ds(0, 24), pl.ds(24, ROWS - 24)
    loads = [
        pltpu.make_async_copy(tally_h, tally.at[pl.ds(0, ROWS)], in_sem.at[3]),
        pltpu.make_async_copy(dx_h, dx, in_sem.at[4]),
        pltpu.make_async_copy(region_h, region, in_sem.at[2]),
        pltpu.make_async_copy(dz_h, dz_s, in_sem.at[9]),
        pltpu.make_async_copy(theta_h.at[:, first], th.at[:, first], in_sem.at[5]),
        pltpu.make_async_copy(speed_h.at[:, first], sp.at[:, first], in_sem.at[6]),
        pltpu.make_async_copy(flux_h, flux, in_sem.at[0]),
        pltpu.make_async_copy(area_h, area, in_sem.at[1]),
        pltpu.make_async_copy(theta_h.at[:, rest], th.at[:, rest], in_sem.at[7]),
        pltpu.make_async_copy(speed_h.at[:, rest], sp.at[:, rest], in_sem.at[8]),
        pltpu.make_async_copy(seam_h, seam_s, in_sem.at[10]),
    ]
    for load in loads:
        load.start()

    barrier = pltpu.get_barrier_semaphore()
    for d in range(1, NLON):
        pl.semaphore_signal(barrier, inc=1, device_id={"lon": lax.rem(o + d, NLON)}, device_id_type=MESH)
    chip, core = lax.div(l, 2), lax.rem(l, 2)
    sibling = l + 1 - 2 * core
    for q in range(NLON):
        pl.semaphore_signal(barrier, inc=1, device_id={"lon": q, "lat": sibling}, device_id_type=MESH)
    near = (l - 2, l + 2, l - 1 + 2 * core)
    for n in near:
        @pl.when(jnp.logical_and(n >= 0, n < NLAT))
        def _():
            pl.semaphore_signal(barrier, inc=1, device_id={"lat": n}, device_id_type=MESH)

    def halo_copy():
        return pltpu.make_async_remote_copy(
            halo_send, halo_recv, halo_ssem, halo_rsem, device_id={"lat": lax.max(l - 1, 0)}, device_id_type=MESH)

    def fold_copy(dst):
        return pltpu.make_async_remote_copy(
            fold_send, fold_recv.at[o], fold_ssem, fold_rsem, device_id={"lon": dst}, device_id_type=MESH)

    def pair_copy():
        return pltpu.make_async_remote_copy(
            own_flux, pair_flux, pair_ssem, pair_rsem, device_id={"lat": sibling}, device_id_type=MESH)

    def down_copy():
        return pltpu.make_async_remote_copy(
            south_flux, pair_flux, pair_ssem, pair_rsem, device_id={"lat": sibling}, device_id_type=MESH)

    def chain_copy():
        return pltpu.make_async_remote_copy(
            north_flux, south_flux, chain_ssem, chain_rsem,
            device_id={"lat": lax.min(l + 2, NLAT - 1)}, device_id_type=MESH)

    def offset_copy(dst):
        return pltpu.make_async_remote_copy(
            offset, offsets.at[o], off_ssem, off_rsem, device_id={"lon": dst}, device_id_type=MESH)

    def chain_step(turn):
        @pl.when(jnp.logical_and(turn, core == 1))
        def _():
            pair_copy().wait_recv()

            @pl.when(chip > 0)
            def _():
                chain_copy().wait_recv()
                down_copy().start()

            @pl.when(chip < NLAT // 2 - 1)
            def _():
                north_flux[...] = south_flux[...] + own_flux[...] + pair_flux[...]
                chain_copy().start()

    def owner(g, t):
        turn = lax.rem(g if t < REGIONS else g + 3, 4)
        late = lax.div(g, 4)
        high, low = (t // 2, t % 2) if t < REGIONS else (1 - late, 1 - late)
        x = high + 2 * (1 - lax.rem(turn, 2))
        y = jnp.where(turn >= 2, 3 * low, 1 + low)
        return 4 * x + y, (late if t < REGIONS else 2)

    def rs_copy(g, t):
        dst, slot = owner(g, t)
        return pltpu.make_async_remote_copy(
            rs_send.at[g, t], rs_recv.at[(3 * core + slot) * NLON + o], rs_ssem, rs_rsem.at[core, slot],
            device_id={"lon": dst, "lat": 2 * chip + 1}, device_id_type=MESH)

    def remote_tile(g, t):
        dst, _ = owner(g, t)
        return jnp.logical_or(core == 0, dst != o)

    x_own, y_own = lax.div(o, 4), lax.rem(o, 4)
    outer = jnp.where(jnp.logical_or(y_own == 0, y_own == 3), 1, 0)
    turn = 2 * outer + jnp.where(x_own < 2, 1, 0)
    b_own = 2 * lax.rem(x_own, 2) + jnp.where(y_own >= 2, 1, 0)
    peers = (0, 4, 1, 5, 8, 12, 2, 9, 3, 6, 13, 7, 10, 11, 14, 15)

    def to_peers(act, all_of_them=False):
        for q in peers:
            if all_of_them:
                act(q)
            else:
                @pl.when(o != q)
                def _():
                    act(q)

    def landed(ref, sem):
        pltpu.make_async_copy(ref, ref, sem).wait()

    def flux_totals():
        acc = [jnp.zeros((8, COLS), F32) for _ in range(REGIONS)]
        for g in range(ROWS // 8):
            rows = slice(8 * g, 8 * g + 8)
            f = flux[rows, :] * area[rows, :]
            reg = region[rows, :]
            for b in range(REGIONS):
                acc[b] = acc[b] + jnp.where(reg == b, f, 0.0)
        totals = jnp.zeros((8, 128), F32)
        for b in range(REGIONS):
            t = jnp.sum(jnp.sum(acc[b], axis=0, keepdims=True), axis=1, keepdims=True)
            totals = jnp.where(lane8 == SOUTH + b, t, totals)
        own_flux[...] = totals

        @pl.when(chip == 0)
        def _():
            south_flux[...] = jnp.zeros((8, 128), F32)

            @pl.when(core == 0)
            def _():
                pair_flux[...] = jnp.zeros((8, 128), F32)

    def edge_rows():
        for k in range(TIERS):
            halo_send[k : k + 1, :] = th[k, 0:1, :]
            fold_send[k : k + 1, :] = th[k, ROWS - 1 : ROWS, :]
        halo_send[TIERS:24, :] = jnp.broadcast_to(tally[0:1, :].astype(F32), (8, COLS))
        fold_send[TIERS:24, :] = jnp.broadcast_to(tally[ROWS - 1 : ROWS, :].astype(F32), (8, COLS))

    def first_sends():
        known = 2 * NLON - 1
        for n in near:
            known = known + jnp.where(jnp.logical_and(n >= 0, n < NLAT), 1, 0)
        pl.semaphore_wait(barrier, known)

        @pl.when(core == 0)
        def _():
            pair_copy().start()

        @pl.when(l == NLAT - 1)
        def _():
            to_peers(lambda q: fold_copy(q).start())
            fold_recv[o] = fold_send[...]

        @pl.when(l > 0)
        def _():
            halo_copy().start()

    def put_north():
        for k in range(TIERS):
            th[k, ROWS : ROWS + 1, :] = halo_recv[k : k + 1, :]
        tally[ROWS : ROWS + 1, :] = halo_recv[TIERS : TIERS + 1, :].astype(jnp.int32)

    def north_row():
        halo_copy().wait_recv()
        put_north()

    def fold_row():
        landed(fold_recv.at[pl.ds(0, NLON - 1)], fold_rsem)
        first = seam_s[0]
        source = lax.shift_right_logical(first, 8)
        at = jnp.bitwise_and(first, COLS - 1)
        high = fold_recv[source]
        low = fold_recv[jnp.bitwise_and(source + NLON - 1, NLON - 1)]
        for t in range(COLS // 128):
            i = lane8 + 128 * t
            spot = jnp.bitwise_and(at - i, COLS - 1)
            lane = jnp.bitwise_and(spot, 127)
            for r in range(3):
                rows = slice(8 * r, 8 * r + 8)
                pick = [
                    jnp.where(
                        spot >= 128,
                        jnp.take_along_axis(src[rows, 128:], lane, axis=1),
                        jnp.take_along_axis(src[rows, :128], lane, axis=1),
                    )
                    for src in (high, low)
                ]
                halo_recv[rows, 128 * t : 128 * t + 128] = jnp.where(i <= at, pick[0], pick[1])
        put_north()

    sub8 = iota((8, COLS), 0)
    hi_iota = lax.shift_right_logical(iota((SIDE, COLS), 0), 2).astype(F32).astype(BF16)
    cl_iota = iota((SIDE, COLS), 0).astype(F32).astype(BF16)
    zero = jnp.zeros((SIDE, COLS), BF16)
    one = jnp.ones((SIDE, COLS), BF16)

    def prepare(g, hi_r, cl_r, val_r):
        base = g * GROUP if isinstance(g, int) else pl.multiple_of(g * GROUP, GROUP)
        here = pl.ds(base, GROUP)
        nxt = pl.ds(base + GROUP, 1)
        deep = tally[here, :]
        face_depth = jnp.minimum(deep, jnp.where(sub8 == 7, tally[nxt, :], pltpu.roll(deep, 7, 0)))
        width = dx[here, :]
        reg = region[here, :]
        regf = reg.astype(F32) * LO
        member = [reg == b for b in range(REGIONS)]
        heat = theta_sum = wet_sum = jnp.zeros((8, COLS), F32)
        stats = jnp.zeros((8, 128), F32)
        for k in range(TIERS):
            t = th[k, here, :]
            face = 0.5 * (t + jnp.where(sub8 == 7, th[k, nxt, :], pltpu.roll(t, 7, 0)))
            vol = jnp.where(face_depth > k, dz_s[k] * width, 0.0)
            mass = vol * sp[k, here, :]
            pos = jnp.clip((face - (-2.0)) * (BINS / 32.0), 0.0, BINS - 1.0)
            low = jnp.minimum(jnp.floor(pos), BINS - 2.0)
            hi = jnp.floor((low + 0.5) * (1.0 / LO))
            hi_r[k] = hi
            cl_r[k] = (low - hi * LO) + regf
            for n, x in enumerate(two_terms(mass) + two_terms(mass * (pos - low))):
                for half in range(2):
                    val_r[k, half, pl.ds(n, 8, stride=8), :] = x[:, 128 * half : 128 * half + 128]
                    val_r[k, half, pl.ds(n + 4, 8, stride=8), :] = x[:, 128 * half : 128 * half + 128]
            heat = heat + mass * face
            theta_sum = theta_sum + vol * face
            wet_sum = wet_sum + vol
            for b in range(REGIONS):
                red = jnp.sum(jnp.where(member[b], mass, 0.0), axis=1, keepdims=True)
                stats = jnp.where(lane8 == b * TIERS + k, red, stats)
            yield
        f = flux[here, :] * area[here, :]
        for b in range(REGIONS):
            red = jnp.sum(jnp.where(member[b], heat, 0.0), axis=1, keepdims=True)
            stats = jnp.where(lane8 == HEAT + b, red, stats)
            red = jnp.sum(jnp.where(member[b], f, 0.0), axis=1, keepdims=True)
            stats = jnp.where(lane8 == FLUX + b, red, stats)
        stats = jnp.where(lane8 == THETA, jnp.sum(theta_sum, axis=1, keepdims=True), stats)
        stats = jnp.where(lane8 == WET, jnp.sum(wet_sum, axis=1, keepdims=True), stats)
        rs_send[g, REGIONS] = stats
        yield

    def bin_rows(hi_r, cl_r, val_r, part_r):
        for jj in range(GROUP):
            total = None
            for k in range(TIERS):
                hi = jnp.broadcast_to(hi_r[k, jj : jj + 1, :], (SIDE, COLS)).astype(BF16)
                cl = jnp.broadcast_to(cl_r[k, jj : jj + 1, :], (SIDE, COLS)).astype(BF16)
                val = jnp.concatenate([val_r[k, half, 8 * jj : 8 * jj + 8, :] for half in range(2)], axis=1)
                val = jnp.concatenate([val] * (SIDE // 8), axis=0).astype(BF16)
                lhs = jnp.where(hi == hi_iota, val, zero)
                rhs = jnp.where(cl == cl_iota, one, zero)
                d = lax.dot_general(lhs, rhs, (((1,), (1,)), ((), ())), preferred_element_type=F32)
                total = d if total is None else total + d
            part_r[pl.ds(jj, SIDE, stride=8), 0:SIDE] = total
            yield

    bin_lane = lax.rem(lane8, LO)
    bin_block = lax.div(lane8, LO)

    def arrange(g, part_r):
        s0 = [jnp.zeros((8, 128), F32)] * REGIONS
        s1 = [jnp.zeros((8, 128), F32)] * REGIONS
        for hi in range(HI):
            rows = [part_r[32 * hi + 8 * n : 32 * hi + 8 * n + 8, :] for n in range(4)]
            wx = rows[2] + rows[3]
            x = rows[0] + rows[1] - wx
            for b in range(REGIONS):
                at = bin_lane + LO * b
                s0[b] = jnp.where(bin_block == hi, jnp.take_along_axis(x, at, axis=1), s0[b])
                s1[b] = jnp.where(bin_block == hi, jnp.take_along_axis(wx, at, axis=1), s1[b])
            yield
        for b in range(REGIONS):
            rs_send[g, b] = s0[b] + jnp.where(lane8 == 0, 0.0, pltpu.roll(s1[b], 1, 1))
        yield

    def together(*parts):
        parts = [p for p in parts if p is not None]
        done = object()
        lead, rest = parts[0], parts[1:]
        per = [2] * len(rest)
        while next(lead, done) is not done:
            for p, n in zip(rest, per):
                for _ in range(n):
                    next(p, done)
        for p in rest:
            while next(p, done) is not done:
                pass

    def send(g):
        for t in range(REGIONS + 1):
            @pl.when(remote_tile(g, t))
            def _():
                rs_copy(g, t).start()

    set_a = (hi_a, cl_a, val_a)
    set_b = (hi_b, cl_b, val_b)

    for load in loads[:8]:
        load.wait()
    together(prepare(0, *set_a))

    def pair(i, carry):
        g = 2 * i
        together(bin_rows(*set_a, part_a), prepare(g + 1, *set_b), arrange(lax.max(g - 1, 0), part_b))

        @pl.when(i == 0)
        def _():
            for load in loads[8:]:
                load.wait()
            flux_totals()
            edge_rows()
            first_sends()

        chain_step(jnp.logical_and(i > 0, chip == 2 * i - 1))

        @pl.when(i > 0)
        def _():
            send(g - 1)
        together(bin_rows(*set_b, part_b), prepare(g + 2, *set_a), arrange(g, part_a))

        chain_step(chip == 2 * i)
        send(g)
        return carry

    lax.fori_loop(0, 3, pair, 0)
    @pl.when(l < NLAT - 1)
    def _():
        north_row()
        together(bin_rows(*set_a, part_a), prepare(7, *set_b), arrange(5, part_b))

    @pl.when(l == NLAT - 1)
    def _():
        together(bin_rows(*set_a, part_a), arrange(5, part_b))
        fold_row()
        together(prepare(7, *set_b))
    send(5)
    chain_step(chip == 5)
    together(bin_rows(*set_b, part_b), arrange(6, part_a))
    send(6)

    together(arrange(7, part_b))
    send(7)

    chain_step(chip >= 6)

    @pl.when(jnp.logical_and(core == 0, chip > 0))
    def _():
        down_copy().wait_recv()
    offset[...] = pair_flux[...] + jnp.where(core == 1, south_flux[...], 0.0)
    to_peers(lambda q: offset_copy(q).start())

    tiles = NLON * 2 + NLON // 2

    def owned(slot, g, t, scale, put):
        for c in (0, 1):
            at = 3 * c + slot
            landed(rs_recv.at[pl.ds(0, NLON - c)], rs_rsem.at[c, slot])
            parts = [rs_recv[at * NLON + q] for q in range(NLON)]
            if c == 1:
                parts = [jnp.where(q != o, p, 0.0) for q, p in enumerate(parts)] + [rs_send[g, t]]
            while len(parts) > 1:
                parts = [sum(parts[i : i + 2]) for i in range(0, len(parts), 2)]
            ag_send[at] = parts[0] * scale
            to = put(slot, g)
            to_peers(lambda q: pltpu.make_async_remote_copy(
                ag_send.at[at], to, ag_ssem, ag_rsem,
                device_id={"lon": q, "lat": 2 * chip + c}, device_id_type=MESH).start(), c == 0)
        to[...] = ag_send[at]

    def put_class(slot, g):
        return out_class.at[b_own, pl.ds(pl.multiple_of(8 * g, 8), 8)]

    def put_sums(slot, g):
        return out_sums.at[pl.ds(pl.multiple_of(8 * g, 8), 8)]

    has_sums = jnp.logical_or(b_own == 0, b_own == 3)
    no_sums = jnp.logical_not(has_sums)
    g_sum = lax.rem(turn + 1, 4) + jnp.where(b_own == 0, 4, 0)

    @pl.when(core == 1)
    def _():
        owned(0, turn, b_own, UNIT, put_class)

        @pl.when(jnp.logical_and(has_sums, g_sum < 7))
        def _():
            owned(2, g_sum, REGIONS, 1.0, put_sums)
        owned(1, 4 + turn, b_own, UNIT, put_class)

        @pl.when(jnp.logical_and(has_sums, g_sum == 7))
        def _():
            owned(2, g_sum, REGIONS, 1.0, put_sums)

    @pl.when(core == 0)
    def _():
        landed(rs_recv.at[pl.ds(0, tiles)], rs_ssem)
        pair_copy().wait_send()

    @pl.when(core == 1)
    def _():
        @pl.when(has_sums)
        def _():
            landed(rs_recv.at[pl.ds(0, tiles - 3)], rs_ssem)
            landed(rs_recv.at[pl.ds(0, 3 * (2 * NLON - 1))], ag_ssem)

        @pl.when(no_sums)
        def _():
            landed(rs_recv.at[pl.ds(0, tiles - 2)], rs_ssem)
            landed(rs_recv.at[pl.ds(0, 2 * (2 * NLON - 1))], ag_ssem)

        @pl.when(chip > 0)
        def _():
            pair_copy().wait_send()

        @pl.when(chip < NLAT // 2 - 1)
        def _():
            chain_copy().wait_send()

    landed(rs_recv.at[pl.ds(0, NLON - 1)], off_ssem)

    @pl.when(l > 0)
    def _():
        halo_copy().wait_send()

    @pl.when(l == NLAT - 1)
    def _():
        landed(fold_recv.at[pl.ds(0, NLON - 1)], fold_ssem)

    landed(offsets.at[pl.ds(0, NLON - 1)], off_rsem)
    south = offset[...]
    for q in range(NLON):
        south = south + jnp.where(q != o, offsets[q], 0.0)

    @pl.when(core == 0)
    def _():
        landed(rs_recv.at[pl.ds(0, tiles)], ag_rsem)

    @pl.when(core == 1)
    def _():
        @pl.when(has_sums)
        def _():
            landed(rs_recv.at[pl.ds(0, tiles - 3)], ag_rsem)

        @pl.when(no_sums)
        def _():
            landed(rs_recv.at[pl.ds(0, tiles - 2)], ag_rsem)
    out_sums[ROWS - 8 : ROWS, :] = out_sums[ROWS - 8 : ROWS, :] + south


def finish(classes, sums, out_class, out_over, out_heat, out_impl):
    out_class[...] = classes[...]
    row, lane = iota((88, 128), 0), iota((88, 128), 1)
    upto = (row < HEAT) & (lane <= row) & (lax.div(lane, TIERS) == lax.div(row, TIERS))
    volume = (row >= HEAT) & (row < HEAT + 4) & (lax.div(lane, TIERS) == row - HEAT)
    same = (row >= 72) & (lane == row - 8)
    pick = jnp.where(upto | volume | same, 1.0, 0.0)
    res = lax.dot_general(
        pick, sums[...], (((1,), (1,)), ((), ())), precision=lax.Precision.HIGHEST, preferred_element_type=F32)
    for b in range(REGIONS):
        out_over[b] = UNIT * res[TIERS * b : TIERS * b + TIERS]
    at = HEAT + 8
    mean = res[at + 4 : at + 5] / res[at + 5 : at + 6]
    out_heat[...] = (UNIT / 16.0) * (res[at : at + 4] - res[HEAT : HEAT + 4] * mean)
    flux = res[FLUX + 8 : FLUX + 16]
    south_of = jnp.where(iota((ROWS, ROWS), 0) <= iota((ROWS, ROWS), 1), 1.0, 0.0)
    c = jnp.dot(flux, south_of, precision=lax.Precision.HIGHEST, preferred_element_type=F32)
    out_impl[...] = IMPLIED * (c[0:4] + flux[4:8, ROWS - 1 : ROWS])


def body(speed, theta, dz, dx, area, flux, tally, region, seam):
    any_ = pl.BlockSpec(memory_space=pltpu.HBM)
    vmem = pl.BlockSpec(memory_space=pltpu.VMEM)
    dma = pltpu.SemaphoreType.DMA
    inputs = (speed, theta, dz, dx, area, flux, tally, region, seam)
    inputs = [pltpu.with_memory_space_constraint(x, pltpu.HBM) for x in inputs]
    rows = [pltpu.VMEM((TIERS, GROUP, COLS), F32)] * 2
    sets = (rows + [pltpu.VMEM((TIERS, 2, 8 * GROUP, 128), F32), pltpu.VMEM((8 * SIDE, 128), F32)]) * 2
    classes, sums = pl.pallas_call(
        kernel,
        out_shape=(
            jax.ShapeDtypeStruct((REGIONS, ROWS, BINS), F32),
            jax.ShapeDtypeStruct((ROWS, 128), F32),
        ),
        in_specs=[any_] * 9,
        out_specs=(vmem, vmem),
        scratch_shapes=[
            pltpu.VMEM((TIERS, ROWS + 8, COLS), F32),
            pltpu.VMEM((TIERS, ROWS, COLS), F32),
            pltpu.VMEM((ROWS, COLS), F32),
            pltpu.VMEM((ROWS, COLS), F32),
            pltpu.VMEM((ROWS, COLS), F32),
            pltpu.VMEM((ROWS + 8, COLS), jnp.int32),
            pltpu.VMEM((ROWS, COLS), jnp.int32),
            pltpu.SMEM((TIERS,), F32),
            pltpu.SMEM((COLS,), jnp.int32),
            *sets,
            pltpu.VMEM((ROWS // 8, REGIONS + 1, 8, 128), F32),
            pltpu.VMEM((2 * 3 * NLON, 8, 128), F32),
            pltpu.VMEM((2 * 3, 8, 128), F32),
            pltpu.VMEM((24, COLS), F32),
            pltpu.VMEM((24, COLS), F32),
            pltpu.VMEM((24, COLS), F32),
            pltpu.VMEM((NLON, 24, COLS), F32),
            *([pltpu.VMEM((8, 128), F32)] * 5),
            pltpu.VMEM((NLON, 8, 128), F32),
            dma((11,)),
            dma, dma((2, 3)), dma, dma,
            dma, dma,
            *([dma] * 8),
        ],
        compiler_params=pltpu.CompilerParams(collective_id=0, has_side_effects=True, vmem_limit_bytes=VMEM_LIMIT),
    )(*inputs)
    out_class, over, heat, impl = pl.pallas_call(
        finish,
        out_shape=(
            jax.ShapeDtypeStruct((REGIONS, ROWS, BINS), F32),
            jax.ShapeDtypeStruct((REGIONS, TIERS, ROWS), F32),
            jax.ShapeDtypeStruct((REGIONS, ROWS), F32),
            jax.ShapeDtypeStruct((REGIONS, ROWS), F32),
        ),
        in_specs=[vmem, vmem],
        out_specs=(vmem,) * 4,
        compiler_params=pltpu.CompilerParams(vmem_limit_bytes=4 * 2**20),
    )(classes, sums)
    return out_class, jnp.transpose(over, (0, 2, 1)), heat, impl


def solution(mesh):
    in_specs = (
        P(None, "lat", "lon"),
        P(None, "lat", "lon"),
        P(),
        P("lat", "lon"),
        P("lat", "lon"),
        P("lat", "lon"),
        P("lat", "lon"),
        P("lat", "lon"),
        P("lon"),
    )
    out_specs = (P(None, "lat", None), P(None, "lat", None), P(None, "lat"), P(None, "lat"))
    return jax.shard_map(body, mesh=mesh, in_specs=in_specs, out_specs=out_specs, check_vma=False)
```

```python
import math

import jax
import jax.numpy as jnp
from jax import lax
from jax.experimental import pallas as pl
from jax.experimental.pallas import tpu as pltpu
from jax.sharding import PartitionSpec as P

BINS = 128
REGIONS = 4
TIERS = 16
ROWS = 64
COLS = 256
NLON = 16
NLAT = 16
GROUP = 8
OWNED = ROWS // NLON
LO = 12
HI = 11
SIDE = REGIONS * LO

HEAT, THETA, WET, FLUX, SOUTH = 64, 68, 69, 72, 76

UNIT = math.sqrt(BINS / (COLS * NLON * TIERS))
IMPLIED = 2.0 / math.sqrt(COLS * NLON * ROWS * NLAT)
VMEM_LIMIT = 32 * 2**20
F32, BF16 = jnp.float32, jnp.bfloat16


def iota(shape, dim):
    return lax.broadcasted_iota(jnp.int32, shape, dim)


def two_terms(x):
    high = x.astype(BF16).astype(F32)
    return high, x - high


def kernel(
    speed_h, theta_h, dz_h, dx_h, area_h, flux_h, tally_h, region_h, seam_h,
    out_class, out_sums,
    th, sp, dx, area, flux, tally, region, dz_s, seam_s,
    hi_a, cl_a, val_a, part_a, hi_b, cl_b, val_b, part_b,
    rs_send, rs_recv, ag_send,
    halo_send, halo_recv, fold_send, fold_recv, own_flux, pair_flux, south_flux, north_flux, offset, offsets,
    in_sem, rs_ssem, rs_rsem, ag_ssem, ag_rsem, fold_ssem, fold_rsem,
    halo_ssem, halo_rsem, pair_ssem, pair_rsem, chain_ssem, chain_rsem, off_ssem, off_rsem,
):
    o = lax.axis_index("lon")
    l = lax.axis_index("lat")
    lane8 = iota((8, 128), 1)
    MESH = pl.DeviceIdType.MESH

    first, rest = pl.ds(0, 24), pl.ds(24, ROWS - 24)
    loads = [
        pltpu.make_async_copy(tally_h, tally.at[pl.ds(0, ROWS)], in_sem.at[3]),
        pltpu.make_async_copy(dx_h, dx, in_sem.at[4]),
        pltpu.make_async_copy(region_h, region, in_sem.at[2]),
        pltpu.make_async_copy(dz_h, dz_s, in_sem.at[9]),
        pltpu.make_async_copy(theta_h.at[:, first], th.at[:, first], in_sem.at[5]),
        pltpu.make_async_copy(speed_h.at[:, first], sp.at[:, first], in_sem.at[6]),
        pltpu.make_async_copy(flux_h, flux, in_sem.at[0]),
        pltpu.make_async_copy(area_h, area, in_sem.at[1]),
        pltpu.make_async_copy(theta_h.at[:, rest], th.at[:, rest], in_sem.at[7]),
        pltpu.make_async_copy(speed_h.at[:, rest], sp.at[:, rest], in_sem.at[8]),
        pltpu.make_async_copy(seam_h, seam_s, in_sem.at[10]),
    ]
    for load in loads:
        load.start()

    barrier = pltpu.get_barrier_semaphore()
    for d in range(1, NLON):
        pl.semaphore_signal(barrier, inc=1, device_id={"lon": lax.rem(o + d, NLON)}, device_id_type=MESH)
    chip, core = lax.div(l, 2), lax.rem(l, 2)
    sibling = l + 1 - 2 * core
    for q in range(NLON):
        pl.semaphore_signal(barrier, inc=1, device_id={"lon": q, "lat": sibling}, device_id_type=MESH)
    near = (l - 2, l + 2, l - 1 + 2 * core)
    for n in near:
        @pl.when(jnp.logical_and(n >= 0, n < NLAT))
        def _():
            pl.semaphore_signal(barrier, inc=1, device_id={"lat": n}, device_id_type=MESH)

    def halo_copy():
        return pltpu.make_async_remote_copy(
            halo_send, halo_recv, halo_ssem, halo_rsem, device_id={"lat": lax.max(l - 1, 0)}, device_id_type=MESH)

    def fold_copy(dst):
        return pltpu.make_async_remote_copy(
            fold_send, fold_recv.at[o], fold_ssem, fold_rsem, device_id={"lon": dst}, device_id_type=MESH)

    def pair_copy():
        return pltpu.make_async_remote_copy(
            own_flux, pair_flux, pair_ssem, pair_rsem, device_id={"lat": sibling}, device_id_type=MESH)

    def down_copy():
        return pltpu.make_async_remote_copy(
            south_flux, pair_flux, pair_ssem, pair_rsem, device_id={"lat": sibling}, device_id_type=MESH)

    def chain_copy():
        return pltpu.make_async_remote_copy(
            north_flux, south_flux, chain_ssem, chain_rsem,
            device_id={"lat": lax.min(l + 2, NLAT - 1)}, device_id_type=MESH)

    def offset_copy(dst):
        return pltpu.make_async_remote_copy(
            offset, offsets.at[o], off_ssem, off_rsem, device_id={"lon": dst}, device_id_type=MESH)

    def chain_step(turn):
        @pl.when(jnp.logical_and(turn, core == 1))
        def _():
            pair_copy().wait_recv()

            @pl.when(chip > 0)
            def _():
                chain_copy().wait_recv()
                down_copy().start()

            @pl.when(chip < NLAT // 2 - 1)
            def _():
                north_flux[...] = south_flux[...] + own_flux[...] + pair_flux[...]
                chain_copy().start()

    def owner(g, t):
        turn = lax.rem(g if t < REGIONS else g + 3, 4)
        wide_x, wide_y = lax.div(turn, 2), lax.rem(turn, 2)
        late = lax.div(g, 4)
        b = t if t < REGIONS else 3 * (1 - late)
        x, y = (b // 2, b % 2) if t < REGIONS else (1 - late, 1 - late)
        x = jnp.where(wide_x == 1, 3 * x, 1 + x)
        y = jnp.where(wide_y == 1, 3 * y, 1 + y)
        return 4 * x + y, (late if t < REGIONS else 2)

    def rs_copy(g, t):
        dst, slot = owner(g, t)
        return pltpu.make_async_remote_copy(
            rs_send.at[g, t], rs_recv.at[(3 * core + slot) * NLON + o], rs_ssem, rs_rsem.at[core, slot],
            device_id={"lon": dst, "lat": 2 * chip + 1}, device_id_type=MESH)

    def remote_tile(g, t):
        dst, _ = owner(g, t)
        return jnp.logical_or(core == 0, dst != o)

    x_own, y_own = lax.div(o, 4), lax.rem(o, 4)
    wide = [jnp.where(jnp.logical_or(v == 0, v == 3), 1, 0) for v in (x_own, y_own)]
    turn = 2 * wide[0] + wide[1]
    b_own = 2 * jnp.where(x_own >= 2, 1, 0) + jnp.where(y_own >= 2, 1, 0)
    peers = (0, 4, 1, 5, 8, 12, 2, 9, 3, 6, 13, 7, 10, 11, 14, 15)

    def to_peers(act, all_of_them=False):
        for q in peers:
            if all_of_them:
                act(q)
            else:
                @pl.when(o != q)
                def _():
                    act(q)

    def landed(ref, sem):
        pltpu.make_async_copy(ref, ref, sem).wait()

    def flux_totals():
        acc = [jnp.zeros((8, COLS), F32) for _ in range(REGIONS)]
        for g in range(ROWS // 8):
            rows = slice(8 * g, 8 * g + 8)
            f = flux[rows, :] * area[rows, :]
            reg = region[rows, :]
            for b in range(REGIONS):
                acc[b] = acc[b] + jnp.where(reg == b, f, 0.0)
        totals = jnp.zeros((8, 128), F32)
        for b in range(REGIONS):
            t = jnp.sum(jnp.sum(acc[b], axis=0, keepdims=True), axis=1, keepdims=True)
            totals = jnp.where(lane8 == SOUTH + b, t, totals)
        own_flux[...] = totals

        @pl.when(chip == 0)
        def _():
            south_flux[...] = jnp.zeros((8, 128), F32)

            @pl.when(core == 0)
            def _():
                pair_flux[...] = jnp.zeros((8, 128), F32)

    def edge_rows():
        for k in range(TIERS):
            halo_send[k : k + 1, :] = th[k, 0:1, :]
            fold_send[k : k + 1, :] = th[k, ROWS - 1 : ROWS, :]
        halo_send[TIERS:24, :] = jnp.broadcast_to(tally[0:1, :].astype(F32), (8, COLS))
        fold_send[TIERS:24, :] = jnp.broadcast_to(tally[ROWS - 1 : ROWS, :].astype(F32), (8, COLS))

    def first_sends():
        known = 2 * NLON - 1
        for n in near:
            known = known + jnp.where(jnp.logical_and(n >= 0, n < NLAT), 1, 0)
        pl.semaphore_wait(barrier, known)

        @pl.when(core == 0)
        def _():
            pair_copy().start()

        @pl.when(l == NLAT - 1)
        def _():
            to_peers(lambda q: fold_copy(q).start())
            fold_recv[o] = fold_send[...]

        @pl.when(l > 0)
        def _():
            halo_copy().start()

    def put_north():
        for k in range(TIERS):
            th[k, ROWS : ROWS + 1, :] = halo_recv[k : k + 1, :]
        tally[ROWS : ROWS + 1, :] = halo_recv[TIERS : TIERS + 1, :].astype(jnp.int32)

    def north_row():
        halo_copy().wait_recv()
        put_north()

    def fold_row():
        landed(fold_recv.at[pl.ds(0, NLON - 1)], fold_rsem)
        first = seam_s[0]
        source = lax.shift_right_logical(first, 8)
        at = jnp.bitwise_and(first, COLS - 1)
        high = fold_recv[source]
        low = fold_recv[jnp.bitwise_and(source + NLON - 1, NLON - 1)]
        for t in range(COLS // 128):
            i = lane8 + 128 * t
            spot = jnp.bitwise_and(at - i, COLS - 1)
            lane = jnp.bitwise_and(spot, 127)
            for r in range(3):
                rows = slice(8 * r, 8 * r + 8)
                pick = [
                    jnp.where(
                        spot >= 128,
                        jnp.take_along_axis(src[rows, 128:], lane, axis=1),
                        jnp.take_along_axis(src[rows, :128], lane, axis=1),
                    )
                    for src in (high, low)
                ]
                halo_recv[rows, 128 * t : 128 * t + 128] = jnp.where(i <= at, pick[0], pick[1])
        put_north()

    sub8 = iota((8, COLS), 0)
    hi_iota = lax.shift_right_logical(iota((SIDE, COLS), 0), 2).astype(F32).astype(BF16)
    cl_iota = iota((SIDE, COLS), 0).astype(F32).astype(BF16)
    zero = jnp.zeros((SIDE, COLS), BF16)
    one = jnp.ones((SIDE, COLS), BF16)

    def prepare(g, hi_r, cl_r, val_r):
        base = g * GROUP if isinstance(g, int) else pl.multiple_of(g * GROUP, GROUP)
        here = pl.ds(base, GROUP)
        nxt = pl.ds(base + GROUP, 1)
        deep = tally[here, :]
        face_depth = jnp.minimum(deep, jnp.where(sub8 == 7, tally[nxt, :], pltpu.roll(deep, 7, 0)))
        width = dx[here, :]
        reg = region[here, :]
        regf = reg.astype(F32) * LO
        member = [reg == b for b in range(REGIONS)]
        heat = theta_sum = wet_sum = jnp.zeros((8, COLS), F32)
        stats = jnp.zeros((8, 128), F32)
        for k in range(TIERS):
            t = th[k, here, :]
            face = 0.5 * (t + jnp.where(sub8 == 7, th[k, nxt, :], pltpu.roll(t, 7, 0)))
            vol = jnp.where(face_depth > k, dz_s[k] * width, 0.0)
            mass = vol * sp[k, here, :]
            pos = jnp.clip((face - (-2.0)) * (BINS / 32.0), 0.0, BINS - 1.0)
            low = jnp.minimum(jnp.floor(pos), BINS - 2.0)
            hi = jnp.floor((low + 0.5) * (1.0 / LO))
            hi_r[k] = hi
            cl_r[k] = (low - hi * LO) + regf
            for n, x in enumerate(two_terms(mass) + two_terms(mass * (pos - low))):
                for half in range(2):
                    val_r[k, half, pl.ds(n, 8, stride=8), :] = x[:, 128 * half : 128 * half + 128]
                    val_r[k, half, pl.ds(n + 4, 8, stride=8), :] = x[:, 128 * half : 128 * half + 128]
            heat = heat + mass * face
            theta_sum = theta_sum + vol * face
            wet_sum = wet_sum + vol
            for b in range(REGIONS):
                red = jnp.sum(jnp.where(member[b], mass, 0.0), axis=1, keepdims=True)
                stats = jnp.where(lane8 == b * TIERS + k, red, stats)
            yield
        f = flux[here, :] * area[here, :]
        for b in range(REGIONS):
            red = jnp.sum(jnp.where(member[b], heat, 0.0), axis=1, keepdims=True)
            stats = jnp.where(lane8 == HEAT + b, red, stats)
            red = jnp.sum(jnp.where(member[b], f, 0.0), axis=1, keepdims=True)
            stats = jnp.where(lane8 == FLUX + b, red, stats)
        stats = jnp.where(lane8 == THETA, jnp.sum(theta_sum, axis=1, keepdims=True), stats)
        stats = jnp.where(lane8 == WET, jnp.sum(wet_sum, axis=1, keepdims=True), stats)
        rs_send[g, REGIONS] = stats
        yield

    def bin_rows(hi_r, cl_r, val_r, part_r):
        for jj in range(GROUP):
            total = None
            for k in range(TIERS):
                hi = jnp.broadcast_to(hi_r[k, jj : jj + 1, :], (SIDE, COLS)).astype(BF16)
                cl = jnp.broadcast_to(cl_r[k, jj : jj + 1, :], (SIDE, COLS)).astype(BF16)
                val = jnp.concatenate([val_r[k, half, 8 * jj : 8 * jj + 8, :] for half in range(2)], axis=1)
                val = jnp.concatenate([val] * (SIDE // 8), axis=0).astype(BF16)
                lhs = jnp.where(hi == hi_iota, val, zero)
                rhs = jnp.where(cl == cl_iota, one, zero)
                d = lax.dot_general(lhs, rhs, (((1,), (1,)), ((), ())), preferred_element_type=F32)
                total = d if total is None else total + d
            part_r[pl.ds(jj, SIDE, stride=8), 0:SIDE] = total
            yield

    bin_lane = lax.rem(lane8, LO)
    bin_block = lax.div(lane8, LO)

    def arrange(g, part_r):
        s0 = [jnp.zeros((8, 128), F32)] * REGIONS
        s1 = [jnp.zeros((8, 128), F32)] * REGIONS
        for hi in range(HI):
            rows = [part_r[32 * hi + 8 * n : 32 * hi + 8 * n + 8, :] for n in range(4)]
            wx = rows[2] + rows[3]
            x = rows[0] + rows[1] - wx
            for b in range(REGIONS):
                at = bin_lane + LO * b
                s0[b] = jnp.where(bin_block == hi, jnp.take_along_axis(x, at, axis=1), s0[b])
                s1[b] = jnp.where(bin_block == hi, jnp.take_along_axis(wx, at, axis=1), s1[b])
            yield
        for b in range(REGIONS):
            rs_send[g, b] = s0[b] + jnp.where(lane8 == 0, 0.0, pltpu.roll(s1[b], 1, 1))
        yield

    def together(*parts):
        parts = [p for p in parts if p is not None]
        done = object()
        lead, rest = parts[0], parts[1:]
        per = [2] * len(rest)
        while next(lead, done) is not done:
            for p, n in zip(rest, per):
                for _ in range(n):
                    next(p, done)
        for p in rest:
            while next(p, done) is not done:
                pass

    def send(g):
        for t in range(REGIONS + 1):
            @pl.when(remote_tile(g, t))
            def _():
                rs_copy(g, t).start()

    set_a = (hi_a, cl_a, val_a)
    set_b = (hi_b, cl_b, val_b)

    for load in loads[:8]:
        load.wait()
    together(prepare(0, *set_a))

    fold_early = (l == NLAT - 1) & (x_own >= 2) & (y_own >= 2)

    def pair(i, carry):
        g = 2 * i
        together(bin_rows(*set_a, part_a), prepare(g + 1, *set_b), arrange(lax.max(g - 1, 0), part_b))

        @pl.when(i == 0)
        def _():
            for load in loads[8:]:
                load.wait()
            flux_totals()
            edge_rows()

        @pl.when(jnp.logical_and(i == 0, fold_early))
        def _():
            first_sends()

        chain_step(jnp.logical_and(i > 0, chip == 2 * i - 2))

        @pl.when(i > 0)
        def _():
            send(g - 1)
        together(bin_rows(*set_b, part_b), prepare(g + 2, *set_a), arrange(g, part_a))

        @pl.when(jnp.logical_and(i == 0, jnp.logical_not(fold_early)))
        def _():
            first_sends()

        chain_step(jnp.logical_and(i > 0, chip == 2 * i - 1))
        send(g)
        return carry

    lax.fori_loop(0, 3, pair, 0)
    @pl.when(l < NLAT - 1)
    def _():
        north_row()
        together(bin_rows(*set_a, part_a), prepare(7, *set_b), arrange(5, part_b))

    @pl.when(l == NLAT - 1)
    def _():
        together(bin_rows(*set_a, part_a), arrange(5, part_b))
        fold_row()
        together(prepare(7, *set_b))
    send(5)
    chain_step(chip == 4)
    together(bin_rows(*set_b, part_b), arrange(6, part_a))
    send(6)
    chain_step(chip == 5)
    together(arrange(7, part_b))
    send(7)

    chain_step(chip >= 6)

    @pl.when(jnp.logical_and(core == 0, chip > 0))
    def _():
        down_copy().wait_recv()
    offset[...] = pair_flux[...] + jnp.where(core == 1, south_flux[...], 0.0)
    to_peers(lambda q: offset_copy(q).start())

    tiles = NLON * 2 + NLON // 2

    def owned(slot, g, t, scale, put):
        for c in (0, 1):
            at = 3 * c + slot
            landed(rs_recv.at[pl.ds(0, NLON - c)], rs_rsem.at[c, slot])
            parts = [rs_recv[at * NLON + q] for q in range(NLON)]
            if c == 1:
                parts = [jnp.where(q != o, p, 0.0) for q, p in enumerate(parts)] + [rs_send[g, t]]
            while len(parts) > 1:
                parts = [sum(parts[i : i + 2]) for i in range(0, len(parts), 2)]
            ag_send[at] = parts[0] * scale
            to = put(slot, g)
            to_peers(lambda q: pltpu.make_async_remote_copy(
                ag_send.at[at], to, ag_ssem, ag_rsem,
                device_id={"lon": q, "lat": 2 * chip + c}, device_id_type=MESH).start(), c == 0)
        to[...] = ag_send[at]

    def put_class(slot, g):
        return out_class.at[b_own, pl.ds(pl.multiple_of(8 * g, 8), 8)]

    def put_sums(slot, g):
        return out_sums.at[pl.ds(pl.multiple_of(8 * g, 8), 8)]

    has_sums = jnp.logical_or(b_own == 0, b_own == 3)
    no_sums = jnp.logical_not(has_sums)
    g_sum = lax.rem(turn + 1, 4) + jnp.where(b_own == 0, 4, 0)

    @pl.when(core == 1)
    def _():
        owned(0, turn, b_own, UNIT, put_class)

        @pl.when(jnp.logical_and(has_sums, g_sum < 7))
        def _():
            owned(2, g_sum, REGIONS, 1.0, put_sums)
        owned(1, 4 + turn, b_own, UNIT, put_class)

        @pl.when(jnp.logical_and(has_sums, g_sum == 7))
        def _():
            owned(2, g_sum, REGIONS, 1.0, put_sums)

    @pl.when(core == 0)
    def _():
        landed(rs_recv.at[pl.ds(0, tiles)], rs_ssem)
        pair_copy().wait_send()

    @pl.when(core == 1)
    def _():
        @pl.when(has_sums)
        def _():
            landed(rs_recv.at[pl.ds(0, tiles - 3)], rs_ssem)
            landed(rs_recv.at[pl.ds(0, 3 * (2 * NLON - 1))], ag_ssem)

        @pl.when(no_sums)
        def _():
            landed(rs_recv.at[pl.ds(0, tiles - 2)], rs_ssem)
            landed(rs_recv.at[pl.ds(0, 2 * (2 * NLON - 1))], ag_ssem)

        @pl.when(chip > 0)
        def _():
            pair_copy().wait_send()

        @pl.when(chip < NLAT // 2 - 1)
        def _():
            chain_copy().wait_send()

    landed(rs_recv.at[pl.ds(0, NLON - 1)], off_ssem)

    @pl.when(l > 0)
    def _():
        halo_copy().wait_send()

    @pl.when(l == NLAT - 1)
    def _():
        landed(fold_recv.at[pl.ds(0, NLON - 1)], fold_ssem)

    landed(offsets.at[pl.ds(0, NLON - 1)], off_rsem)
    south = offset[...]
    for q in range(NLON):
        south = south + jnp.where(q != o, offsets[q], 0.0)

    @pl.when(core == 0)
    def _():
        landed(rs_recv.at[pl.ds(0, tiles)], ag_rsem)

    @pl.when(core == 1)
    def _():
        @pl.when(has_sums)
        def _():
            landed(rs_recv.at[pl.ds(0, tiles - 3)], ag_rsem)

        @pl.when(no_sums)
        def _():
            landed(rs_recv.at[pl.ds(0, tiles - 2)], ag_rsem)
    out_sums[ROWS - 8 : ROWS, :] = out_sums[ROWS - 8 : ROWS, :] + south


def finish(classes, sums, out_class, out_over, out_heat, out_impl):
    out_class[...] = classes[...]
    row, lane = iota((88, 128), 0), iota((88, 128), 1)
    upto = (row < HEAT) & (lane <= row) & (lax.div(lane, TIERS) == lax.div(row, TIERS))
    volume = (row >= HEAT) & (row < HEAT + 4) & (lax.div(lane, TIERS) == row - HEAT)
    same = (row >= 72) & (lane == row - 8)
    pick = jnp.where(upto | volume | same, 1.0, 0.0)
    res = lax.dot_general(
        pick, sums[...], (((1,), (1,)), ((), ())), precision=lax.Precision.HIGHEST, preferred_element_type=F32)
    for b in range(REGIONS):
        out_over[b] = UNIT * res[TIERS * b : TIERS * b + TIERS]
    at = HEAT + 8
    mean = res[at + 4 : at + 5] / res[at + 5 : at + 6]
    out_heat[...] = (UNIT / 16.0) * (res[at : at + 4] - res[HEAT : HEAT + 4] * mean)
    flux = res[FLUX + 8 : FLUX + 16]
    south_of = jnp.where(iota((ROWS, ROWS), 0) <= iota((ROWS, ROWS), 1), 1.0, 0.0)
    c = jnp.dot(flux, south_of, precision=lax.Precision.HIGHEST, preferred_element_type=F32)
    out_impl[...] = IMPLIED * (c[0:4] + flux[4:8, ROWS - 1 : ROWS])


def body(speed, theta, dz, dx, area, flux, tally, region, seam):
    any_ = pl.BlockSpec(memory_space=pltpu.HBM)
    vmem = pl.BlockSpec(memory_space=pltpu.VMEM)
    dma = pltpu.SemaphoreType.DMA
    inputs = (speed, theta, dz, dx, area, flux, tally, region, seam)
    inputs = [pltpu.with_memory_space_constraint(x, pltpu.HBM) for x in inputs]
    rows = [pltpu.VMEM((TIERS, GROUP, COLS), F32)] * 2
    sets = (rows + [pltpu.VMEM((TIERS, 2, 8 * GROUP, 128), F32), pltpu.VMEM((8 * SIDE, 128), F32)]) * 2
    classes, sums = pl.pallas_call(
        kernel,
        out_shape=(
            jax.ShapeDtypeStruct((REGIONS, ROWS, BINS), F32),
            jax.ShapeDtypeStruct((ROWS, 128), F32),
        ),
        in_specs=[any_] * 9,
        out_specs=(vmem, vmem),
        scratch_shapes=[
            pltpu.VMEM((TIERS, ROWS + 8, COLS), F32),
            pltpu.VMEM((TIERS, ROWS, COLS), F32),
            pltpu.VMEM((ROWS, COLS), F32),
            pltpu.VMEM((ROWS, COLS), F32),
            pltpu.VMEM((ROWS, COLS), F32),
            pltpu.VMEM((ROWS + 8, COLS), jnp.int32),
            pltpu.VMEM((ROWS, COLS), jnp.int32),
            pltpu.SMEM((TIERS,), F32),
            pltpu.SMEM((COLS,), jnp.int32),
            *sets,
            pltpu.VMEM((ROWS // 8, REGIONS + 1, 8, 128), F32),
            pltpu.VMEM((2 * 3 * NLON, 8, 128), F32),
            pltpu.VMEM((2 * 3, 8, 128), F32),
            pltpu.VMEM((24, COLS), F32),
            pltpu.VMEM((24, COLS), F32),
            pltpu.VMEM((24, COLS), F32),
            pltpu.VMEM((NLON, 24, COLS), F32),
            *([pltpu.VMEM((8, 128), F32)] * 5),
            pltpu.VMEM((NLON, 8, 128), F32),
            dma((11,)),
            dma, dma((2, 3)), dma, dma,
            dma, dma,
            *([dma] * 8),
        ],
        compiler_params=pltpu.CompilerParams(collective_id=0, has_side_effects=True, vmem_limit_bytes=VMEM_LIMIT),
    )(*inputs)
    out_class, over, heat, impl = pl.pallas_call(
        finish,
        out_shape=(
            jax.ShapeDtypeStruct((REGIONS, ROWS, BINS), F32),
            jax.ShapeDtypeStruct((REGIONS, TIERS, ROWS), F32),
            jax.ShapeDtypeStruct((REGIONS, ROWS), F32),
            jax.ShapeDtypeStruct((REGIONS, ROWS), F32),
        ),
        in_specs=[vmem, vmem],
        out_specs=(vmem,) * 4,
        compiler_params=pltpu.CompilerParams(vmem_limit_bytes=4 * 2**20),
    )(classes, sums)
    return out_class, jnp.transpose(over, (0, 2, 1)), heat, impl


def solution(mesh):
    in_specs = (
        P(None, "lat", "lon"),
        P(None, "lat", "lon"),
        P(),
        P("lat", "lon"),
        P("lat", "lon"),
        P("lat", "lon"),
        P("lat", "lon"),
        P("lat", "lon"),
        P("lon"),
    )
    out_specs = (P(None, "lat", None), P(None, "lat", None), P(None, "lat"), P(None, "lat"))
    return jax.shard_map(body, mesh=mesh, in_specs=in_specs, out_specs=out_specs, check_vma=False)
```

```python
import math

import jax
import jax.numpy as jnp
from jax import lax
from jax.experimental import pallas as pl
from jax.experimental.pallas import tpu as pltpu
from jax.sharding import PartitionSpec as P

BINS = 128
REGIONS = 4
TIERS = 16
ROWS = 64
COLS = 256
NLON = 16
NLAT = 16
GROUP = 8
OWNED = ROWS // NLON
LO = 12
HI = 11
SIDE = REGIONS * LO

HEAT, THETA, WET, FLUX, SOUTH = 64, 68, 69, 72, 76

UNIT = math.sqrt(BINS / (COLS * NLON * TIERS))
IMPLIED = 2.0 / math.sqrt(COLS * NLON * ROWS * NLAT)
VMEM_LIMIT = 32 * 2**20
F32, BF16 = jnp.float32, jnp.bfloat16


def iota(shape, dim):
    return lax.broadcasted_iota(jnp.int32, shape, dim)


def two_terms(x):
    high = x.astype(BF16).astype(F32)
    return high, x - high


def kernel(
    speed_h, theta_h, dz_h, dx_h, area_h, flux_h, tally_h, region_h, seam_h,
    out_class, out_sums,
    th, sp, dx, area, flux, tally, region, dz_s, seam_s,
    hi_a, cl_a, val_a, part_a, hi_b, cl_b, val_b, part_b,
    rs_send, rs_recv, ag_send,
    halo_send, halo_recv, fold_send, fold_recv, own_flux, pair_flux, south_flux, north_flux, offset, offsets, skipped,
    in_sem, rs_ssem, rs_rsem, ag_ssem, ag_rsem, fold_ssem, fold_rsem,
    halo_ssem, halo_rsem, pair_ssem, pair_rsem, chain_ssem, chain_rsem, off_ssem, off_rsem, skip_ssem, skip_rsem,
):
    o = lax.axis_index("lon")
    l = lax.axis_index("lat")
    lane8 = iota((8, 128), 1)
    MESH = pl.DeviceIdType.MESH

    first, rest = pl.ds(0, 24), pl.ds(24, ROWS - 24)
    loads = [
        pltpu.make_async_copy(tally_h, tally.at[pl.ds(0, ROWS)], in_sem.at[3]),
        pltpu.make_async_copy(dx_h, dx, in_sem.at[4]),
        pltpu.make_async_copy(region_h, region, in_sem.at[2]),
        pltpu.make_async_copy(dz_h, dz_s, in_sem.at[9]),
        pltpu.make_async_copy(theta_h.at[:, first], th.at[:, first], in_sem.at[5]),
        pltpu.make_async_copy(speed_h.at[:, first], sp.at[:, first], in_sem.at[6]),
        pltpu.make_async_copy(flux_h, flux, in_sem.at[0]),
        pltpu.make_async_copy(area_h, area, in_sem.at[1]),
        pltpu.make_async_copy(theta_h.at[:, rest], th.at[:, rest], in_sem.at[7]),
        pltpu.make_async_copy(speed_h.at[:, rest], sp.at[:, rest], in_sem.at[8]),
        pltpu.make_async_copy(seam_h, seam_s, in_sem.at[10]),
    ]
    for load in loads:
        load.start()

    barrier = pltpu.get_barrier_semaphore()
    for d in range(1, NLON):
        pl.semaphore_signal(barrier, inc=1, device_id={"lon": lax.rem(o + d, NLON)}, device_id_type=MESH)
    chip, core = lax.div(l, 2), lax.rem(l, 2)
    sibling = l + 1 - 2 * core
    for q in range(NLON):
        pl.semaphore_signal(barrier, inc=1, device_id={"lon": q, "lat": sibling}, device_id_type=MESH)
    near = [l - 2, l + 2, l - 1 + 2 * core]
    far = jnp.logical_and(core == 1, chip >= 4)
    near += [jnp.where(far & (l + d > 8), l + d, -1) for d in (-6, -4, 4, 6)]
    for n in near:
        @pl.when(jnp.logical_and(n >= 0, n < NLAT))
        def _():
            pl.semaphore_signal(barrier, inc=1, device_id={"lat": n}, device_id_type=MESH)

    def halo_copy():
        return pltpu.make_async_remote_copy(
            halo_send, halo_recv, halo_ssem, halo_rsem, device_id={"lat": lax.max(l - 1, 0)}, device_id_type=MESH)

    def fold_copy(dst):
        return pltpu.make_async_remote_copy(
            fold_send, fold_recv.at[o], fold_ssem, fold_rsem, device_id={"lon": dst}, device_id_type=MESH)

    def pair_copy():
        return pltpu.make_async_remote_copy(
            own_flux, pair_flux, pair_ssem, pair_rsem, device_id={"lat": sibling}, device_id_type=MESH)

    def down_copy():
        return pltpu.make_async_remote_copy(
            south_flux, pair_flux, pair_ssem, pair_rsem, device_id={"lat": sibling}, device_id_type=MESH)

    def chain_copy():
        return pltpu.make_async_remote_copy(
            north_flux, south_flux, chain_ssem, chain_rsem,
            device_id={"lat": lax.min(l + 2, NLAT - 1)}, device_id_type=MESH)

    def offset_copy(dst):
        return pltpu.make_async_remote_copy(
            offset, offsets.at[o], off_ssem, off_rsem, device_id={"lon": dst}, device_id_type=MESH)

    def skip_copy(src, dst):
        return pltpu.make_async_remote_copy(
            north_flux, skipped.at[src - 4], skip_ssem.at[dst - 5], skip_rsem.at[src - 4],
            device_id={"lat": 2 * dst + 1}, device_id_type=MESH)

    def skip_sends(act):
        for src in (4, 5, 6):
            for dst in range(src + 1, 8):
                @pl.when(jnp.logical_and(core == 1, chip == src))
                def _():
                    act(skip_copy(src, dst))

    def chain_step(turn):
        @pl.when(jnp.logical_and(turn, core == 1))
        def _():
            pair_copy().wait_recv()

            @pl.when(chip > 0)
            def _():
                chain_copy().wait_recv()
                down_copy().start()
            north_flux[...] = south_flux[...] + own_flux[...] + pair_flux[...]

            @pl.when(chip < 4)
            def _():
                chain_copy().start()

            @pl.when(chip == 4)
            def _():
                for dst in (5, 6, 7):
                    skip_copy(4, dst).start()

    def early_step(turn):
        @pl.when(jnp.logical_and(turn, core == 1))
        def _():
            pair_copy().wait_recv()
            north_flux[...] = own_flux[...] + pair_flux[...]
            for src in (5, 6):
                @pl.when(chip == src)
                def _():
                    for dst in range(src + 1, 8):
                        skip_copy(src, dst).start()

    def last_step():
        @pl.when(jnp.logical_and(chip >= 5, core == 1))
        def _():
            @pl.when(chip == 7)
            def _():
                pair_copy().wait_recv()
            south_flux[...] = jnp.zeros((8, 128), F32)
            for src in (4, 5, 6):
                @pl.when(chip > src)
                def _():
                    skip_copy(src, 7).wait_recv()
                    south_flux[...] = south_flux[...] + skipped[src - 4]
            down_copy().start()

    def owner(g, t):
        turn = lax.rem(g if t < REGIONS else g + 3, 4)
        wide_x, wide_y = lax.div(turn, 2), lax.rem(turn, 2)
        late = lax.div(g, 4)
        b = t if t < REGIONS else 3 * (1 - late)
        x, y = (b // 2, b % 2) if t < REGIONS else (1 - late, 1 - late)
        x = jnp.where(wide_x == 1, 3 * x, 1 + x)
        y = jnp.where(wide_y == 1, 3 * y, 1 + y)
        return 4 * x + y, (late if t < REGIONS else 2)

    def rs_copy(g, t):
        dst, slot = owner(g, t)
        return pltpu.make_async_remote_copy(
            rs_send.at[g, t], rs_recv.at[(3 * core + slot) * NLON + o], rs_ssem, rs_rsem.at[core, slot],
            device_id={"lon": dst, "lat": 2 * chip + 1}, device_id_type=MESH)

    def remote_tile(g, t):
        dst, _ = owner(g, t)
        return jnp.logical_or(core == 0, dst != o)

    x_own, y_own = lax.div(o, 4), lax.rem(o, 4)
    wide = [jnp.where(jnp.logical_or(v == 0, v == 3), 1, 0) for v in (x_own, y_own)]
    turn = 2 * wide[0] + wide[1]
    b_own = 2 * jnp.where(x_own >= 2, 1, 0) + jnp.where(y_own >= 2, 1, 0)
    peers = (0, 4, 1, 5, 8, 12, 2, 9, 3, 6, 13, 7, 10, 11, 14, 15)

    def to_peers(act, all_of_them=False):
        for q in peers:
            if all_of_them:
                act(q)
            else:
                @pl.when(o != q)
                def _():
                    act(q)

    def landed(ref, sem):
        pltpu.make_async_copy(ref, ref, sem).wait()

    def flux_totals():
        acc = [jnp.zeros((8, COLS), F32) for _ in range(REGIONS)]
        for g in range(ROWS // 8):
            rows = slice(8 * g, 8 * g + 8)
            f = flux[rows, :] * area[rows, :]
            reg = region[rows, :]
            for b in range(REGIONS):
                acc[b] = acc[b] + jnp.where(reg == b, f, 0.0)
        totals = jnp.zeros((8, 128), F32)
        for b in range(REGIONS):
            t = jnp.sum(jnp.sum(acc[b], axis=0, keepdims=True), axis=1, keepdims=True)
            totals = jnp.where(lane8 == SOUTH + b, t, totals)
        own_flux[...] = totals

        @pl.when(chip == 0)
        def _():
            south_flux[...] = jnp.zeros((8, 128), F32)

            @pl.when(core == 0)
            def _():
                pair_flux[...] = jnp.zeros((8, 128), F32)

    def edge_rows():
        for k in range(TIERS):
            halo_send[k : k + 1, :] = th[k, 0:1, :]
            fold_send[k : k + 1, :] = th[k, ROWS - 1 : ROWS, :]
        halo_send[TIERS:24, :] = jnp.broadcast_to(tally[0:1, :].astype(F32), (8, COLS))
        fold_send[TIERS:24, :] = jnp.broadcast_to(tally[ROWS - 1 : ROWS, :].astype(F32), (8, COLS))

    def first_sends():
        known = 2 * NLON - 1
        for n in near:
            known = known + jnp.where(jnp.logical_and(n >= 0, n < NLAT), 1, 0)
        pl.semaphore_wait(barrier, known)

        @pl.when(core == 0)
        def _():
            pair_copy().start()

        @pl.when(l == NLAT - 1)
        def _():
            to_peers(lambda q: fold_copy(q).start())
            fold_recv[o] = fold_send[...]

        @pl.when(l > 0)
        def _():
            halo_copy().start()

    def put_north():
        for k in range(TIERS):
            th[k, ROWS : ROWS + 1, :] = halo_recv[k : k + 1, :]
        tally[ROWS : ROWS + 1, :] = halo_recv[TIERS : TIERS + 1, :].astype(jnp.int32)

    def north_row():
        halo_copy().wait_recv()
        put_north()

    def fold_row():
        landed(fold_recv.at[pl.ds(0, NLON - 1)], fold_rsem)
        first = seam_s[0]
        source = lax.shift_right_logical(first, 8)
        at = jnp.bitwise_and(first, COLS - 1)
        high = fold_recv[source]
        low = fold_recv[jnp.bitwise_and(source + NLON - 1, NLON - 1)]
        for t in range(COLS // 128):
            i = lane8 + 128 * t
            spot = jnp.bitwise_and(at - i, COLS - 1)
            lane = jnp.bitwise_and(spot, 127)
            for r in range(3):
                rows = slice(8 * r, 8 * r + 8)
                pick = [
                    jnp.where(
                        spot >= 128,
                        jnp.take_along_axis(src[rows, 128:], lane, axis=1),
                        jnp.take_along_axis(src[rows, :128], lane, axis=1),
                    )
                    for src in (high, low)
                ]
                halo_recv[rows, 128 * t : 128 * t + 128] = jnp.where(i <= at, pick[0], pick[1])
        put_north()

    sub8 = iota((8, COLS), 0)
    hi_iota = lax.shift_right_logical(iota((SIDE, COLS), 0), 2).astype(F32).astype(BF16)
    cl_iota = iota((SIDE, COLS), 0).astype(F32).astype(BF16)
    zero = jnp.zeros((SIDE, COLS), BF16)
    one = jnp.ones((SIDE, COLS), BF16)

    def prepare(g, hi_r, cl_r, val_r):
        base = g * GROUP if isinstance(g, int) else pl.multiple_of(g * GROUP, GROUP)
        here = pl.ds(base, GROUP)
        nxt = pl.ds(base + GROUP, 1)
        deep = tally[here, :]
        face_depth = jnp.minimum(deep, jnp.where(sub8 == 7, tally[nxt, :], pltpu.roll(deep, 7, 0)))
        width = dx[here, :]
        reg = region[here, :]
        regf = reg.astype(F32) * LO
        member = [reg == b for b in range(REGIONS)]
        heat = theta_sum = wet_sum = jnp.zeros((8, COLS), F32)
        stats = jnp.zeros((8, 128), F32)
        for k in range(TIERS):
            t = th[k, here, :]
            face = 0.5 * (t + jnp.where(sub8 == 7, th[k, nxt, :], pltpu.roll(t, 7, 0)))
            vol = jnp.where(face_depth > k, dz_s[k] * width, 0.0)
            mass = vol * sp[k, here, :]
            pos = jnp.clip((face - (-2.0)) * (BINS / 32.0), 0.0, BINS - 1.0)
            low = jnp.minimum(jnp.floor(pos), BINS - 2.0)
            hi = jnp.floor((low + 0.5) * (1.0 / LO))
            hi_r[k] = hi
            cl_r[k] = (low - hi * LO) + regf
            for n, x in enumerate(two_terms(mass) + two_terms(mass * (pos - low))):
                for half in range(2):
                    val_r[k, half, pl.ds(n, 8, stride=8), :] = x[:, 128 * half : 128 * half + 128]
                    val_r[k, half, pl.ds(n + 4, 8, stride=8), :] = x[:, 128 * half : 128 * half + 128]
            heat = heat + mass * face
            theta_sum = theta_sum + vol * face
            wet_sum = wet_sum + vol
            for b in range(REGIONS):
                red = jnp.sum(jnp.where(member[b], mass, 0.0), axis=1, keepdims=True)
                stats = jnp.where(lane8 == b * TIERS + k, red, stats)
            yield
        f = flux[here, :] * area[here, :]
        for b in range(REGIONS):
            red = jnp.sum(jnp.where(member[b], heat, 0.0), axis=1, keepdims=True)
            stats = jnp.where(lane8 == HEAT + b, red, stats)
            red = jnp.sum(jnp.where(member[b], f, 0.0), axis=1, keepdims=True)
            stats = jnp.where(lane8 == FLUX + b, red, stats)
        stats = jnp.where(lane8 == THETA, jnp.sum(theta_sum, axis=1, keepdims=True), stats)
        stats = jnp.where(lane8 == WET, jnp.sum(wet_sum, axis=1, keepdims=True), stats)
        rs_send[g, REGIONS] = stats
        yield

    def bin_rows(hi_r, cl_r, val_r, part_r):
        for jj in range(GROUP):
            total = None
            for k in range(TIERS):
                hi = jnp.broadcast_to(hi_r[k, jj : jj + 1, :], (SIDE, COLS)).astype(BF16)
                cl = jnp.broadcast_to(cl_r[k, jj : jj + 1, :], (SIDE, COLS)).astype(BF16)
                val = jnp.concatenate([val_r[k, half, 8 * jj : 8 * jj + 8, :] for half in range(2)], axis=1)
                val = jnp.concatenate([val] * (SIDE // 8), axis=0).astype(BF16)
                lhs = jnp.where(hi == hi_iota, val, zero)
                rhs = jnp.where(cl == cl_iota, one, zero)
                d = lax.dot_general(lhs, rhs, (((1,), (1,)), ((), ())), preferred_element_type=F32)
                total = d if total is None else total + d
            part_r[pl.ds(jj, SIDE, stride=8), 0:SIDE] = total
            yield

    bin_lane = lax.rem(lane8, LO)
    bin_block = lax.div(lane8, LO)

    def arrange(g, part_r):
        s0 = [jnp.zeros((8, 128), F32)] * REGIONS
        s1 = [jnp.zeros((8, 128), F32)] * REGIONS
        for hi in range(HI):
            rows = [part_r[32 * hi + 8 * n : 32 * hi + 8 * n + 8, :] for n in range(4)]
            wx = rows[2] + rows[3]
            x = rows[0] + rows[1] - wx
            for b in range(REGIONS):
                at = bin_lane + LO * b
                s0[b] = jnp.where(bin_block == hi, jnp.take_along_axis(x, at, axis=1), s0[b])
                s1[b] = jnp.where(bin_block == hi, jnp.take_along_axis(wx, at, axis=1), s1[b])
            yield
        for b in range(REGIONS):
            rs_send[g, b] = s0[b] + jnp.where(lane8 == 0, 0.0, pltpu.roll(s1[b], 1, 1))
        yield

    def together(*parts):
        parts = [p for p in parts if p is not None]
        done = object()
        lead, rest = parts[0], parts[1:]
        per = [2] * len(rest)
        while next(lead, done) is not done:
            for p, n in zip(rest, per):
                for _ in range(n):
                    next(p, done)
        for p in rest:
            while next(p, done) is not done:
                pass

    def send(g):
        for t in range(REGIONS + 1):
            @pl.when(remote_tile(g, t))
            def _():
                rs_copy(g, t).start()

    set_a = (hi_a, cl_a, val_a)
    set_b = (hi_b, cl_b, val_b)

    for load in loads[:8]:
        load.wait()
    together(prepare(0, *set_a))

    fold_early = (l == NLAT - 1) & (x_own >= 2) & (y_own >= 2)

    def pair(i, carry):
        g = 2 * i
        together(bin_rows(*set_a, part_a), prepare(g + 1, *set_b), arrange(lax.max(g - 1, 0), part_b))

        @pl.when(i == 0)
        def _():
            for load in loads[8:]:
                load.wait()
            flux_totals()
            edge_rows()

        @pl.when(jnp.logical_and(i == 0, fold_early))
        def _():
            first_sends()

        chain_step(jnp.logical_and(i > 0, chip == 2 * i - 2))

        @pl.when(i > 0)
        def _():
            send(g - 1)
        together(bin_rows(*set_b, part_b), prepare(g + 2, *set_a), arrange(g, part_a))

        @pl.when(jnp.logical_and(i == 0, jnp.logical_not(fold_early)))
        def _():
            first_sends()

        chain_step(jnp.logical_and(i > 0, chip == 2 * i - 1))
        early_step(jnp.logical_and(i == 1, jnp.logical_or(chip == 5, chip == 6)))
        send(g)
        return carry

    lax.fori_loop(0, 3, pair, 0)
    @pl.when(l < NLAT - 1)
    def _():
        north_row()
        together(bin_rows(*set_a, part_a), prepare(7, *set_b), arrange(5, part_b))

    @pl.when(l == NLAT - 1)
    def _():
        together(bin_rows(*set_a, part_a), arrange(5, part_b))
        fold_row()
        together(prepare(7, *set_b))
    send(5)
    chain_step(chip == 4)
    together(bin_rows(*set_b, part_b), arrange(6, part_a))
    send(6)
    together(arrange(7, part_b))
    send(7)

    last_step()

    @pl.when(jnp.logical_and(core == 0, chip > 0))
    def _():
        down_copy().wait_recv()
    offset[...] = pair_flux[...] + jnp.where(core == 1, south_flux[...], 0.0)
    to_peers(lambda q: offset_copy(q).start())

    tiles = NLON * 2 + NLON // 2

    def owned(slot, g, t, scale, put):
        for c in (0, 1):
            at = 3 * c + slot
            landed(rs_recv.at[pl.ds(0, NLON - c)], rs_rsem.at[c, slot])
            parts = [rs_recv[at * NLON + q] for q in range(NLON)]
            if c == 1:
                parts = [jnp.where(q != o, p, 0.0) for q, p in enumerate(parts)] + [rs_send[g, t]]
            while len(parts) > 1:
                parts = [sum(parts[i : i + 2]) for i in range(0, len(parts), 2)]
            ag_send[at] = parts[0] * scale
            to = put(slot, g)
            to_peers(lambda q: pltpu.make_async_remote_copy(
                ag_send.at[at], to, ag_ssem, ag_rsem,
                device_id={"lon": q, "lat": 2 * chip + c}, device_id_type=MESH).start(), c == 0)
        to[...] = ag_send[at]

    def put_class(slot, g):
        return out_class.at[b_own, pl.ds(pl.multiple_of(8 * g, 8), 8)]

    def put_sums(slot, g):
        return out_sums.at[pl.ds(pl.multiple_of(8 * g, 8), 8)]

    has_sums = jnp.logical_or(b_own == 0, b_own == 3)
    no_sums = jnp.logical_not(has_sums)
    g_sum = lax.rem(turn + 1, 4) + jnp.where(b_own == 0, 4, 0)

    @pl.when(core == 1)
    def _():
        owned(0, turn, b_own, UNIT, put_class)

        @pl.when(jnp.logical_and(has_sums, g_sum < 7))
        def _():
            owned(2, g_sum, REGIONS, 1.0, put_sums)
        owned(1, 4 + turn, b_own, UNIT, put_class)

        @pl.when(jnp.logical_and(has_sums, g_sum == 7))
        def _():
            owned(2, g_sum, REGIONS, 1.0, put_sums)

    @pl.when(core == 0)
    def _():
        landed(rs_recv.at[pl.ds(0, tiles)], rs_ssem)
        pair_copy().wait_send()

    @pl.when(core == 1)
    def _():
        @pl.when(has_sums)
        def _():
            landed(rs_recv.at[pl.ds(0, tiles - 3)], rs_ssem)
            landed(rs_recv.at[pl.ds(0, 3 * (2 * NLON - 1))], ag_ssem)

        @pl.when(no_sums)
        def _():
            landed(rs_recv.at[pl.ds(0, tiles - 2)], rs_ssem)
            landed(rs_recv.at[pl.ds(0, 2 * (2 * NLON - 1))], ag_ssem)

        @pl.when(chip > 0)
        def _():
            pair_copy().wait_send()

        @pl.when(chip < 4)
        def _():
            chain_copy().wait_send()
    skip_sends(lambda copy: copy.wait_send())

    landed(rs_recv.at[pl.ds(0, NLON - 1)], off_ssem)

    @pl.when(l > 0)
    def _():
        halo_copy().wait_send()

    @pl.when(l == NLAT - 1)
    def _():
        landed(fold_recv.at[pl.ds(0, NLON - 1)], fold_ssem)

    landed(offsets.at[pl.ds(0, NLON - 1)], off_rsem)
    south = offset[...]
    for q in range(NLON):
        south = south + jnp.where(q != o, offsets[q], 0.0)

    @pl.when(core == 0)
    def _():
        landed(rs_recv.at[pl.ds(0, tiles)], ag_rsem)

    @pl.when(core == 1)
    def _():
        @pl.when(has_sums)
        def _():
            landed(rs_recv.at[pl.ds(0, tiles - 3)], ag_rsem)

        @pl.when(no_sums)
        def _():
            landed(rs_recv.at[pl.ds(0, tiles - 2)], ag_rsem)
    out_sums[ROWS - 8 : ROWS, :] = out_sums[ROWS - 8 : ROWS, :] + south


def finish(classes, sums, out_class, out_over, out_heat, out_impl):
    out_class[...] = classes[...]
    row, lane = iota((88, 128), 0), iota((88, 128), 1)
    upto = (row < HEAT) & (lane <= row) & (lax.div(lane, TIERS) == lax.div(row, TIERS))
    volume = (row >= HEAT) & (row < HEAT + 4) & (lax.div(lane, TIERS) == row - HEAT)
    same = (row >= 72) & (lane == row - 8)
    pick = jnp.where(upto | volume | same, 1.0, 0.0)
    res = lax.dot_general(
        pick, sums[...], (((1,), (1,)), ((), ())), precision=lax.Precision.HIGHEST, preferred_element_type=F32)
    for b in range(REGIONS):
        out_over[b] = UNIT * res[TIERS * b : TIERS * b + TIERS]
    at = HEAT + 8
    mean = res[at + 4 : at + 5] / res[at + 5 : at + 6]
    out_heat[...] = (UNIT / 16.0) * (res[at : at + 4] - res[HEAT : HEAT + 4] * mean)
    flux = res[FLUX + 8 : FLUX + 16]
    south_of = jnp.where(iota((ROWS, ROWS), 0) <= iota((ROWS, ROWS), 1), 1.0, 0.0)
    c = jnp.dot(flux, south_of, precision=lax.Precision.HIGHEST, preferred_element_type=F32)
    out_impl[...] = IMPLIED * (c[0:4] + flux[4:8, ROWS - 1 : ROWS])


def body(speed, theta, dz, dx, area, flux, tally, region, seam):
    any_ = pl.BlockSpec(memory_space=pltpu.HBM)
    vmem = pl.BlockSpec(memory_space=pltpu.VMEM)
    dma = pltpu.SemaphoreType.DMA
    inputs = (speed, theta, dz, dx, area, flux, tally, region, seam)
    inputs = [pltpu.with_memory_space_constraint(x, pltpu.HBM) for x in inputs]
    rows = [pltpu.VMEM((TIERS, GROUP, COLS), F32)] * 2
    sets = (rows + [pltpu.VMEM((TIERS, 2, 8 * GROUP, 128), F32), pltpu.VMEM((8 * SIDE, 128), F32)]) * 2
    classes, sums = pl.pallas_call(
        kernel,
        out_shape=(
            jax.ShapeDtypeStruct((REGIONS, ROWS, BINS), F32),
            jax.ShapeDtypeStruct((ROWS, 128), F32),
        ),
        in_specs=[any_] * 9,
        out_specs=(vmem, vmem),
        scratch_shapes=[
            pltpu.VMEM((TIERS, ROWS + 8, COLS), F32),
            pltpu.VMEM((TIERS, ROWS, COLS), F32),
            pltpu.VMEM((ROWS, COLS), F32),
            pltpu.VMEM((ROWS, COLS), F32),
            pltpu.VMEM((ROWS, COLS), F32),
            pltpu.VMEM((ROWS + 8, COLS), jnp.int32),
            pltpu.VMEM((ROWS, COLS), jnp.int32),
            pltpu.SMEM((TIERS,), F32),
            pltpu.SMEM((COLS,), jnp.int32),
            *sets,
            pltpu.VMEM((ROWS // 8, REGIONS + 1, 8, 128), F32),
            pltpu.VMEM((2 * 3 * NLON, 8, 128), F32),
            pltpu.VMEM((2 * 3, 8, 128), F32),
            pltpu.VMEM((24, COLS), F32),
            pltpu.VMEM((24, COLS), F32),
            pltpu.VMEM((24, COLS), F32),
            pltpu.VMEM((NLON, 24, COLS), F32),
            *([pltpu.VMEM((8, 128), F32)] * 5),
            pltpu.VMEM((NLON, 8, 128), F32),
            pltpu.VMEM((3, 8, 128), F32),
            dma((11,)),
            dma, dma((2, 3)), dma, dma,
            dma, dma,
            *([dma] * 8), dma((3,)), dma((3,)),
        ],
        compiler_params=pltpu.CompilerParams(collective_id=0, has_side_effects=True, vmem_limit_bytes=VMEM_LIMIT),
    )(*inputs)
    out_class, over, heat, impl = pl.pallas_call(
        finish,
        out_shape=(
            jax.ShapeDtypeStruct((REGIONS, ROWS, BINS), F32),
            jax.ShapeDtypeStruct((REGIONS, TIERS, ROWS), F32),
            jax.ShapeDtypeStruct((REGIONS, ROWS), F32),
            jax.ShapeDtypeStruct((REGIONS, ROWS), F32),
        ),
        in_specs=[vmem, vmem],
        out_specs=(vmem,) * 4,
        compiler_params=pltpu.CompilerParams(vmem_limit_bytes=4 * 2**20),
    )(classes, sums)
    return out_class, jnp.transpose(over, (0, 2, 1)), heat, impl


def solution(mesh):
    in_specs = (
        P(None, "lat", "lon"),
        P(None, "lat", "lon"),
        P(),
        P("lat", "lon"),
        P("lat", "lon"),
        P("lat", "lon"),
        P("lat", "lon"),
        P("lat", "lon"),
        P("lon"),
    )
    out_specs = (P(None, "lat", None), P(None, "lat", None), P(None, "lat"), P(None, "lat"))
    return jax.shard_map(body, mesh=mesh, in_specs=in_specs, out_specs=out_specs, check_vma=False)
```

```python
import math

import jax
import jax.numpy as jnp
from jax import lax
from jax.experimental import pallas as pl
from jax.experimental.pallas import tpu as pltpu
from jax.sharding import PartitionSpec as P

BINS = 128
REGIONS = 4
TIERS = 16
ROWS = 64
COLS = 256
NLON = 16
NLAT = 16
GROUP = 8
OWNED = ROWS // NLON
LO = 12
HI = 11
SIDE = REGIONS * LO

HEAT, THETA, WET, FLUX, SOUTH = 64, 68, 69, 72, 76

UNIT = math.sqrt(BINS / (COLS * NLON * TIERS))
IMPLIED = 2.0 / math.sqrt(COLS * NLON * ROWS * NLAT)
VMEM_LIMIT = 32 * 2**20
F32, BF16 = jnp.float32, jnp.bfloat16


def iota(shape, dim):
    return lax.broadcasted_iota(jnp.int32, shape, dim)


def two_terms(x):
    high = x.astype(BF16).astype(F32)
    return high, x - high


def kernel(
    speed_h, theta_h, dz_h, dx_h, area_h, flux_h, tally_h, region_h, seam_h,
    out_class, out_sums,
    th, sp, dx, area, flux, tally, region, dz_s, seam_s,
    hi_a, cl_a, val_a, part_a, hi_b, cl_b, val_b, part_b,
    rs_send, rs_recv, ag_send,
    halo_send, halo_recv, fold_send, fold_recv, own_flux, pair_flux, south_flux, north_flux, offset, offsets, skipped,
    in_sem, rs_ssem, rs_rsem, ag_ssem, ag_rsem, fold_ssem, fold_rsem,
    halo_ssem, halo_rsem, pair_ssem, pair_rsem, chain_ssem, chain_rsem, off_ssem, off_rsem, skip_ssem, skip_rsem,
):
    o = lax.axis_index("lon")
    l = lax.axis_index("lat")
    lane8 = iota((8, 128), 1)
    MESH = pl.DeviceIdType.MESH

    first, rest = pl.ds(0, 24), pl.ds(24, ROWS - 24)
    loads = [
        pltpu.make_async_copy(tally_h, tally.at[pl.ds(0, ROWS)], in_sem.at[3]),
        pltpu.make_async_copy(dx_h, dx, in_sem.at[4]),
        pltpu.make_async_copy(region_h, region, in_sem.at[2]),
        pltpu.make_async_copy(dz_h, dz_s, in_sem.at[9]),
        pltpu.make_async_copy(theta_h.at[:, first], th.at[:, first], in_sem.at[5]),
        pltpu.make_async_copy(speed_h.at[:, first], sp.at[:, first], in_sem.at[6]),
        pltpu.make_async_copy(flux_h, flux, in_sem.at[0]),
        pltpu.make_async_copy(area_h, area, in_sem.at[1]),
        pltpu.make_async_copy(theta_h.at[:, rest], th.at[:, rest], in_sem.at[7]),
        pltpu.make_async_copy(speed_h.at[:, rest], sp.at[:, rest], in_sem.at[8]),
        pltpu.make_async_copy(seam_h, seam_s, in_sem.at[10]),
    ]
    for load in loads:
        load.start()

    barrier = pltpu.get_barrier_semaphore()
    for d in range(1, NLON):
        pl.semaphore_signal(barrier, inc=1, device_id={"lon": lax.rem(o + d, NLON)}, device_id_type=MESH)
    chip, core = lax.div(l, 2), lax.rem(l, 2)
    sibling = l + 1 - 2 * core
    for q in range(NLON):
        pl.semaphore_signal(barrier, inc=1, device_id={"lon": q, "lat": sibling}, device_id_type=MESH)
    near = [l - 2, l + 2, l - 1 + 2 * core]
    far = jnp.logical_and(core == 1, chip >= 4)
    near += [jnp.where(far & (l + d > 8), l + d, -1) for d in (-6, -4, 4, 6)]
    for n in near:
        @pl.when(jnp.logical_and(n >= 0, n < NLAT))
        def _():
            pl.semaphore_signal(barrier, inc=1, device_id={"lat": n}, device_id_type=MESH)

    def halo_copy():
        return pltpu.make_async_remote_copy(
            halo_send, halo_recv, halo_ssem, halo_rsem, device_id={"lat": lax.max(l - 1, 0)}, device_id_type=MESH)

    def fold_copy(dst):
        return pltpu.make_async_remote_copy(
            fold_send, fold_recv.at[o], fold_ssem, fold_rsem, device_id={"lon": dst}, device_id_type=MESH)

    def pair_copy():
        return pltpu.make_async_remote_copy(
            own_flux, pair_flux, pair_ssem, pair_rsem, device_id={"lat": sibling}, device_id_type=MESH)

    def down_copy():
        return pltpu.make_async_remote_copy(
            south_flux, pair_flux, pair_ssem, pair_rsem, device_id={"lat": sibling}, device_id_type=MESH)

    def chain_copy():
        return pltpu.make_async_remote_copy(
            north_flux, south_flux, chain_ssem, chain_rsem,
            device_id={"lat": lax.min(l + 2, NLAT - 1)}, device_id_type=MESH)

    def offset_copy(dst):
        return pltpu.make_async_remote_copy(
            offset, offsets.at[o], off_ssem, off_rsem, device_id={"lon": dst}, device_id_type=MESH)

    def skip_copy(src, dst):
        return pltpu.make_async_remote_copy(
            north_flux, skipped.at[src - 4], skip_ssem.at[dst - 5], skip_rsem.at[src - 4],
            device_id={"lat": 2 * dst + 1}, device_id_type=MESH)

    def skip_sends(act):
        for src in (4, 5, 6):
            for dst in range(src + 1, 8):
                @pl.when(jnp.logical_and(core == 1, chip == src))
                def _():
                    act(skip_copy(src, dst))

    def chain_step(turn):
        @pl.when(jnp.logical_and(turn, core == 1))
        def _():
            pair_copy().wait_recv()

            @pl.when(chip > 0)
            def _():
                chain_copy().wait_recv()
                down_copy().start()
            north_flux[...] = south_flux[...] + own_flux[...] + pair_flux[...]

            @pl.when(chip < 4)
            def _():
                chain_copy().start()

            @pl.when(chip == 4)
            def _():
                for dst in (5, 6, 7):
                    skip_copy(4, dst).start()

    def early_step(turn):
        @pl.when(jnp.logical_and(turn, core == 1))
        def _():
            pair_copy().wait_recv()
            north_flux[...] = own_flux[...] + pair_flux[...]
            for src in (5, 6):
                @pl.when(chip == src)
                def _():
                    for dst in range(src + 1, 8):
                        skip_copy(src, dst).start()

    def last_step():
        @pl.when(jnp.logical_and(chip >= 5, core == 1))
        def _():
            @pl.when(chip == 7)
            def _():
                pair_copy().wait_recv()
            south_flux[...] = jnp.zeros((8, 128), F32)
            for src in (4, 5, 6):
                @pl.when(chip > src)
                def _():
                    skip_copy(src, 7).wait_recv()
                    south_flux[...] = south_flux[...] + skipped[src - 4]
            down_copy().start()

    def owner(g, t):
        turn = lax.rem(g if t < REGIONS else g + 3, 4)
        wide_x, wide_y = lax.div(turn, 2), lax.rem(turn, 2)
        late = lax.div(g, 4)
        b = t if t < REGIONS else 3 * (1 - late)
        x, y = (b // 2, b % 2) if t < REGIONS else (1 - late, 1 - late)
        x = jnp.where(wide_x == 1, 3 * x, 1 + x)
        y = jnp.where(wide_y == 1, 3 * y, 1 + y)
        return 4 * x + y, (late if t < REGIONS else 2)

    def rs_copy(g, t):
        dst, slot = owner(g, t)
        return pltpu.make_async_remote_copy(
            rs_send.at[g, t], rs_recv.at[(3 * core + slot) * NLON + o], rs_ssem, rs_rsem.at[core, slot],
            device_id={"lon": dst, "lat": 2 * chip + 1}, device_id_type=MESH)

    def remote_tile(g, t):
        dst, _ = owner(g, t)
        return jnp.logical_or(core == 0, dst != o)

    x_own, y_own = lax.div(o, 4), lax.rem(o, 4)
    wide = [jnp.where(jnp.logical_or(v == 0, v == 3), 1, 0) for v in (x_own, y_own)]
    turn = 2 * wide[0] + wide[1]
    b_own = 2 * jnp.where(x_own >= 2, 1, 0) + jnp.where(y_own >= 2, 1, 0)
    peers = (0, 4, 1, 5, 8, 12, 2, 9, 3, 6, 13, 7, 10, 11, 14, 15)

    def to_peers(act, all_of_them=False):
        for q in peers:
            if all_of_them:
                act(q)
            else:
                @pl.when(o != q)
                def _():
                    act(q)

    def landed(ref, sem):
        pltpu.make_async_copy(ref, ref, sem).wait()

    def flux_totals():
        acc = [jnp.zeros((8, COLS), F32) for _ in range(REGIONS)]
        for g in range(ROWS // 8):
            rows = slice(8 * g, 8 * g + 8)
            f = flux[rows, :] * area[rows, :]
            reg = region[rows, :]
            for b in range(REGIONS):
                acc[b] = acc[b] + jnp.where(reg == b, f, 0.0)
        totals = jnp.zeros((8, 128), F32)
        for b in range(REGIONS):
            t = jnp.sum(jnp.sum(acc[b], axis=0, keepdims=True), axis=1, keepdims=True)
            totals = jnp.where(lane8 == SOUTH + b, t, totals)
        own_flux[...] = totals

        @pl.when(chip == 0)
        def _():
            south_flux[...] = jnp.zeros((8, 128), F32)

            @pl.when(core == 0)
            def _():
                pair_flux[...] = jnp.zeros((8, 128), F32)

    def edge_rows():
        for k in range(TIERS):
            halo_send[k : k + 1, :] = th[k, 0:1, :]
            fold_send[k : k + 1, :] = th[k, ROWS - 1 : ROWS, :]
        halo_send[TIERS:24, :] = jnp.broadcast_to(tally[0:1, :].astype(F32), (8, COLS))
        fold_send[TIERS:24, :] = jnp.broadcast_to(tally[ROWS - 1 : ROWS, :].astype(F32), (8, COLS))

    def first_sends():
        known = 2 * NLON - 1
        for n in near:
            known = known + jnp.where(jnp.logical_and(n >= 0, n < NLAT), 1, 0)
        pl.semaphore_wait(barrier, known)

        @pl.when(core == 0)
        def _():
            pair_copy().start()

        @pl.when(l == NLAT - 1)
        def _():
            to_peers(lambda q: fold_copy(q).start())
            fold_recv[o] = fold_send[...]

        @pl.when(l > 0)
        def _():
            halo_copy().start()

    def put_north():
        for k in range(TIERS):
            th[k, ROWS : ROWS + 1, :] = halo_recv[k : k + 1, :]
        tally[ROWS : ROWS + 1, :] = halo_recv[TIERS : TIERS + 1, :].astype(jnp.int32)

    def north_row():
        halo_copy().wait_recv()
        put_north()

    def fold_row():
        landed(fold_recv.at[pl.ds(0, NLON - 1)], fold_rsem)
        first = seam_s[0]
        source = lax.shift_right_logical(first, 8)
        at = jnp.bitwise_and(first, COLS - 1)
        high = fold_recv[source]
        low = fold_recv[jnp.bitwise_and(source + NLON - 1, NLON - 1)]
        for t in range(COLS // 128):
            i = lane8 + 128 * t
            spot = jnp.bitwise_and(at - i, COLS - 1)
            lane = jnp.bitwise_and(spot, 127)
            for r in range(3):
                rows = slice(8 * r, 8 * r + 8)
                pick = [
                    jnp.where(
                        spot >= 128,
                        jnp.take_along_axis(src[rows, 128:], lane, axis=1),
                        jnp.take_along_axis(src[rows, :128], lane, axis=1),
                    )
                    for src in (high, low)
                ]
                halo_recv[rows, 128 * t : 128 * t + 128] = jnp.where(i <= at, pick[0], pick[1])
        put_north()

    sub8 = iota((8, COLS), 0)
    hi_iota = lax.shift_right_logical(iota((SIDE, COLS), 0), 2).astype(F32).astype(BF16)
    cl_iota = iota((SIDE, COLS), 0).astype(F32).astype(BF16)
    zero = jnp.zeros((SIDE, COLS), BF16)
    one = jnp.ones((SIDE, COLS), BF16)

    def prepare(g, hi_r, cl_r, val_r):
        base = g * GROUP if isinstance(g, int) else pl.multiple_of(g * GROUP, GROUP)
        here = pl.ds(base, GROUP)
        nxt = pl.ds(base + GROUP, 1)
        deep = tally[here, :]
        face_depth = jnp.minimum(deep, jnp.where(sub8 == 7, tally[nxt, :], pltpu.roll(deep, 7, 0)))
        width = dx[here, :]
        reg = region[here, :]
        regf = reg.astype(F32) * LO
        member = [reg == b for b in range(REGIONS)]
        heat = theta_sum = wet_sum = jnp.zeros((8, COLS), F32)
        stats = jnp.zeros((8, 128), F32)
        for k in range(TIERS):
            t = th[k, here, :]
            face = 0.5 * (t + jnp.where(sub8 == 7, th[k, nxt, :], pltpu.roll(t, 7, 0)))
            vol = jnp.where(face_depth > k, dz_s[k] * width, 0.0)
            mass = vol * sp[k, here, :]
            pos = jnp.clip((face - (-2.0)) * (BINS / 32.0), 0.0, BINS - 1.0)
            low = jnp.minimum(jnp.floor(pos), BINS - 2.0)
            hi = jnp.floor((low + 0.5) * (1.0 / LO))
            hi_r[k] = hi
            cl_r[k] = (low - hi * LO) + regf
            for n, x in enumerate(two_terms(mass) + two_terms(mass * (pos - low))):
                for half in range(2):
                    val_r[k, half, pl.ds(n, 8, stride=8), :] = x[:, 128 * half : 128 * half + 128]
                    val_r[k, half, pl.ds(n + 4, 8, stride=8), :] = x[:, 128 * half : 128 * half + 128]
            heat = heat + mass * face
            theta_sum = theta_sum + vol * face
            wet_sum = wet_sum + vol
            for b in range(REGIONS):
                red = jnp.sum(jnp.where(member[b], mass, 0.0), axis=1, keepdims=True)
                stats = jnp.where(lane8 == b * TIERS + k, red, stats)
            yield
        f = flux[here, :] * area[here, :]
        for b in range(REGIONS):
            red = jnp.sum(jnp.where(member[b], heat, 0.0), axis=1, keepdims=True)
            stats = jnp.where(lane8 == HEAT + b, red, stats)
            red = jnp.sum(jnp.where(member[b], f, 0.0), axis=1, keepdims=True)
            stats = jnp.where(lane8 == FLUX + b, red, stats)
        stats = jnp.where(lane8 == THETA, jnp.sum(theta_sum, axis=1, keepdims=True), stats)
        stats = jnp.where(lane8 == WET, jnp.sum(wet_sum, axis=1, keepdims=True), stats)
        rs_send[g, REGIONS] = stats
        yield

    def bin_rows(hi_r, cl_r, val_r, part_r):
        for jj in range(GROUP):
            total = None
            for k in range(TIERS):
                hi = jnp.broadcast_to(hi_r[k, jj : jj + 1, :], (SIDE, COLS)).astype(BF16)
                cl = jnp.broadcast_to(cl_r[k, jj : jj + 1, :], (SIDE, COLS)).astype(BF16)
                val = jnp.concatenate([val_r[k, half, 8 * jj : 8 * jj + 8, :] for half in range(2)], axis=1)
                val = jnp.concatenate([val] * (SIDE // 8), axis=0).astype(BF16)
                lhs = jnp.where(hi == hi_iota, val, zero)
                rhs = jnp.where(cl == cl_iota, one, zero)
                d = lax.dot_general(lhs, rhs, (((1,), (1,)), ((), ())), preferred_element_type=F32)
                total = d if total is None else total + d
            part_r[pl.ds(jj, SIDE, stride=8), 0:SIDE] = total
            yield

    bin_lane = lax.rem(lane8, LO)
    bin_block = lax.div(lane8, LO)

    def arrange(g, part_r):
        s0 = [jnp.zeros((8, 128), F32)] * REGIONS
        s1 = [jnp.zeros((8, 128), F32)] * REGIONS
        for hi in range(HI):
            rows = [part_r[32 * hi + 8 * n : 32 * hi + 8 * n + 8, :] for n in range(4)]
            wx = rows[2] + rows[3]
            x = rows[0] + rows[1] - wx
            for b in range(REGIONS):
                at = bin_lane + LO * b
                s0[b] = jnp.where(bin_block == hi, jnp.take_along_axis(x, at, axis=1), s0[b])
                s1[b] = jnp.where(bin_block == hi, jnp.take_along_axis(wx, at, axis=1), s1[b])
            yield
        for b in range(REGIONS):
            rs_send[g, b] = s0[b] + jnp.where(lane8 == 0, 0.0, pltpu.roll(s1[b], 1, 1))
        yield

    def together(*parts):
        parts = [p for p in parts if p is not None]
        done = object()
        lead, rest = parts[0], parts[1:]
        per = [2] * len(rest)
        while next(lead, done) is not done:
            for p, n in zip(rest, per):
                for _ in range(n):
                    next(p, done)
        for p in rest:
            while next(p, done) is not done:
                pass

    def send(g):
        for t in range(REGIONS + 1):
            @pl.when(remote_tile(g, t))
            def _():
                rs_copy(g, t).start()

    set_a = (hi_a, cl_a, val_a)
    set_b = (hi_b, cl_b, val_b)

    for load in loads[:8]:
        load.wait()
    together(prepare(0, *set_a))

    fold_early = (l == NLAT - 1) & (x_own >= 2) & (y_own >= 2)

    def pair(i, carry):
        g = 2 * i
        together(bin_rows(*set_a, part_a), prepare(g + 1, *set_b), arrange(lax.max(g - 1, 0), part_b))

        @pl.when(i == 0)
        def _():
            for load in loads[8:]:
                load.wait()
            flux_totals()
            edge_rows()

        @pl.when(jnp.logical_and(i == 0, fold_early))
        def _():
            first_sends()

        chain_step(jnp.logical_and(i > 0, chip == 2 * i - 2))

        @pl.when(i > 0)
        def _():
            send(g - 1)
        together(bin_rows(*set_b, part_b), prepare(g + 2, *set_a), arrange(g, part_a))

        @pl.when(jnp.logical_and(i == 0, jnp.logical_not(fold_early)))
        def _():
            first_sends()

        chain_step(jnp.logical_and(i > 0, chip == 2 * i - 1))
        early_step(jnp.logical_and(i == 1, jnp.logical_or(chip == 5, chip == 6)))
        send(g)
        return carry

    lax.fori_loop(0, 3, pair, 0)
    @pl.when(l < NLAT - 1)
    def _():
        north_row()
        together(bin_rows(*set_a, part_a), prepare(7, *set_b), arrange(5, part_b))

    @pl.when(l == NLAT - 1)
    def _():
        together(bin_rows(*set_a, part_a), arrange(5, part_b))
        fold_row()
        together(prepare(7, *set_b))
    send(5)
    chain_step(chip == 4)
    together(bin_rows(*set_b, part_b), arrange(6, part_a))
    send(6)
    together(arrange(7, part_b))
    send(7)

    last_step()

    @pl.when(jnp.logical_and(core == 0, chip > 0))
    def _():
        down_copy().wait_recv()
    offset[...] = pair_flux[...] + jnp.where(core == 1, south_flux[...], 0.0)
    to_peers(lambda q: offset_copy(q).start())

    tiles = NLON * 2 + NLON // 2

    def owned(slot, g, t, scale, put):
        for c in (1, 0):
            at = 3 * c + slot
            landed(rs_recv.at[pl.ds(0, NLON - c)], rs_rsem.at[c, slot])
            parts = [rs_recv[at * NLON + q] for q in range(NLON)]
            if c == 1:
                parts = [jnp.where(q != o, p, 0.0) for q, p in enumerate(parts)] + [rs_send[g, t]]
            while len(parts) > 1:
                parts = [sum(parts[i : i + 2]) for i in range(0, len(parts), 2)]
            ag_send[at] = parts[0] * scale
            to = put(slot, g)
            to_peers(lambda q: pltpu.make_async_remote_copy(
                ag_send.at[at], to, ag_ssem, ag_rsem,
                device_id={"lon": q, "lat": 2 * chip + c}, device_id_type=MESH).start(), c == 0)
            if c == 1:
                to[...] = ag_send[at]

    def put_class(slot, g):
        return out_class.at[b_own, pl.ds(pl.multiple_of(8 * g, 8), 8)]

    def put_sums(slot, g):
        return out_sums.at[pl.ds(pl.multiple_of(8 * g, 8), 8)]

    has_sums = jnp.logical_or(b_own == 0, b_own == 3)
    no_sums = jnp.logical_not(has_sums)
    g_sum = lax.rem(turn + 1, 4) + jnp.where(b_own == 0, 4, 0)

    @pl.when(core == 1)
    def _():
        owned(0, turn, b_own, UNIT, put_class)

        @pl.when(jnp.logical_and(has_sums, g_sum < 7))
        def _():
            owned(2, g_sum, REGIONS, 1.0, put_sums)
        owned(1, 4 + turn, b_own, UNIT, put_class)

        @pl.when(jnp.logical_and(has_sums, g_sum == 7))
        def _():
            owned(2, g_sum, REGIONS, 1.0, put_sums)

    @pl.when(core == 0)
    def _():
        landed(rs_recv.at[pl.ds(0, tiles)], rs_ssem)
        pair_copy().wait_send()

    @pl.when(core == 1)
    def _():
        @pl.when(has_sums)
        def _():
            landed(rs_recv.at[pl.ds(0, tiles - 3)], rs_ssem)
            landed(rs_recv.at[pl.ds(0, 3 * (2 * NLON - 1))], ag_ssem)

        @pl.when(no_sums)
        def _():
            landed(rs_recv.at[pl.ds(0, tiles - 2)], rs_ssem)
            landed(rs_recv.at[pl.ds(0, 2 * (2 * NLON - 1))], ag_ssem)

        @pl.when(chip > 0)
        def _():
            pair_copy().wait_send()

        @pl.when(chip < 4)
        def _():
            chain_copy().wait_send()
    skip_sends(lambda copy: copy.wait_send())

    landed(rs_recv.at[pl.ds(0, NLON - 1)], off_ssem)

    @pl.when(l > 0)
    def _():
        halo_copy().wait_send()

    @pl.when(l == NLAT - 1)
    def _():
        landed(fold_recv.at[pl.ds(0, NLON - 1)], fold_ssem)

    landed(offsets.at[pl.ds(0, NLON - 1)], off_rsem)
    south = offset[...]
    for q in range(NLON):
        south = south + jnp.where(q != o, offsets[q], 0.0)

    @pl.when(core == 0)
    def _():
        landed(rs_recv.at[pl.ds(0, tiles)], ag_rsem)

    @pl.when(core == 1)
    def _():
        @pl.when(has_sums)
        def _():
            landed(rs_recv.at[pl.ds(0, tiles - 3)], ag_rsem)

        @pl.when(no_sums)
        def _():
            landed(rs_recv.at[pl.ds(0, tiles - 2)], ag_rsem)
    out_sums[ROWS - 8 : ROWS, :] = out_sums[ROWS - 8 : ROWS, :] + south


def finish(classes, sums, out_class, out_over, out_heat, out_impl):
    out_class[...] = classes[...]
    row, lane = iota((88, 128), 0), iota((88, 128), 1)
    upto = (row < HEAT) & (lane <= row) & (lax.div(lane, TIERS) == lax.div(row, TIERS))
    volume = (row >= HEAT) & (row < HEAT + 4) & (lax.div(lane, TIERS) == row - HEAT)
    same = (row >= 72) & (lane == row - 8)
    pick = jnp.where(upto | volume | same, 1.0, 0.0)
    res = lax.dot_general(
        pick, sums[...], (((1,), (1,)), ((), ())), precision=lax.Precision.HIGHEST, preferred_element_type=F32)
    for b in range(REGIONS):
        out_over[b] = UNIT * res[TIERS * b : TIERS * b + TIERS]
    at = HEAT + 8
    mean = res[at + 4 : at + 5] / res[at + 5 : at + 6]
    out_heat[...] = (UNIT / 16.0) * (res[at : at + 4] - res[HEAT : HEAT + 4] * mean)
    flux = res[FLUX + 8 : FLUX + 16]
    south_of = jnp.where(iota((ROWS, ROWS), 0) <= iota((ROWS, ROWS), 1), 1.0, 0.0)
    c = jnp.dot(flux, south_of, precision=lax.Precision.HIGHEST, preferred_element_type=F32)
    out_impl[...] = IMPLIED * (c[0:4] + flux[4:8, ROWS - 1 : ROWS])


def body(speed, theta, dz, dx, area, flux, tally, region, seam):
    any_ = pl.BlockSpec(memory_space=pltpu.HBM)
    vmem = pl.BlockSpec(memory_space=pltpu.VMEM)
    dma = pltpu.SemaphoreType.DMA
    inputs = (speed, theta, dz, dx, area, flux, tally, region, seam)
    inputs = [pltpu.with_memory_space_constraint(x, pltpu.HBM) for x in inputs]
    rows = [pltpu.VMEM((TIERS, GROUP, COLS), F32)] * 2
    sets = (rows + [pltpu.VMEM((TIERS, 2, 8 * GROUP, 128), F32), pltpu.VMEM((8 * SIDE, 128), F32)]) * 2
    classes, sums = pl.pallas_call(
        kernel,
        out_shape=(
            jax.ShapeDtypeStruct((REGIONS, ROWS, BINS), F32),
            jax.ShapeDtypeStruct((ROWS, 128), F32),
        ),
        in_specs=[any_] * 9,
        out_specs=(vmem, vmem),
        scratch_shapes=[
            pltpu.VMEM((TIERS, ROWS + 8, COLS), F32),
            pltpu.VMEM((TIERS, ROWS, COLS), F32),
            pltpu.VMEM((ROWS, COLS), F32),
            pltpu.VMEM((ROWS, COLS), F32),
            pltpu.VMEM((ROWS, COLS), F32),
            pltpu.VMEM((ROWS + 8, COLS), jnp.int32),
            pltpu.VMEM((ROWS, COLS), jnp.int32),
            pltpu.SMEM((TIERS,), F32),
            pltpu.SMEM((COLS,), jnp.int32),
            *sets,
            pltpu.VMEM((ROWS // 8, REGIONS + 1, 8, 128), F32),
            pltpu.VMEM((2 * 3 * NLON, 8, 128), F32),
            pltpu.VMEM((2 * 3, 8, 128), F32),
            pltpu.VMEM((24, COLS), F32),
            pltpu.VMEM((24, COLS), F32),
            pltpu.VMEM((24, COLS), F32),
            pltpu.VMEM((NLON, 24, COLS), F32),
            *([pltpu.VMEM((8, 128), F32)] * 5),
            pltpu.VMEM((NLON, 8, 128), F32),
            pltpu.VMEM((3, 8, 128), F32),
            dma((11,)),
            dma, dma((2, 3)), dma, dma,
            dma, dma,
            *([dma] * 8), dma((3,)), dma((3,)),
        ],
        compiler_params=pltpu.CompilerParams(collective_id=0, has_side_effects=True, vmem_limit_bytes=VMEM_LIMIT),
    )(*inputs)
    out_class, over, heat, impl = pl.pallas_call(
        finish,
        out_shape=(
            jax.ShapeDtypeStruct((REGIONS, ROWS, BINS), F32),
            jax.ShapeDtypeStruct((REGIONS, TIERS, ROWS), F32),
            jax.ShapeDtypeStruct((REGIONS, ROWS), F32),
            jax.ShapeDtypeStruct((REGIONS, ROWS), F32),
        ),
        in_specs=[vmem, vmem],
        out_specs=(vmem,) * 4,
        compiler_params=pltpu.CompilerParams(vmem_limit_bytes=4 * 2**20),
    )(classes, sums)
    return out_class, jnp.transpose(over, (0, 2, 1)), heat, impl


def solution(mesh):
    in_specs = (
        P(None, "lat", "lon"),
        P(None, "lat", "lon"),
        P(),
        P("lat", "lon"),
        P("lat", "lon"),
        P("lat", "lon"),
        P("lat", "lon"),
        P("lat", "lon"),
        P("lon"),
    )
    out_specs = (P(None, "lat", None), P(None, "lat", None), P(None, "lat"), P(None, "lat"))
    return jax.shard_map(body, mesh=mesh, in_specs=in_specs, out_specs=out_specs, check_vma=False)
```
